32 devices in a mesh: gx: 4 (over z), gy: 8 (over y, x, core).
Axes of the slice: x: 2, y: 2, z: 4, core: 2. Of those that a mesh axis runs over, the one named last changes fastest.
Arguments:
- inputs: float32 [4096, 2304], P('gy', 'gx'), may hold values from -8 to 8
- segment_ids: int32 [32, 128], P(('gx', 'gy')), may hold values from 0 to 3, never falling along the last dimension, each value on 1 to 64 neighbouring positions
- qkv_weight: bfloat16 [2304, 4096], P('gx', 'gy'), may hold values from -1 to 1
- out_weight: bfloat16 [2048, 2304], P('gy', 'gx'), may hold values from -0.125 to 0.125
- gate_up_weight: bfloat16 [2304, 2, 9216], P('gx', None, 'gy'), may hold values from -0.125 to 0.125
- down_weight: bfloat16 [9216, 2304], P('gy', 'gx'), may hold values from -0.0625 to 0.0625
- first_gain: float32 [2304], P('gx'), may hold values from 0.5 to 1.5
- second_gain: float32 [2304], P('gx'), may hold values from 0.5 to 1.5
- third_gain: float32 [2304], P('gx'), may hold values from 0.5 to 1.5
- fourth_gain: float32 [2304], P('gx'), may hold values from 0.5 to 1.5
- cotangent: float32 [4096, 2304], P('gy', 'gx'), may hold values from -6 to 6
Outputs:
- outputs: float32 [4096, 2304], P('gy', 'gx')
- input_grad: float32 [4096, 2304], P('gy', 'gx')
- qkv_grad: float32 [2304, 4096], P('gx', 'gy')
- out_grad: float32 [2048, 2304], P('gy', 'gx')
- gate_up_grad: float32 [2304, 2, 9216], P('gx', None, 'gy')
- down_grad: float32 [9216, 2304], P('gy', 'gx')
- first_grad: float32 [2304], P('gx')
- second_grad: float32 [2304], P('gx')
- third_grad: float32 [2304], P('gx')
- fourth_grad: float32 [2304], P('gx')
The draws below stay inside these ranges and needn't reach their ends.
Inputs may be any that keep to these rules, and one draw needn't show every extreme that they name: `segment_ids`: in each row (one block of 128 tokens) the ids never fall, every id appears, and one id's tokens are one packed sequence of at most 64 tokens.
All inputs are finite; a program needn't handle non-finite values.
Results may differ from the reference program's by a relative error of at most 0.013.
Values may be sent and summed in bfloat16 or wider, within the bound.
A program may use at most 320 MiB of HBM per device.

```python
import math
import jax
import jax.numpy as jnp
import numpy as np
from jax import lax

D = 2304
QUERY_HEADS = 8
KEY_VALUE_HEADS = 4
HEAD_SIZE = 256
FF = 9216
TOK_DEV = 128
SEG_COUNT = 4
SEQ_MAX = 64
QW = 2048
QKV = 4096
BLOCKS = 32
TOKENS = 4096


def shared_direction(key):
    return jax.random.truncated_normal(jax.random.fold_in(key, 4099), -2.5, 2.5, (D,), jnp.float32)


def draw_inputs(key, part):
    common = shared_direction(key)
    jitter_key = jax.random.fold_in(key, 17)
    jitter = jax.random.truncated_normal(jitter_key, -5.0, 5.0, (TOKENS, D), jnp.float32)
    return jitter + common[None, :]


def draw_qkv_weight(key, part):
    common = shared_direction(key)
    base_part = jax.random.truncated_normal(jax.random.fold_in(key, 29), -3.0, 3.0, (D, QKV), jnp.float32) * D ** (-0.5)
    half_dim = HEAD_SIZE // 2
    places = jnp.arange(HEAD_SIZE, dtype=jnp.int32)
    slow_dims = (places % half_dim >= 3 * half_dim // 4).astype(jnp.float32)
    slow_count = 2 * (half_dim - 3 * half_dim // 4)
    strength = math.sqrt(80.0 * math.sqrt(HEAD_SIZE) / slow_count)
    rotation_signs = (2 * jax.random.randint(jax.random.fold_in(key, 31), (KEY_VALUE_HEADS, HEAD_SIZE), 0, 2) - 1).astype(jnp.float32)
    key_extent = jax.random.uniform(jax.random.fold_in(key, 37), (KEY_VALUE_HEADS, HEAD_SIZE), jnp.float32, 0.75, 1.25)
    query_extent = jax.random.uniform(jax.random.fold_in(key, 41), (KEY_VALUE_HEADS, QUERY_HEADS // KEY_VALUE_HEADS, HEAD_SIZE), jnp.float32, 0.75, 1.25)
    key_offset = strength * rotation_signs * key_extent * slow_dims[None, :]
    query_shift = strength * rotation_signs[:, None, :] * query_extent * slow_dims[None, None, :]
    query_cols = query_shift.reshape(QUERY_HEADS * HEAD_SIZE)
    key_columns = key_offset.reshape(KEY_VALUE_HEADS * HEAD_SIZE)
    value_columns = jnp.zeros((KEY_VALUE_HEADS * HEAD_SIZE,), jnp.float32)
    extra_cols = jnp.concatenate([query_cols, key_columns, value_columns])
    return (base_part + common[:, None] * extra_cols[None, :] / D).astype(jnp.bfloat16)


def shard_levels(stream_key, shape, shards, least, largest):
    loudness, own = 1.0, jax.random.fold_in(stream_key, 6)
    for dim, shards_of in shards:
        draws = jnp.exp(jax.random.uniform(jax.random.fold_in(own, dim), (shards_of,), jnp.float32, least / len(shards), largest / len(shards)))
        loudness = loudness * jnp.repeat(draws, shape[dim] // shards_of).reshape([-1 if axis == dim else 1 for axis in range(len(shape))])
    return loudness


def profile(count, total, most, skew):
    portions = [(1 << 20) // math.isqrt(rank ** skew) + 1 for rank in range(2, count + 1)]
    rest, given = total - most - (count - 1), [1] * (count - 1)
    while rest > 0:
        free = [i for i in range(count - 1) if given[i] < most]
        mass, remaining = sum([portions[i] for i in free]), rest
        for i in free:
            extra = min(most - given[i], max(1, remaining * portions[i] // mass), rest)
            given[i] = given[i] + extra
            rest = rest - extra
    return np.array([most] + given)


def ragged_sizes(key, amount, total, bound, lean):
    if amount == 2:
        one = jax.random.randint(key, (), max(1, total - bound), min(bound, total - 1) + 1)
        return jnp.stack([one, total - one])
    tallies = jnp.asarray(profile(amount, total, bound, lean), jnp.int32)
    twos = (amount - 1) // 2
    donor, receiver = tallies[1:1 + 2 * twos:2], tallies[2:2 + 2 * twos:2]
    room = jnp.minimum(donor - 1, bound - receiver)
    moved = jax.random.randint(jax.random.fold_in(key, 1), (twos,), 0, 1 << 20) % (room + 1)
    tallies = tallies.at[1:1 + 2 * twos:2].set(donor - moved).at[2:2 + 2 * twos:2].set(receiver + moved)
    return tallies[jax.random.permutation(jax.random.fold_in(key, 2), amount)]


def normal_values(rng, extent, scale, limit, pieces=(), held_as=jnp.bfloat16):
    entries = jax.random.normal(rng, extent, jnp.float32) * scale
    if len(pieces) > 0:
        entries = shard_levels(rng, extent, pieces, -0.22, 0.18) * entries
    return jnp.clip(entries, min=-limit, max=limit).astype(held_as)


def setup_inputs(seed: int = 0) -> dict:
    splits = jax.random.split(jax.random.key(seed), 12)
    inputs = draw_inputs(jax.random.fold_in(splits[11], 71), 0)
    segment_ids = jax.vmap(lambda own: jnp.searchsorted(jnp.cumsum(ragged_sizes(own, SEG_COUNT, TOK_DEV, SEQ_MAX, 1)), jnp.arange(TOK_DEV), side="right"))(jax.random.split(splits[1], BLOCKS)).reshape((BLOCKS, TOK_DEV)).astype(jnp.int32)
    qkv_weight = draw_qkv_weight(jax.random.fold_in(splits[11], 71), 0)
    out_weight = normal_values(splits[3], (QW, D), QW ** -0.5, 0.125, ((0, 8), (1, 4)))
    gate_up_weight = normal_values(splits[4], (D, 2, FF), D ** -0.5, 0.125, ((0, 4), (2, 8)))
    down_weight = normal_values(splits[5], (FF, D), FF ** -0.5, 0.0625, ((0, 8), (1, 4)))
    first_gain = jnp.clip(1.0 + 0.1 * jax.random.normal(splits[6], (D,), jnp.float32), 0.5, 1.5)
    second_gain = jnp.clip(1.0 + 0.1 * jax.random.normal(splits[7], (D,), jnp.float32), 0.5, 1.5)
    third_gain = jnp.clip(1.0 + 0.1 * jax.random.normal(splits[8], (D,), jnp.float32), 0.5, 1.5)
    fourth_gain = jnp.clip(1.0 + 0.1 * jax.random.normal(splits[9], (D,), jnp.float32), 0.5, 1.5)
    cotangent = normal_values(splits[10], (TOKENS, D), 1.0, 6.0, ((0, 8), (1, 4)), jnp.float32)
    return dict(inputs=inputs, segment_ids=segment_ids, qkv_weight=qkv_weight, out_weight=out_weight, gate_up_weight=gate_up_weight, down_weight=down_weight, first_gain=first_gain, second_gain=second_gain, third_gain=third_gain, fourth_gain=fourth_gain, cotangent=cotangent)


EPSILON = 1e-06
SOFT_CAP = 50.0
GELU_COEF = 0.7978845608028654
CUBIC_COEF = 0.044715

def rounded(values):
    return lax.optimization_barrier(values.astype(jnp.bfloat16)).astype(jnp.float32)

def gelu_parts(pre_gate):
    inner_arg = GELU_COEF * (pre_gate + CUBIC_COEF * pre_gate * pre_gate * pre_gate)
    tanh_value = jnp.tanh(inner_arg)
    activated = 0.5 * pre_gate * (1.0 + tanh_value)
    derivative = 0.5 * (1.0 + tanh_value) + 0.5 * pre_gate * (1.0 - tanh_value * tanh_value) * GELU_COEF * (1.0 + 3.0 * CUBIC_COEF * pre_gate * pre_gate)
    return (activated, derivative)

def block_layout(segment_row):
    length_total = segment_row.shape[0]
    places = jnp.arange(length_total, dtype=jnp.int32)
    same_doc = segment_row[:, None] == segment_row[None, :]
    starts = lax.optimization_barrier(jnp.min(jnp.where(same_doc, places[None, :], length_total), axis=1)).astype(jnp.int32)
    allowed = jnp.logical_and(same_doc, places[None, :] <= places[:, None])
    return (places - starts, allowed)

def rope_tables(position):
    half_dim = HEAD_SIZE // 2
    freq_steps = jnp.arange(half_dim, dtype=jnp.float32)
    frequency = jnp.exp(freq_steps * (-2.0 * math.log(10000.0) / HEAD_SIZE))
    angles = position.astype(jnp.float32)[:, None] * frequency[None, :]
    return (jnp.cos(angles)[:, None, :], jnp.sin(angles)[:, None, :])

def rotate(values, cos_table, sin_table, direction):
    half_dim = values.shape[-1] // 2
    leading = values[..., :half_dim]
    trailing = values[..., half_dim:]
    return jnp.concatenate([leading * cos_table - direction * trailing * sin_table, trailing * cos_table + direction * leading * sin_table], axis=-1)

def capped_scores(rotated_query, k_rot):
    token_rows = rotated_query.shape[0]
    query_groups = rotated_query.reshape(token_rows, KEY_VALUE_HEADS, QUERY_HEADS // KEY_VALUE_HEADS, HEAD_SIZE).astype(jnp.float32)
    raw_scores = jnp.einsum('tkgd,skd->kgts', query_groups, k_rot.astype(jnp.float32)) * HEAD_SIZE ** (-0.5)
    return SOFT_CAP * jnp.tanh(raw_scores / SOFT_CAP)

def attention_forward(query_key_value_rows, segment_row):
    token_rows = query_key_value_rows.shape[0]
    query_span_width = QUERY_HEADS * HEAD_SIZE
    key_value_width = KEY_VALUE_HEADS * HEAD_SIZE
    position, allowed = block_layout(segment_row)
    cos_table, sin_table = rope_tables(position)
    query_part = query_key_value_rows[:, :query_span_width].astype(jnp.float32).reshape(token_rows, QUERY_HEADS, HEAD_SIZE)
    key_slice = query_key_value_rows[:, query_span_width:query_span_width + key_value_width].astype(jnp.float32).reshape(token_rows, KEY_VALUE_HEADS, HEAD_SIZE)
    value_slice = query_key_value_rows[:, query_span_width + key_value_width:].reshape(token_rows, KEY_VALUE_HEADS, HEAD_SIZE)
    rotated_query = rotate(query_part, cos_table, sin_table, 1.0).astype(jnp.bfloat16)
    k_rot = rotate(key_slice, cos_table, sin_table, 1.0).astype(jnp.bfloat16)
    capped = capped_scores(rotated_query, k_rot)
    log_total = jnp.log(lax.optimization_barrier(jnp.sum(jnp.where(allowed, jnp.exp(capped), 0.0), axis=-1)))
    weights_f = jnp.where(allowed, jnp.exp(capped - log_total[..., None]), 0.0)
    mixing_rows = jnp.einsum('kgts,skd->tkgd', rounded(weights_f), value_slice.astype(jnp.float32))
    mixing_rows = mixing_rows.astype(jnp.bfloat16).reshape(token_rows, query_span_width)
    return (mixing_rows, (rotated_query, k_rot, value_slice, log_total))

def attention_backward(mixing_gradient, mixing_rows, saved, segment_row):
    rotated_query, k_rot, value_slice, log_total = saved
    token_rows = mixing_gradient.shape[0]
    heads_per_group = QUERY_HEADS // KEY_VALUE_HEADS
    position, allowed = block_layout(segment_row)
    cos_table, sin_table = rope_tables(position)
    capped = capped_scores(rotated_query, k_rot)
    weights_f = jnp.where(allowed, jnp.exp(capped - log_total[..., None]), 0.0)
    gradient_by_group = mixing_gradient.reshape(token_rows, KEY_VALUE_HEADS, heads_per_group, HEAD_SIZE).astype(jnp.float32)
    output_by_group = mixing_rows.reshape(token_rows, KEY_VALUE_HEADS, heads_per_group, HEAD_SIZE).astype(jnp.float32)
    row_delta = jnp.einsum('tkgd,tkgd->kgt', gradient_by_group, output_by_group)
    value_gradient = jnp.einsum('maew,emaq->wmq', rounded(weights_f), gradient_by_group)
    weight_grad = jnp.einsum('tkgd,skd->kgts', gradient_by_group, value_slice.astype(jnp.float32))
    score_gradient = weights_f * (weight_grad - row_delta[..., None]) * (1.0 - (capped / SOFT_CAP) ** 2) * HEAD_SIZE ** (-0.5)
    score_gradient = rounded(score_gradient)
    query_gradient = jnp.einsum('kgts,skd->tkgd', score_gradient, k_rot.astype(jnp.float32)).reshape(token_rows, QUERY_HEADS, HEAD_SIZE)
    key_gradient = jnp.einsum('maew,emaq->wmq', score_gradient, rotated_query.reshape(token_rows, KEY_VALUE_HEADS, heads_per_group, HEAD_SIZE).astype(jnp.float32))
    query_gradient = rotate(query_gradient, cos_table, sin_table, -1.0)
    key_gradient = rotate(key_gradient, cos_table, sin_table, -1.0)
    return jnp.concatenate([query_gradient.reshape(token_rows, QUERY_HEADS * HEAD_SIZE), key_gradient.reshape(token_rows, KEY_VALUE_HEADS * HEAD_SIZE), value_gradient.reshape(token_rows, KEY_VALUE_HEADS * HEAD_SIZE)], axis=1).astype(jnp.bfloat16)

def row_scale(values):
    return lax.rsqrt(lax.optimization_barrier(jnp.mean(values * values, axis=1, keepdims=True)) + EPSILON)

def norm_back(grad_rows, unit_rows, scale_rows, gain):
    scaled = grad_rows * gain
    return scale_rows * (scaled - unit_rows * lax.optimization_barrier(jnp.mean(scaled * unit_rows, axis=1, keepdims=True)))

def reference(inputs, segment_ids, qkv_weight, out_weight, gate_up_weight, down_weight, first_gain, second_gain, third_gain, fourth_gain, cotangent):
    total_rows = inputs.shape[0]
    width = inputs.shape[1]
    span = min(total_rows, 4096)
    steps_total = total_rows // span
    per_block = span // TOK_DEV
    gate_weight = gate_up_weight[:, 0, :]
    up_weight = gate_up_weight[:, 1, :]
    f32 = jnp.float32

    def one_span(grads, rows_in):
        x_rows, seg_rows, cot_rows = rows_in
        scale_one = row_scale(x_rows)
        unit_one = x_rows * scale_one
        normed_one = (unit_one * first_gain).astype(jnp.bfloat16)
        query_key_value_rows = jnp.dot(normed_one, qkv_weight, preferred_element_type=f32).astype(jnp.bfloat16)
        mixing_rows, saved = jax.vmap(attention_forward)(query_key_value_rows.reshape(per_block, TOK_DEV, QKV), seg_rows)
        mixed_flat = mixing_rows.reshape(span, QW)
        attn_branch = jnp.dot(mixed_flat, out_weight, preferred_element_type=f32)
        scale_two = row_scale(attn_branch)
        unit_two = attn_branch * scale_two
        middle = x_rows + unit_two * second_gain
        scale_three = row_scale(middle)
        unit_three = middle * scale_three
        normed_two = (unit_three * third_gain).astype(jnp.bfloat16)
        pre_gate = jnp.dot(normed_two, gate_weight, preferred_element_type=f32)
        up_part = jnp.dot(normed_two, up_weight, preferred_element_type=f32)
        gelu_value, gelu_slope = gelu_parts(pre_gate)
        hidden = (gelu_value * up_part).astype(jnp.bfloat16)
        ff_branch = jnp.dot(hidden, down_weight, preferred_element_type=f32)
        scale_four = row_scale(ff_branch)
        unit_four = ff_branch * scale_four
        outputs = middle + unit_four * fourth_gain
        ff_grad = norm_back(cot_rows, unit_four, scale_four, fourth_gain).astype(jnp.bfloat16)
        hidden_grad = jnp.dot(ff_grad, down_weight.T, preferred_element_type=f32)
        gate_grad = (hidden_grad * up_part * gelu_slope).astype(jnp.bfloat16)
        up_grad = (hidden_grad * gelu_value).astype(jnp.bfloat16)
        normed_two_grad = jnp.dot(gate_grad, gate_weight.T, preferred_element_type=f32) + jnp.dot(up_grad, up_weight.T, preferred_element_type=f32)
        middle_grad = cot_rows + norm_back(normed_two_grad, unit_three, scale_three, third_gain)
        branch_grad = norm_back(middle_grad, unit_two, scale_two, second_gain).astype(jnp.bfloat16)
        mixing_gradient = jnp.dot(branch_grad, out_weight.T, preferred_element_type=f32).astype(jnp.bfloat16)
        qkv_grad_rows = jax.vmap(attention_backward)(mixing_gradient.reshape(per_block, TOK_DEV, QW), mixing_rows, saved, seg_rows)
        qkv_grad_rows = qkv_grad_rows.reshape(span, QKV)
        normed_one_grad = jnp.dot(qkv_grad_rows, qkv_weight.T, preferred_element_type=f32)
        input_grad = middle_grad + norm_back(normed_one_grad, unit_one, scale_one, first_gain)
        gate_up_step = jnp.stack([jnp.dot(normed_two.T, gate_grad, preferred_element_type=f32), jnp.dot(normed_two.T, up_grad, preferred_element_type=f32)], axis=1)
        updated = (grads[0] + jnp.dot(normed_one.T, qkv_grad_rows, preferred_element_type=f32), grads[1] + jnp.dot(mixed_flat.T, branch_grad, preferred_element_type=f32), grads[2] + gate_up_step, grads[3] + jnp.dot(hidden.T, ff_grad, preferred_element_type=f32), grads[4] + lax.optimization_barrier(jnp.sum(normed_one_grad * unit_one, axis=0)), grads[5] + lax.optimization_barrier(jnp.sum(middle_grad * unit_two, axis=0)), grads[6] + lax.optimization_barrier(jnp.sum(normed_two_grad * unit_three, axis=0)), grads[7] + lax.optimization_barrier(jnp.sum(cot_rows * unit_four, axis=0)))
        return (updated, (outputs, input_grad))
    start_grads = (jnp.zeros(qkv_weight.shape, jnp.float32), jnp.zeros(out_weight.shape, jnp.float32), jnp.zeros(gate_up_weight.shape, jnp.float32), jnp.zeros(down_weight.shape, jnp.float32), jnp.zeros((width,), jnp.float32), jnp.zeros((width,), jnp.float32), jnp.zeros((width,), jnp.float32), jnp.zeros((width,), jnp.float32))
    stacked_in = (inputs.reshape(steps_total, span, width), segment_ids.reshape(steps_total, per_block, TOK_DEV), cotangent.reshape(steps_total, span, width))
    grads, (outputs, input_grad) = lax.scan(one_span, start_grads, stacked_in)
    return (outputs.reshape(total_rows, width), input_grad.reshape(total_rows, width), grads[0], grads[1], grads[2], grads[3], grads[4], grads[5], grads[6], grads[7])
```

```python
import functools
import math

import jax
import jax.numpy as jnp
from jax import lax
from jax.experimental import pallas as pl
from jax.experimental.pallas import tpu as pltpu
from jax.sharding import PartitionSpec as P

QUERY_HEADS = 8
KEY_VALUE_HEADS = 4
HEAD_SIZE = 256


EPSILON = 1e-06
SOFT_CAP = 50.0
GELU_COEF = 0.7978845608028654
CUBIC_COEF = 0.044715

BF = jnp.bfloat16
F32 = jnp.float32
MESH = pl.DeviceIdType.MESH


def product(form, left, right):
    return jnp.einsum(form, left, right, preferred_element_type=F32)


def gelu_parts(pre_gate):
    inner_arg = GELU_COEF * (pre_gate + CUBIC_COEF * pre_gate * pre_gate * pre_gate)
    tanh_value = jnp.tanh(inner_arg)
    activated = 0.5 * pre_gate * (1.0 + tanh_value)
    derivative = 0.5 * (1.0 + tanh_value) + 0.5 * pre_gate * (
        1.0 - tanh_value * tanh_value
    ) * GELU_COEF * (1.0 + 3.0 * CUBIC_COEF * pre_gate * pre_gate)
    return (activated, derivative)


def block_layout(segment_row):
    length_total = segment_row.shape[0]
    places = jnp.arange(length_total, dtype=jnp.int32)
    same_doc = segment_row[:, None] == segment_row[None, :]
    starts = jnp.min(jnp.where(same_doc, places[None, :], length_total), axis=1)
    allowed = jnp.logical_and(same_doc, places[None, :] <= places[:, None])
    return (places - starts, allowed)


def rope_tables(position):
    half_dim = HEAD_SIZE // 2
    freq_steps = jnp.arange(half_dim, dtype=F32)
    frequency = jnp.exp(freq_steps * (-2.0 * math.log(10000.0) / HEAD_SIZE))
    angles = position.astype(F32)[:, None] * frequency[None, :]
    return (jnp.cos(angles)[:, None, :], jnp.sin(angles)[:, None, :])


def rotate(values, cos_table, sin_table, direction):
    half_dim = values.shape[-1] // 2
    leading = values[..., :half_dim]
    trailing = values[..., half_dim:]
    return jnp.concatenate(
        [
            leading * cos_table - direction * trailing * sin_table,
            trailing * cos_table + direction * leading * sin_table,
        ],
        axis=-1,
    )


def capped_scores(rotated_query, k_rot):
    token_rows = rotated_query.shape[0]
    query_groups = rotated_query.reshape(
        token_rows, KEY_VALUE_HEADS, QUERY_HEADS // KEY_VALUE_HEADS, HEAD_SIZE
    )
    raw_scores = product("tkgd,skd->kgts", query_groups, k_rot) * HEAD_SIZE ** (-0.5)
    return SOFT_CAP * jnp.tanh(raw_scores / SOFT_CAP)


def attention_forward(rows, layout):
    token_rows = rows.shape[0]
    query_span_width = QUERY_HEADS * HEAD_SIZE
    key_value_width = KEY_VALUE_HEADS * HEAD_SIZE
    allowed, cos_table, sin_table = layout
    query_part = (
        rows[:, :query_span_width].astype(F32).reshape(token_rows, QUERY_HEADS, HEAD_SIZE)
    )
    key_slice = (
        rows[:, query_span_width : query_span_width + key_value_width]
        .astype(F32)
        .reshape(token_rows, KEY_VALUE_HEADS, HEAD_SIZE)
    )
    value_slice = rows[:, query_span_width + key_value_width :].reshape(
        token_rows, KEY_VALUE_HEADS, HEAD_SIZE
    )
    rotated_query = rotate(query_part, cos_table, sin_table, 1.0).astype(BF)
    k_rot = rotate(key_slice, cos_table, sin_table, 1.0).astype(BF)
    capped = capped_scores(rotated_query, k_rot)
    log_total = jnp.log(jnp.sum(jnp.where(allowed, jnp.exp(capped), 0.0), axis=-1))
    weights_f = jnp.where(allowed, jnp.exp(capped - log_total[..., None]), 0.0)
    mixing_rows = product("kgts,skd->tkgd", weights_f.astype(BF), value_slice)
    mixing_rows = mixing_rows.astype(BF).reshape(token_rows, query_span_width)
    return (mixing_rows, (rotated_query, k_rot, value_slice, log_total))


def attention_backward(mixing_gradient, mixing_rows, saved, layout):
    rotated_query, k_rot, value_slice, log_total = saved
    token_rows = mixing_gradient.shape[0]
    heads_per_group = QUERY_HEADS // KEY_VALUE_HEADS
    allowed, cos_table, sin_table = layout
    capped = capped_scores(rotated_query, k_rot)
    weights_f = jnp.where(allowed, jnp.exp(capped - log_total[..., None]), 0.0)
    gradient_by_group = mixing_gradient.reshape(
        token_rows, KEY_VALUE_HEADS, heads_per_group, HEAD_SIZE
    )
    output_by_group = mixing_rows.reshape(token_rows, KEY_VALUE_HEADS, heads_per_group, HEAD_SIZE)
    row_delta = product("tkgd,tkgd->kgt", gradient_by_group, output_by_group)
    value_gradient = product("maew,emaq->wmq", weights_f.astype(BF), gradient_by_group)
    weight_grad = product("tkgd,skd->kgts", gradient_by_group, value_slice)
    score_gradient = (
        weights_f
        * (weight_grad - row_delta[..., None])
        * (1.0 - (capped / SOFT_CAP) ** 2)
        * HEAD_SIZE ** (-0.5)
    )
    score_gradient = score_gradient.astype(BF)
    query_gradient = product("kgts,skd->tkgd", score_gradient, k_rot).reshape(
        token_rows, QUERY_HEADS, HEAD_SIZE
    )
    key_gradient = product(
        "maew,emaq->wmq",
        score_gradient,
        rotated_query.reshape(token_rows, KEY_VALUE_HEADS, heads_per_group, HEAD_SIZE),
    )
    query_gradient = rotate(query_gradient, cos_table, sin_table, -1.0)
    key_gradient = rotate(key_gradient, cos_table, sin_table, -1.0)
    return jnp.concatenate(
        [
            query_gradient.reshape(token_rows, QUERY_HEADS * HEAD_SIZE),
            key_gradient.reshape(token_rows, KEY_VALUE_HEADS * HEAD_SIZE),
            value_gradient.reshape(token_rows, KEY_VALUE_HEADS * HEAD_SIZE),
        ],
        axis=1,
    ).astype(BF)


def inverse_rms(values):
    return lax.rsqrt(jnp.mean(values * values, axis=1, keepdims=True) + EPSILON)


def norm_back(grad_rows, unit_rows, scale_rows, gain):
    scaled = grad_rows * gain
    return scale_rows * (scaled - unit_rows * jnp.mean(scaled * unit_rows, axis=1, keepdims=True))


def thirds(values):
    high = lax.reduce_precision(values, 8, 7)
    rest = values - high
    middle = lax.reduce_precision(rest, 8, 7)
    return jnp.concatenate([high, middle, rest - middle], axis=0).astype(BF)


def join_thirds(rows):
    count = rows.shape[-2] // 3
    rows = rows.astype(F32)
    return rows[..., :count, :] + rows[..., count : 2 * count, :] + rows[..., 2 * count :, :]


def to_whole_rows(values, nx, extra=None):
    width = values.shape[1]
    parts = values.astype(BF).reshape(nx, -1, width)
    if extra is not None:
        parts = jnp.concatenate(
            [parts, jnp.broadcast_to(extra[None], (nx,) + extra.shape)], axis=1
        )
    parts = lax.all_to_all(parts, "gx", split_axis=0, concat_axis=0, tiled=True)
    return parts.transpose(1, 0, 2).reshape(-1, nx * width)


def to_width_blocks(values, nx, extra=None):
    values = values.astype(BF)
    if extra is not None:
        values = jnp.concatenate([values, extra], axis=0)
    rows, whole = values.shape
    parts = values.reshape(rows, nx, whole // nx).transpose(1, 0, 2)
    return lax.all_to_all(parts, "gx", split_axis=0, concat_axis=0, tiled=True)


def flip(index, mask):
    return index + mask - 2 * mask * ((index // mask) % 2)


def flip_all(index, masks):
    bit = 1
    while bit <= masks:
        if masks & bit:
            index = flip(index, bit)
        bit *= 2
    return index


def greet(me, bits):
    barrier = pltpu.get_barrier_semaphore()
    for bit in bits:
        pl.semaphore_signal(barrier, inc=1, device_id={"gy": flip(me, bit)}, device_id_type=MESH)
    pl.semaphore_wait(barrier, len(bits))


def bit_orders(size):
    bits = []
    bit = 2
    while bit < size:
        bits.append(bit)
        bit *= 2
    return (bits + [1], bits[::-1] + [1])


def spread_kernel(size, own_ref, all_ref, local_sem, send_sem, recv_sem):
    me = lax.axis_index("gy")
    orders = bit_orders(size)
    half = own_ref.shape[0] // 2
    greet(me, orders[0])
    keep = pltpu.make_async_copy(own_ref, all_ref.at[me], local_sem)
    keep.start()
    copies = {}
    arrival = {}

    def copy(h, bit, r):
        n = len(copies)
        rows = pl.ds(h * half, half)
        where = flip_all(me, r)
        source = own_ref.at[rows] if r == 0 else all_ref.at[where, rows]
        made = pltpu.make_async_remote_copy(
            src_ref=source,
            dst_ref=all_ref.at[where, rows],
            send_sem=send_sem.at[n],
            recv_sem=recv_sem.at[n],
            device_id={"gy": flip(me, bit)},
            device_id_type=MESH,
        )
        copies[h, bit, r] = made
        arrival[h, r ^ bit] = made
        made.start()

    for step in range(len(orders[0])):
        for h in range(2):
            copy(h, orders[h][step], 0)
    landed = set()

    def land(h, r):
        if (h, r) not in landed:
            landed.add((h, r))
            arrival[h, r].wait_recv()

    held = [[0], [0]]
    for step in range(len(orders[0])):
        for h in range(2):
            bit = orders[h][step]
            for r in held[h]:
                if r:
                    land(h, r)
                    copy(h, bit, r)
        for h in range(2):
            held[h] = held[h] + [r ^ orders[h][step] for r in held[h]]
    for h in range(2):
        for r in range(1, size):
            land(h, r)
    for made in copies.values():
        made.wait_send()
    keep.wait()


def spread(values):
    size = lax.axis_size("gy")
    values = values.astype(BF)
    rows, width = values.shape
    count = 2 * (size - 1)
    out = pl.pallas_call(
        functools.partial(spread_kernel, size),
        out_shape=jax.ShapeDtypeStruct((size, rows, width), values.dtype),
        in_specs=[pl.BlockSpec(memory_space=pltpu.VMEM)],
        out_specs=pl.BlockSpec(memory_space=pltpu.VMEM),
        scratch_shapes=[
            pltpu.SemaphoreType.DMA,
            pltpu.SemaphoreType.DMA((count,)),
            pltpu.SemaphoreType.DMA((count,)),
        ],
        compiler_params=pltpu.CompilerParams(collective_id=0, has_side_effects=True, vmem_limit_bytes=32 << 20),
        cost_estimate=pl.CostEstimate(flops=0, bytes_accessed=size * rows * width * 16, transcendentals=0),
        name="spread",
    )(values)
    return out.reshape(size * rows, width)


def settle_kernel(size, parts_ref, sum_ref, came, kept, send_sem, recv_sem):
    me = lax.axis_index("gy")
    orders = tuple(order[::-1] for order in bit_orders(size))
    half = sum_ref.shape[0] // 2
    strip = 16
    greet(me, orders[0])
    slot = {}
    for h in range(2):
        held = list(range(size))
        for step, bit in enumerate(orders[h]):
            held = [r for r in held if not r & bit]
            for r in held:
                slot[h, step, r] = len(slot)
    copies = {}

    def view(h, step, r):
        if step == 0:
            return parts_ref.at[flip_all(me, r), pl.ds(h * half, half)]
        return kept.at[h, r]

    def send(h, step):
        bit = orders[h][step]
        gone = set()
        for b in orders[h][:step]:
            gone.add(b)
        for r in range(size):
            if r & bit and not any(r & b for b in gone):
                n = slot[h, step, r ^ bit]
                made = pltpu.make_async_remote_copy(
                    src_ref=view(h, step, r),
                    dst_ref=came.at[n],
                    send_sem=send_sem.at[n],
                    recv_sem=recv_sem.at[n],
                    device_id={"gy": flip(me, bit)},
                    device_id_type=MESH,
                )
                copies[h, step, r ^ bit] = made
                made.start()

    def gather(h, step, r, last):
        n = slot[h, step, r]
        copies[h, step, r].wait_recv()

        @pl.loop(0, half // strip)
        def _(i):
            rows = pl.ds(i * strip, strip)
            total = view(h, step, r)[rows].astype(F32) + came[n, rows].astype(F32)
            if last:
                sum_ref[pl.ds(h * half + i * strip, strip)] = total
            else:
                kept[h, r, rows] = total.astype(BF)

    steps = len(orders[0])
    for h in range(2):
        send(h, 0)
    for step in range(steps):
        for h in range(2):
            bits = orders[h][: step + 1]
            later = orders[h][step + 1] if step + 1 < steps else 0
            left = [r for r in range(size) if not any(r & b for b in bits)]
            for r in left:
                if r & later:
                    gather(h, step, r, False)
            if later:
                send(h, step + 1)
            for r in left:
                if not r & later:
                    gather(h, step, r, step == steps - 1)
    for made in copies.values():
        made.wait_send()


def settle(parts):
    size = lax.axis_size("gy")
    parts = parts.astype(BF)
    total, width = parts.shape
    rows = total // size
    count = 2 * (size - 1)
    return pl.pallas_call(
        functools.partial(settle_kernel, size),
        out_shape=jax.ShapeDtypeStruct((rows, width), F32),
        in_specs=[pl.BlockSpec(memory_space=pltpu.VMEM)],
        out_specs=pl.BlockSpec(memory_space=pltpu.VMEM),
        scratch_shapes=[
            pltpu.VMEM((count, rows // 2, width), BF),
            pltpu.VMEM((2, size, rows // 2, width), BF),
            pltpu.SemaphoreType.DMA((count,)),
            pltpu.SemaphoreType.DMA((count,)),
        ],
        compiler_params=pltpu.CompilerParams(collective_id=1, has_side_effects=True, vmem_limit_bytes=32 << 20),
        cost_estimate=pl.CostEstimate(flops=0, bytes_accessed=total * width * 16, transcendentals=0),
        name="settle",
    )(parts.reshape(size, rows, width))


def tally_kernel(size, own_ref, sum_ref, came, send_sem, recv_sem):
    me = lax.axis_index("gy")
    barrier = pltpu.get_barrier_semaphore()
    for d in range(1, size):
        pl.semaphore_signal(
            barrier, inc=1, device_id={"gy": (me + d) % size}, device_id_type=MESH
        )
    pl.semaphore_wait(barrier, size - 1)
    copies = []
    for d in range(1, size):
        made = pltpu.make_async_remote_copy(
            src_ref=own_ref,
            dst_ref=came.at[d],
            send_sem=send_sem.at[d],
            recv_sem=recv_sem.at[d],
            device_id={"gy": (me + d) % size},
            device_id_type=MESH,
        )
        made.start()
        copies.append(made)
    total = own_ref[...]
    for d in range(1, size):
        copies[d - 1].wait_recv()
        total = total + came[d]
    sum_ref[...] = total
    for made in copies:
        made.wait_send()


def tally(values, size, call):
    return pl.pallas_call(
        functools.partial(tally_kernel, size),
        out_shape=jax.ShapeDtypeStruct(values.shape, F32),
        in_specs=[pl.BlockSpec(memory_space=pltpu.VMEM)],
        out_specs=pl.BlockSpec(memory_space=pltpu.VMEM),
        scratch_shapes=[
            pltpu.VMEM((size,) + values.shape, F32),
            pltpu.SemaphoreType.DMA((size,)),
            pltpu.SemaphoreType.DMA((size,)),
        ],
        compiler_params=pltpu.CompilerParams(collective_id=call, has_side_effects=True),
        name="tally",
    )(values)


def make_shards(nx, ny):
    blocks = [((b // ny) * ny + b % ny, (b % nx) * ny + b // nx) for b in range(nx * ny)]

    def shards(
        inputs,
        segment_ids,
        qkv_weight,
        out_weight,
        gate_up_weight,
        down_weight,
        first_gain,
        second_gain,
        third_gain,
        fourth_gain,
        cotangent,
    ):
        width = inputs.shape[1]

        gains = thirds(jnp.stack([first_gain, second_gain, third_gain, fourth_gain]))
        rows_in = to_whole_rows(inputs, nx, gains)
        own = inputs.shape[0] // nx
        x_rows = rows_in[:own].astype(F32)
        gains = join_thirds(rows_in[own:])[:, None, :]
        qkv_w = lax.all_gather(qkv_weight, "gx", axis=0, tiled=True)
        out_w = lax.all_gather(out_weight, "gx", axis=1, tiled=True)
        gate_up_w = lax.all_gather(gate_up_weight, "gx", axis=0, tiled=True)
        down_w = lax.all_gather(down_weight, "gx", axis=1, tiled=True)
        cot_rows = to_whole_rows(cotangent, nx).astype(F32)

        segment_row = lax.ppermute(segment_ids[0], ("gx", "gy"), blocks)
        position, allowed = block_layout(segment_row)
        layout = (allowed,) + rope_tables(position)

        scale_one = inverse_rms(x_rows)
        unit_one = x_rows * scale_one
        normed_one = spread(unit_one * gains[0])
        rows = product("td,dc->tc", normed_one, qkv_w).astype(BF)
        rows = lax.all_to_all(rows, "gy", split_axis=0, concat_axis=1, tiled=True)
        mixing_rows, saved = attention_forward(rows, layout)
        mixed = lax.all_to_all(mixing_rows, "gy", split_axis=1, concat_axis=0, tiled=True)
        attn_branch = settle(product("tc,cd->td", mixed, out_w))
        scale_two = inverse_rms(attn_branch)
        unit_two = attn_branch * scale_two
        attn_term = unit_two * gains[1]
        middle = x_rows + attn_term
        scale_three = inverse_rms(middle)
        unit_three = middle * scale_three
        normed_two = spread(unit_three * gains[2])
        pre_gate = product("td,df->tf", normed_two, gate_up_w[:, 0, :])
        up_part = product("td,df->tf", normed_two, gate_up_w[:, 1, :])
        value, slope = gelu_parts(pre_gate)
        hidden = (value * up_part).astype(BF)
        ff_branch = settle(product("tf,fd->td", hidden, down_w))
        scale_four = inverse_rms(ff_branch)
        unit_four = ff_branch * scale_four
        ff_grad = spread(norm_back(cot_rows, unit_four, scale_four, gains[3]))
        delta = to_width_blocks(attn_term + unit_four * gains[3], nx)
        outputs = inputs + delta.reshape(inputs.shape).astype(F32)

        hidden_grad = product("td,fd->tf", ff_grad, down_w)
        down_sum = product("tf,tkd->kfd", hidden, ff_grad.reshape(-1, nx, width))
        down_grad = lax.psum_scatter(down_sum.astype(BF), "gx", scatter_dimension=0).astype(F32)
        gate_grad = (hidden_grad * up_part * slope).astype(BF)
        up_grad = (hidden_grad * value).astype(BF)
        normed_two_grad = settle(
            product("tf,df->td", gate_grad, gate_up_w[:, 0, :])
            + product("tf,df->td", up_grad, gate_up_w[:, 1, :])
        )
        gate_up_sum = jnp.stack(
            [
                product("td,tf->df", normed_two, gate_grad).astype(BF),
                product("td,tf->df", normed_two, up_grad).astype(BF),
            ],
            axis=1,
        )
        gate_up_grad = lax.psum_scatter(
            gate_up_sum, "gx", scatter_dimension=0, tiled=True
        ).astype(F32)
        middle_delta = norm_back(normed_two_grad, unit_three, scale_three, gains[2])
        middle_grad = cot_rows + middle_delta
        branch_grad = spread(norm_back(middle_grad, unit_two, scale_two, gains[1]))
        mixing_gradient = product("td,cd->tc", branch_grad, out_w).astype(BF)
        mixing_gradient = lax.all_to_all(
            mixing_gradient, "gy", split_axis=0, concat_axis=1, tiled=True
        )
        out_sum = product("tc,tkd->kcd", mixed, branch_grad.reshape(-1, nx, width))
        out_grad = lax.psum_scatter(out_sum.astype(BF), "gx", scatter_dimension=0).astype(F32)
        qkv_grad_rows = attention_backward(mixing_gradient, mixing_rows, saved, layout)
        qkv_grad_rows = lax.all_to_all(
            qkv_grad_rows, "gy", split_axis=1, concat_axis=0, tiled=True
        )
        normed_one_grad = settle(product("tc,dc->td", qkv_grad_rows, qkv_w))
        qkv_sum = product("td,tc->dc", normed_one, qkv_grad_rows)
        qkv_grad = lax.psum_scatter(
            qkv_sum.astype(BF), "gx", scatter_dimension=0, tiled=True
        ).astype(F32)
        late_term = tally(jnp.sum(normed_one_grad * unit_one, axis=0, keepdims=True), ny, 2)
        early_terms = tally(
            jnp.stack(
                [
                    jnp.sum(middle_grad * unit_two, axis=0),
                    jnp.sum(normed_two_grad * unit_three, axis=0),
                    jnp.sum(cot_rows * unit_four, axis=0),
                ]
            ),
            ny,
            3,
        )
        delta = to_width_blocks(
            middle_delta + norm_back(normed_one_grad, unit_one, scale_one, gains[0]),
            nx,
            thirds(jnp.concatenate([late_term, early_terms], axis=0)),
        )
        input_grad = cotangent + delta[:, :own].reshape(inputs.shape).astype(F32)
        terms = jnp.sum(join_thirds(delta[:, own:]), axis=0)
        return (outputs, input_grad, qkv_grad, out_grad, gate_up_grad, down_grad) + tuple(
            terms[i] for i in range(4)
        )

    return shards


def solution(mesh):
    placed = (
        P("gy", "gx"),
        P(("gx", "gy"), None),
        P("gx", "gy"),
        P("gy", "gx"),
        P("gx", None, "gy"),
        P("gy", "gx"),
        P("gx"),
        P("gx"),
        P("gx"),
        P("gx"),
        P("gy", "gx"),
    )
    return jax.shard_map(
        make_shards(mesh.shape["gx"], mesh.shape["gy"]),
        mesh=mesh,
        in_specs=placed,
        out_specs=(
            P("gy", "gx"),
            P("gy", "gx"),
            P("gx", "gy"),
            P("gy", "gx"),
            P("gx", None, "gy"),
            P("gy", "gx"),
            P("gx"),
            P("gx"),
            P("gx"),
            P("gx"),
        ),
        check_vma=False,
    )
```

```python
import functools
import math

import jax
import jax.numpy as jnp
from jax import lax
from jax.experimental import pallas as pl
from jax.experimental.pallas import tpu as pltpu
from jax.sharding import PartitionSpec as P

QUERY_HEADS = 8
KEY_VALUE_HEADS = 4
HEAD_SIZE = 256


EPSILON = 1e-06
SOFT_CAP = 50.0
GELU_COEF = 0.7978845608028654
CUBIC_COEF = 0.044715

BF = jnp.bfloat16
F32 = jnp.float32
MESH = pl.DeviceIdType.MESH


def product(form, left, right):
    return jnp.einsum(form, left, right, preferred_element_type=F32)


def gelu_parts(pre_gate):
    inner_arg = GELU_COEF * (pre_gate + CUBIC_COEF * pre_gate * pre_gate * pre_gate)
    tanh_value = jnp.tanh(inner_arg)
    activated = 0.5 * pre_gate * (1.0 + tanh_value)
    derivative = 0.5 * (1.0 + tanh_value) + 0.5 * pre_gate * (
        1.0 - tanh_value * tanh_value
    ) * GELU_COEF * (1.0 + 3.0 * CUBIC_COEF * pre_gate * pre_gate)
    return (activated, derivative)


def block_layout(segment_row):
    length_total = segment_row.shape[0]
    places = jnp.arange(length_total, dtype=jnp.int32)
    same_doc = segment_row[:, None] == segment_row[None, :]
    starts = jnp.min(jnp.where(same_doc, places[None, :], length_total), axis=1)
    allowed = jnp.logical_and(same_doc, places[None, :] <= places[:, None])
    return (places - starts, allowed)


def rope_tables(position):
    half_dim = HEAD_SIZE // 2
    freq_steps = jnp.arange(half_dim, dtype=F32)
    frequency = jnp.exp(freq_steps * (-2.0 * math.log(10000.0) / HEAD_SIZE))
    angles = position.astype(F32)[:, None] * frequency[None, :]
    return (jnp.cos(angles)[:, None, :], jnp.sin(angles)[:, None, :])


def rotate(values, cos_table, sin_table, direction):
    half_dim = values.shape[-1] // 2
    leading = values[..., :half_dim]
    trailing = values[..., half_dim:]
    return jnp.concatenate(
        [
            leading * cos_table - direction * trailing * sin_table,
            trailing * cos_table + direction * leading * sin_table,
        ],
        axis=-1,
    )


def capped_scores(rotated_query, k_rot):
    token_rows = rotated_query.shape[0]
    query_groups = rotated_query.reshape(
        token_rows, KEY_VALUE_HEADS, QUERY_HEADS // KEY_VALUE_HEADS, HEAD_SIZE
    )
    raw_scores = product("tkgd,skd->kgts", query_groups, k_rot) * HEAD_SIZE ** (-0.5)
    return SOFT_CAP * jnp.tanh(raw_scores / SOFT_CAP)


def attention_forward(rows, layout):
    token_rows = rows.shape[0]
    query_span_width = QUERY_HEADS * HEAD_SIZE
    key_value_width = KEY_VALUE_HEADS * HEAD_SIZE
    allowed, cos_table, sin_table = layout
    query_part = (
        rows[:, :query_span_width].astype(F32).reshape(token_rows, QUERY_HEADS, HEAD_SIZE)
    )
    key_slice = (
        rows[:, query_span_width : query_span_width + key_value_width]
        .astype(F32)
        .reshape(token_rows, KEY_VALUE_HEADS, HEAD_SIZE)
    )
    value_slice = rows[:, query_span_width + key_value_width :].reshape(
        token_rows, KEY_VALUE_HEADS, HEAD_SIZE
    )
    rotated_query = rotate(query_part, cos_table, sin_table, 1.0).astype(BF)
    k_rot = rotate(key_slice, cos_table, sin_table, 1.0).astype(BF)
    capped = capped_scores(rotated_query, k_rot)
    log_total = jnp.log(jnp.sum(jnp.where(allowed, jnp.exp(capped), 0.0), axis=-1))
    weights_f = jnp.where(allowed, jnp.exp(capped - log_total[..., None]), 0.0)
    mixing_rows = product("kgts,skd->tkgd", weights_f.astype(BF), value_slice)
    mixing_rows = mixing_rows.astype(BF).reshape(token_rows, query_span_width)
    return (mixing_rows, (rotated_query, k_rot, value_slice, log_total))


def attention_backward(mixing_gradient, mixing_rows, saved, layout):
    rotated_query, k_rot, value_slice, log_total = saved
    token_rows = mixing_gradient.shape[0]
    heads_per_group = QUERY_HEADS // KEY_VALUE_HEADS
    allowed, cos_table, sin_table = layout
    capped = capped_scores(rotated_query, k_rot)
    weights_f = jnp.where(allowed, jnp.exp(capped - log_total[..., None]), 0.0)
    gradient_by_group = mixing_gradient.reshape(
        token_rows, KEY_VALUE_HEADS, heads_per_group, HEAD_SIZE
    )
    output_by_group = mixing_rows.reshape(token_rows, KEY_VALUE_HEADS, heads_per_group, HEAD_SIZE)
    row_delta = product("tkgd,tkgd->kgt", gradient_by_group, output_by_group)
    value_gradient = product("maew,emaq->wmq", weights_f.astype(BF), gradient_by_group)
    weight_grad = product("tkgd,skd->kgts", gradient_by_group, value_slice)
    score_gradient = (
        weights_f
        * (weight_grad - row_delta[..., None])
        * (1.0 - (capped / SOFT_CAP) ** 2)
        * HEAD_SIZE ** (-0.5)
    )
    score_gradient = score_gradient.astype(BF)
    query_gradient = product("kgts,skd->tkgd", score_gradient, k_rot).reshape(
        token_rows, QUERY_HEADS, HEAD_SIZE
    )
    key_gradient = product(
        "maew,emaq->wmq",
        score_gradient,
        rotated_query.reshape(token_rows, KEY_VALUE_HEADS, heads_per_group, HEAD_SIZE),
    )
    query_gradient = rotate(query_gradient, cos_table, sin_table, -1.0)
    key_gradient = rotate(key_gradient, cos_table, sin_table, -1.0)
    return jnp.concatenate(
        [
            query_gradient.reshape(token_rows, QUERY_HEADS * HEAD_SIZE),
            key_gradient.reshape(token_rows, KEY_VALUE_HEADS * HEAD_SIZE),
            value_gradient.reshape(token_rows, KEY_VALUE_HEADS * HEAD_SIZE),
        ],
        axis=1,
    ).astype(BF)


def inverse_rms(values):
    return lax.rsqrt(jnp.mean(values * values, axis=1, keepdims=True) + EPSILON)


def norm_back(grad_rows, unit_rows, scale_rows, gain):
    scaled = grad_rows * gain
    return scale_rows * (scaled - unit_rows * jnp.mean(scaled * unit_rows, axis=1, keepdims=True))


def thirds(values):
    high = lax.reduce_precision(values, 8, 7)
    rest = values - high
    middle = lax.reduce_precision(rest, 8, 7)
    return jnp.concatenate([high, middle, rest - middle], axis=0).astype(BF)


def join_thirds(rows):
    count = rows.shape[-2] // 3
    rows = rows.astype(F32)
    return rows[..., :count, :] + rows[..., count : 2 * count, :] + rows[..., 2 * count :, :]


def to_whole_rows(values, nx, extra=None):
    width = values.shape[1]
    parts = values.astype(BF).reshape(nx, -1, width)
    if extra is not None:
        parts = jnp.concatenate(
            [parts, jnp.broadcast_to(extra[None], (nx,) + extra.shape)], axis=1
        )
    parts = lax.all_to_all(parts, "gx", split_axis=0, concat_axis=0, tiled=True)
    return parts.transpose(1, 0, 2).reshape(-1, nx * width)


def to_width_blocks(values, nx, extra=None):
    values = values.astype(BF)
    if extra is not None:
        values = jnp.concatenate([values, extra], axis=0)
    rows, whole = values.shape
    parts = values.reshape(rows, nx, whole // nx).transpose(1, 0, 2)
    return lax.all_to_all(parts, "gx", split_axis=0, concat_axis=0, tiled=True)


def flip(index, mask):
    return index + mask - 2 * mask * ((index // mask) % 2)


def flip_all(index, masks):
    bit = 1
    while bit <= masks:
        if masks & bit:
            index = flip(index, bit)
        bit *= 2
    return index


def greet(me, bits):
    barrier = pltpu.get_barrier_semaphore()
    for bit in bits:
        pl.semaphore_signal(barrier, inc=1, device_id={"gy": flip(me, bit)}, device_id_type=MESH)
    pl.semaphore_wait(barrier, len(bits))


def bit_orders(size):
    bits = []
    bit = 2
    while bit < size:
        bits.append(bit)
        bit *= 2
    return (bits + [1], bits[::-1] + [1])


def spread_kernel(size, own_ref, all_ref, local_sem, send_sem, recv_sem):
    me = lax.axis_index("gy")
    orders = bit_orders(size)
    half = own_ref.shape[0] // 2
    greet(me, orders[0])
    keep = pltpu.make_async_copy(own_ref, all_ref.at[me], local_sem)
    keep.start()
    copies = {}
    arrival = {}

    def copy(h, bit, r):
        n = len(copies)
        rows = pl.ds(h * half, half)
        where = flip_all(me, r)
        source = own_ref.at[rows] if r == 0 else all_ref.at[where, rows]
        made = pltpu.make_async_remote_copy(
            src_ref=source,
            dst_ref=all_ref.at[where, rows],
            send_sem=send_sem.at[n],
            recv_sem=recv_sem.at[n],
            device_id={"gy": flip(me, bit)},
            device_id_type=MESH,
        )
        copies[h, bit, r] = made
        arrival[h, r ^ bit] = made
        made.start()

    for step in range(len(orders[0])):
        for h in range(2):
            copy(h, orders[h][step], 0)
    landed = set()

    def land(h, r):
        if (h, r) not in landed:
            landed.add((h, r))
            arrival[h, r].wait_recv()

    held = [[0], [0]]
    for step in range(len(orders[0])):
        for h in range(2):
            bit = orders[h][step]
            for r in held[h]:
                if r:
                    land(h, r)
                    copy(h, bit, r)
        for h in range(2):
            held[h] = held[h] + [r ^ orders[h][step] for r in held[h]]
    for h in range(2):
        for r in range(1, size):
            land(h, r)
    for made in copies.values():
        made.wait_send()
    keep.wait()


def spread(values):
    size = lax.axis_size("gy")
    values = values.astype(BF)
    rows, width = values.shape
    count = 2 * (size - 1)
    out = pl.pallas_call(
        functools.partial(spread_kernel, size),
        out_shape=jax.ShapeDtypeStruct((size, rows, width), values.dtype),
        in_specs=[pl.BlockSpec(memory_space=pltpu.VMEM)],
        out_specs=pl.BlockSpec(memory_space=pltpu.VMEM),
        scratch_shapes=[
            pltpu.SemaphoreType.DMA,
            pltpu.SemaphoreType.DMA((count,)),
            pltpu.SemaphoreType.DMA((count,)),
        ],
        compiler_params=pltpu.CompilerParams(collective_id=0, has_side_effects=True, vmem_limit_bytes=32 << 20),
        cost_estimate=pl.CostEstimate(flops=0, bytes_accessed=size * rows * width * 16, transcendentals=0),
        name="spread",
    )(values)
    return out.reshape(size * rows, width)


def settle_kernel(size, parts_ref, sum_ref, came, kept, send_sem, recv_sem):
    me = lax.axis_index("gy")
    orders = tuple(order[::-1] for order in bit_orders(size))
    half = sum_ref.shape[0] // 2
    strip = 16
    greet(me, orders[0])
    slot = {}
    for h in range(2):
        held = list(range(size))
        for step, bit in enumerate(orders[h]):
            held = [r for r in held if not r & bit]
            for r in held:
                slot[h, step, r] = len(slot)
    copies = {}

    def view(h, step, r):
        if step == 0:
            return parts_ref.at[flip_all(me, r), pl.ds(h * half, half)]
        return kept.at[h, r]

    def send(h, step):
        bit = orders[h][step]
        gone = set()
        for b in orders[h][:step]:
            gone.add(b)
        for r in range(size):
            if r & bit and not any(r & b for b in gone):
                n = slot[h, step, r ^ bit]
                made = pltpu.make_async_remote_copy(
                    src_ref=view(h, step, r),
                    dst_ref=came.at[n],
                    send_sem=send_sem.at[n],
                    recv_sem=recv_sem.at[n],
                    device_id={"gy": flip(me, bit)},
                    device_id_type=MESH,
                )
                copies[h, step, r ^ bit] = made
                made.start()

    def gather(h, step, r, last):
        n = slot[h, step, r]
        copies[h, step, r].wait_recv()

        @pl.loop(0, half // strip)
        def _(i):
            rows = pl.ds(i * strip, strip)
            total = view(h, step, r)[rows].astype(F32) + came[n, rows].astype(F32)
            if last:
                sum_ref[pl.ds(h * half + i * strip, strip)] = total
            else:
                kept[h, r, rows] = total.astype(BF)

    steps = len(orders[0])
    for h in range(2):
        send(h, 0)
    for step in range(steps):
        for h in range(2):
            bits = orders[h][: step + 1]
            later = orders[h][step + 1] if step + 1 < steps else 0
            left = [r for r in range(size) if not any(r & b for b in bits)]
            for r in left:
                if r & later:
                    gather(h, step, r, False)
            if later:
                send(h, step + 1)
            for r in left:
                if not r & later:
                    gather(h, step, r, step == steps - 1)
    for made in copies.values():
        made.wait_send()


def settle(parts):
    size = lax.axis_size("gy")
    parts = parts.astype(BF)
    total, width = parts.shape
    rows = total // size
    count = 2 * (size - 1)
    return pl.pallas_call(
        functools.partial(settle_kernel, size),
        out_shape=jax.ShapeDtypeStruct((rows, width), F32),
        in_specs=[pl.BlockSpec(memory_space=pltpu.VMEM)],
        out_specs=pl.BlockSpec(memory_space=pltpu.VMEM),
        scratch_shapes=[
            pltpu.VMEM((count, rows // 2, width), BF),
            pltpu.VMEM((2, size, rows // 2, width), BF),
            pltpu.SemaphoreType.DMA((count,)),
            pltpu.SemaphoreType.DMA((count,)),
        ],
        compiler_params=pltpu.CompilerParams(collective_id=1, has_side_effects=True, vmem_limit_bytes=32 << 20),
        cost_estimate=pl.CostEstimate(flops=0, bytes_accessed=total * width * 16, transcendentals=0),
        name="settle",
    )(parts.reshape(size, rows, width))


def tally_kernel(size, own_ref, sum_ref, came, send_sem, recv_sem):
    me = lax.axis_index("gy")
    barrier = pltpu.get_barrier_semaphore()
    for d in range(1, size):
        pl.semaphore_signal(
            barrier, inc=1, device_id={"gy": (me + d) % size}, device_id_type=MESH
        )
    pl.semaphore_wait(barrier, size - 1)
    copies = []
    for d in range(1, size):
        made = pltpu.make_async_remote_copy(
            src_ref=own_ref,
            dst_ref=came.at[d],
            send_sem=send_sem.at[d],
            recv_sem=recv_sem.at[d],
            device_id={"gy": (me + d) % size},
            device_id_type=MESH,
        )
        made.start()
        copies.append(made)
    total = own_ref[...]
    for d in range(1, size):
        copies[d - 1].wait_recv()
        total = total + came[d]
    sum_ref[...] = total
    for made in copies:
        made.wait_send()


def tally(values, size, call):
    return pl.pallas_call(
        functools.partial(tally_kernel, size),
        out_shape=jax.ShapeDtypeStruct(values.shape, F32),
        in_specs=[pl.BlockSpec(memory_space=pltpu.VMEM)],
        out_specs=pl.BlockSpec(memory_space=pltpu.VMEM),
        scratch_shapes=[
            pltpu.VMEM((size,) + values.shape, F32),
            pltpu.SemaphoreType.DMA((size,)),
            pltpu.SemaphoreType.DMA((size,)),
        ],
        compiler_params=pltpu.CompilerParams(collective_id=call, has_side_effects=True),
        name="tally",
    )(values)


def make_shards(nx, ny):
    blocks = [((b // ny) * ny + b % ny, (b % nx) * ny + b // nx) for b in range(nx * ny)]

    def shards(
        inputs,
        segment_ids,
        qkv_weight,
        out_weight,
        gate_up_weight,
        down_weight,
        first_gain,
        second_gain,
        third_gain,
        fourth_gain,
        cotangent,
    ):
        width = inputs.shape[1]

        gains = thirds(jnp.stack([first_gain, second_gain, third_gain, fourth_gain]))
        rows_in = to_whole_rows(inputs, nx, gains)
        own = inputs.shape[0] // nx
        x_rows = rows_in[:own].astype(F32)
        gains = join_thirds(rows_in[own:])[:, None, :]
        qkv_w = lax.all_gather(qkv_weight, "gx", axis=0, tiled=True)
        out_w = lax.all_gather(out_weight, "gx", axis=1, tiled=True)
        gate_up_w = lax.all_gather(gate_up_weight, "gx", axis=0, tiled=True)
        down_w = lax.all_gather(down_weight, "gx", axis=1, tiled=True)
        cot_rows = to_whole_rows(cotangent, nx).astype(F32)

        segment_row = lax.ppermute(segment_ids[0], ("gx", "gy"), blocks)
        position, allowed = block_layout(segment_row)
        layout = (allowed,) + rope_tables(position)

        scale_one = inverse_rms(x_rows)
        unit_one = x_rows * scale_one
        normed_one = spread(unit_one * gains[0])
        rows = product("td,dc->tc", normed_one, qkv_w).astype(BF)
        rows = lax.all_to_all(rows, "gy", split_axis=0, concat_axis=1, tiled=True)
        mixing_rows, saved = attention_forward(rows, layout)
        mixed = lax.all_to_all(mixing_rows, "gy", split_axis=1, concat_axis=0, tiled=True)
        attn_branch = settle(product("tc,cd->td", mixed, out_w))
        scale_two = inverse_rms(attn_branch)
        unit_two = attn_branch * scale_two
        attn_term = unit_two * gains[1]
        middle = x_rows + attn_term
        scale_three = inverse_rms(middle)
        unit_three = middle * scale_three
        normed_two = spread(unit_three * gains[2])
        pre_gate = product("td,df->tf", normed_two, gate_up_w[:, 0, :])
        up_part = product("td,df->tf", normed_two, gate_up_w[:, 1, :])
        value, slope = gelu_parts(pre_gate)
        hidden = (value * up_part).astype(BF)
        ff_branch = settle(product("tf,fd->td", hidden, down_w))
        scale_four = inverse_rms(ff_branch)
        unit_four = ff_branch * scale_four
        ff_grad = spread(norm_back(cot_rows, unit_four, scale_four, gains[3]))
        delta = to_width_blocks(attn_term + unit_four * gains[3], nx)
        outputs = inputs + delta.reshape(inputs.shape).astype(F32)

        down_sum = product("tf,tkd->kfd", hidden, ff_grad.reshape(-1, nx, width)).astype(BF)
        down_sum, ff_grad = lax.optimization_barrier((down_sum, ff_grad))
        down_done = lax.psum_scatter(down_sum, "gx", scatter_dimension=0)
        hidden_grad = product("td,fd->tf", ff_grad, down_w)
        gate_grad = (hidden_grad * up_part * slope).astype(BF)
        up_grad = (hidden_grad * value).astype(BF)
        gate_up_sum = jnp.stack(
            [
                product("td,tf->df", normed_two, gate_grad).astype(BF),
                product("td,tf->df", normed_two, up_grad).astype(BF),
            ],
            axis=1,
        )
        gate_up_sum, gate_grad, up_grad = lax.optimization_barrier(
            (gate_up_sum, gate_grad, up_grad)
        )
        gate_up_done = lax.psum_scatter(gate_up_sum, "gx", scatter_dimension=0, tiled=True)
        normed_two_grad = settle(
            product("tf,df->td", gate_grad, gate_up_w[:, 0, :])
            + product("tf,df->td", up_grad, gate_up_w[:, 1, :])
        )
        middle_delta = norm_back(normed_two_grad, unit_three, scale_three, gains[2])
        middle_grad = cot_rows + middle_delta
        branch_grad = spread(norm_back(middle_grad, unit_two, scale_two, gains[1]))
        out_sum = product("tc,tkd->kcd", mixed, branch_grad.reshape(-1, nx, width)).astype(BF)
        out_sum, branch_grad = lax.optimization_barrier((out_sum, branch_grad))
        mixing_gradient = product("td,cd->tc", branch_grad, out_w).astype(BF)
        mixing_gradient = lax.all_to_all(
            mixing_gradient, "gy", split_axis=0, concat_axis=1, tiled=True
        )
        qkv_grad_rows = attention_backward(mixing_gradient, mixing_rows, saved, layout)
        qkv_grad_rows, down_done = lax.optimization_barrier((qkv_grad_rows, down_done))
        qkv_grad_rows = lax.all_to_all(
            qkv_grad_rows, "gy", split_axis=1, concat_axis=0, tiled=True
        )
        qkv_sum = product("td,tc->dc", normed_one, qkv_grad_rows).astype(BF)
        qkv_sum, qkv_grad_rows = lax.optimization_barrier((qkv_sum, qkv_grad_rows))
        normed_one_grad = settle(product("tc,dc->td", qkv_grad_rows, qkv_w))
        late_term = tally(jnp.sum(normed_one_grad * unit_one, axis=0, keepdims=True), ny, 2)
        early_terms = tally(
            jnp.stack(
                [
                    jnp.sum(middle_grad * unit_two, axis=0),
                    jnp.sum(normed_two_grad * unit_three, axis=0),
                    jnp.sum(cot_rows * unit_four, axis=0),
                ]
            ),
            ny,
            3,
        )
        delta = to_width_blocks(
            middle_delta + norm_back(normed_one_grad, unit_one, scale_one, gains[0]),
            nx,
            thirds(jnp.concatenate([late_term, early_terms], axis=0)),
        )
        input_grad = cotangent + delta[:, :own].reshape(inputs.shape).astype(F32)
        terms = jnp.sum(join_thirds(delta[:, own:]), axis=0)
        gate_up_done, out_sum, qkv_sum = lax.optimization_barrier((gate_up_done, out_sum, qkv_sum))
        out_grad = lax.psum_scatter(out_sum, "gx", scatter_dimension=0).astype(F32)
        qkv_grad = lax.psum_scatter(qkv_sum, "gx", scatter_dimension=0, tiled=True).astype(F32)
        gate_up_grad, down_grad = gate_up_done.astype(F32), down_done.astype(F32)
        return (outputs, input_grad, qkv_grad, out_grad, gate_up_grad, down_grad) + tuple(
            terms[i] for i in range(4)
        )

    return shards


def solution(mesh):
    placed = (
        P("gy", "gx"),
        P(("gx", "gy"), None),
        P("gx", "gy"),
        P("gy", "gx"),
        P("gx", None, "gy"),
        P("gy", "gx"),
        P("gx"),
        P("gx"),
        P("gx"),
        P("gx"),
        P("gy", "gx"),
    )
    return jax.shard_map(
        make_shards(mesh.shape["gx"], mesh.shape["gy"]),
        mesh=mesh,
        in_specs=placed,
        out_specs=(
            P("gy", "gx"),
            P("gy", "gx"),
            P("gx", "gy"),
            P("gy", "gx"),
            P("gx", None, "gy"),
            P("gy", "gx"),
            P("gx"),
            P("gx"),
            P("gx"),
            P("gx"),
        ),
        check_vma=False,
    )
```

```python
import functools
import math

import jax
import jax.numpy as jnp
from jax import lax
from jax.experimental import pallas as pl
from jax.experimental.pallas import tpu as pltpu
from jax.sharding import PartitionSpec as P

QUERY_HEADS = 8
KEY_VALUE_HEADS = 4
HEAD_SIZE = 256


EPSILON = 1e-06
SOFT_CAP = 50.0
GELU_COEF = 0.7978845608028654
CUBIC_COEF = 0.044715

BF = jnp.bfloat16
F32 = jnp.float32
MESH = pl.DeviceIdType.MESH


def product(form, left, right):
    return jnp.einsum(form, left, right, preferred_element_type=F32)


def gelu_parts(pre_gate):
    inner_arg = GELU_COEF * (pre_gate + CUBIC_COEF * pre_gate * pre_gate * pre_gate)
    tanh_value = jnp.tanh(inner_arg)
    activated = 0.5 * pre_gate * (1.0 + tanh_value)
    derivative = 0.5 * (1.0 + tanh_value) + 0.5 * pre_gate * (
        1.0 - tanh_value * tanh_value
    ) * GELU_COEF * (1.0 + 3.0 * CUBIC_COEF * pre_gate * pre_gate)
    return (activated, derivative)


def block_layout(segment_row):
    length_total = segment_row.shape[0]
    places = jnp.arange(length_total, dtype=jnp.int32)
    same_doc = segment_row[:, None] == segment_row[None, :]
    starts = jnp.min(jnp.where(same_doc, places[None, :], length_total), axis=1)
    allowed = jnp.logical_and(same_doc, places[None, :] <= places[:, None])
    return (places - starts, allowed)


def rope_tables(position):
    half_dim = HEAD_SIZE // 2
    freq_steps = jnp.arange(half_dim, dtype=F32)
    frequency = jnp.exp(freq_steps * (-2.0 * math.log(10000.0) / HEAD_SIZE))
    angles = position.astype(F32)[:, None] * frequency[None, :]
    return (jnp.cos(angles)[:, None, :], jnp.sin(angles)[:, None, :])


def rotate(values, cos_table, sin_table, direction):
    half_dim = values.shape[-1] // 2
    leading = values[..., :half_dim]
    trailing = values[..., half_dim:]
    return jnp.concatenate(
        [
            leading * cos_table - direction * trailing * sin_table,
            trailing * cos_table + direction * leading * sin_table,
        ],
        axis=-1,
    )


def capped_scores(rotated_query, k_rot):
    token_rows = rotated_query.shape[0]
    query_groups = rotated_query.reshape(
        token_rows, KEY_VALUE_HEADS, QUERY_HEADS // KEY_VALUE_HEADS, HEAD_SIZE
    )
    raw_scores = product("tkgd,skd->kgts", query_groups, k_rot) * HEAD_SIZE ** (-0.5)
    return SOFT_CAP * jnp.tanh(raw_scores / SOFT_CAP)


def attention_forward(rows, layout):
    token_rows = rows.shape[0]
    query_span_width = QUERY_HEADS * HEAD_SIZE
    key_value_width = KEY_VALUE_HEADS * HEAD_SIZE
    allowed, cos_table, sin_table = layout
    query_part = (
        rows[:, :query_span_width].astype(F32).reshape(token_rows, QUERY_HEADS, HEAD_SIZE)
    )
    key_slice = (
        rows[:, query_span_width : query_span_width + key_value_width]
        .astype(F32)
        .reshape(token_rows, KEY_VALUE_HEADS, HEAD_SIZE)
    )
    value_slice = rows[:, query_span_width + key_value_width :].reshape(
        token_rows, KEY_VALUE_HEADS, HEAD_SIZE
    )
    rotated_query = rotate(query_part, cos_table, sin_table, 1.0).astype(BF)
    k_rot = rotate(key_slice, cos_table, sin_table, 1.0).astype(BF)
    capped = capped_scores(rotated_query, k_rot)
    log_total = jnp.log(jnp.sum(jnp.where(allowed, jnp.exp(capped), 0.0), axis=-1))
    weights_f = jnp.where(allowed, jnp.exp(capped - log_total[..., None]), 0.0)
    mixing_rows = product("kgts,skd->tkgd", weights_f.astype(BF), value_slice)
    mixing_rows = mixing_rows.astype(BF).reshape(token_rows, query_span_width)
    return (mixing_rows, (rotated_query, k_rot, value_slice, log_total))


def attention_backward(mixing_gradient, mixing_rows, saved, layout):
    rotated_query, k_rot, value_slice, log_total = saved
    token_rows = mixing_gradient.shape[0]
    heads_per_group = QUERY_HEADS // KEY_VALUE_HEADS
    allowed, cos_table, sin_table = layout
    capped = capped_scores(rotated_query, k_rot)
    weights_f = jnp.where(allowed, jnp.exp(capped - log_total[..., None]), 0.0)
    gradient_by_group = mixing_gradient.reshape(
        token_rows, KEY_VALUE_HEADS, heads_per_group, HEAD_SIZE
    )
    output_by_group = mixing_rows.reshape(token_rows, KEY_VALUE_HEADS, heads_per_group, HEAD_SIZE)
    row_delta = product("tkgd,tkgd->kgt", gradient_by_group, output_by_group)
    value_gradient = product("maew,emaq->wmq", weights_f.astype(BF), gradient_by_group)
    weight_grad = product("tkgd,skd->kgts", gradient_by_group, value_slice)
    score_gradient = (
        weights_f
        * (weight_grad - row_delta[..., None])
        * (1.0 - (capped / SOFT_CAP) ** 2)
        * HEAD_SIZE ** (-0.5)
    )
    score_gradient = score_gradient.astype(BF)
    query_gradient = product("kgts,skd->tkgd", score_gradient, k_rot).reshape(
        token_rows, QUERY_HEADS, HEAD_SIZE
    )
    key_gradient = product(
        "maew,emaq->wmq",
        score_gradient,
        rotated_query.reshape(token_rows, KEY_VALUE_HEADS, heads_per_group, HEAD_SIZE),
    )
    query_gradient = rotate(query_gradient, cos_table, sin_table, -1.0)
    key_gradient = rotate(key_gradient, cos_table, sin_table, -1.0)
    return jnp.concatenate(
        [
            query_gradient.reshape(token_rows, QUERY_HEADS * HEAD_SIZE),
            key_gradient.reshape(token_rows, KEY_VALUE_HEADS * HEAD_SIZE),
            value_gradient.reshape(token_rows, KEY_VALUE_HEADS * HEAD_SIZE),
        ],
        axis=1,
    ).astype(BF)


def inverse_rms(values):
    return lax.rsqrt(jnp.mean(values * values, axis=1, keepdims=True) + EPSILON)


def norm_back(grad_rows, unit_rows, scale_rows, gain):
    scaled = grad_rows * gain
    return scale_rows * (scaled - unit_rows * jnp.mean(scaled * unit_rows, axis=1, keepdims=True))


def thirds(values):
    high = lax.reduce_precision(values, 8, 7)
    rest = values - high
    middle = lax.reduce_precision(rest, 8, 7)
    return jnp.concatenate([high, middle, rest - middle], axis=0).astype(BF)


def join_thirds(rows):
    count = rows.shape[-2] // 3
    rows = rows.astype(F32)
    return rows[..., :count, :] + rows[..., count : 2 * count, :] + rows[..., 2 * count :, :]


def to_whole_rows(values, nx, extra=None):
    width = values.shape[1]
    parts = values.astype(BF).reshape(nx, -1, width)
    if extra is not None:
        parts = jnp.concatenate(
            [parts, jnp.broadcast_to(extra[None], (nx,) + extra.shape)], axis=1
        )
    parts = lax.all_to_all(parts, "gx", split_axis=0, concat_axis=0, tiled=True)
    return parts.transpose(1, 0, 2).reshape(-1, nx * width)


def to_width_blocks(values, nx, extra=None):
    values = values.astype(BF)
    if extra is not None:
        values = jnp.concatenate([values, extra], axis=0)
    rows, whole = values.shape
    parts = values.reshape(rows, nx, whole // nx).transpose(1, 0, 2)
    return lax.all_to_all(parts, "gx", split_axis=0, concat_axis=0, tiled=True)


def flip(index, mask):
    return index + mask - 2 * mask * ((index // mask) % 2)


def flip_all(index, masks):
    bit = 1
    while bit <= masks:
        if masks & bit:
            index = flip(index, bit)
        bit *= 2
    return index


def greet(me, bits, lanes=0):
    barrier = pltpu.get_barrier_semaphore()
    for bit in bits:
        pl.semaphore_signal(barrier, inc=1, device_id={"gy": flip(me, bit)}, device_id_type=MESH)
    for d in range(1, lanes):
        other = (lax.axis_index("gx") + d) % lanes
        pl.semaphore_signal(barrier, inc=1, device_id={"gx": other}, device_id_type=MESH)
    pl.semaphore_wait(barrier, len(bits) + max(lanes - 1, 0))


def bit_orders(size):
    bits = []
    bit = 2
    while bit < size:
        bits.append(bit)
        bit *= 2
    return (bits + [1], bits[::-1] + [1])


def swap_start(lanes, side_ref, there_ref, sems):
    me = lax.axis_index("gx")
    own, send_sem, recv_sem = sems
    made = [pltpu.make_async_copy(side_ref.at[me], there_ref.at[me], own)]
    for d in range(1, lanes):
        other = (me + d) % lanes
        made.append(
            pltpu.make_async_remote_copy(
                src_ref=side_ref.at[other],
                dst_ref=there_ref.at[me],
                send_sem=send_sem.at[d],
                recv_sem=recv_sem.at[d],
                device_id={"gx": other},
                device_id_type=MESH,
            )
        )
    for copy in made:
        copy.start()
    return made


def swap_sems(lanes):
    return [
        pltpu.SemaphoreType.DMA,
        pltpu.SemaphoreType.DMA((lanes,)),
        pltpu.SemaphoreType.DMA((lanes,)),
    ]


def spread_kernel(size, lanes, *refs):
    if lanes:
        own_ref, side_ref, all_ref, there_ref, local_sem, send_sem, recv_sem, *sems = refs
    else:
        own_ref, all_ref, local_sem, send_sem, recv_sem = refs
    me = lax.axis_index("gy")
    orders = bit_orders(size)
    half = own_ref.shape[0] // 2
    greet(me, orders[0], lanes)
    swapped = swap_start(lanes, side_ref, there_ref, sems) if lanes else []
    keep = pltpu.make_async_copy(own_ref, all_ref.at[me], local_sem)
    keep.start()
    copies = {}
    arrival = {}

    def copy(h, bit, r):
        n = len(copies)
        rows = pl.ds(h * half, half)
        where = flip_all(me, r)
        source = own_ref.at[rows] if r == 0 else all_ref.at[where, rows]
        made = pltpu.make_async_remote_copy(
            src_ref=source,
            dst_ref=all_ref.at[where, rows],
            send_sem=send_sem.at[n],
            recv_sem=recv_sem.at[n],
            device_id={"gy": flip(me, bit)},
            device_id_type=MESH,
        )
        copies[h, bit, r] = made
        arrival[h, r ^ bit] = made
        made.start()

    for step in range(len(orders[0])):
        for h in range(2):
            copy(h, orders[h][step], 0)
    landed = set()

    def land(h, r):
        if (h, r) not in landed:
            landed.add((h, r))
            arrival[h, r].wait_recv()

    held = [[0], [0]]
    for step in range(len(orders[0])):
        for h in range(2):
            bit = orders[h][step]
            for r in held[h]:
                if r:
                    land(h, r)
                    copy(h, bit, r)
        for h in range(2):
            held[h] = held[h] + [r ^ orders[h][step] for r in held[h]]
    for h in range(2):
        for r in range(1, size):
            land(h, r)
    for made in copies.values():
        made.wait_send()
    for copy in [keep] + swapped:
        copy.wait()


def spread(values, side=None):
    size = lax.axis_size("gy")
    values = values.astype(BF)
    rows, width = values.shape
    count = 2 * (size - 1)
    sides = [] if side is None else [side]
    lanes = 0 if side is None else side.shape[0]
    space = pl.BlockSpec(memory_space=pltpu.VMEM)
    out = pl.pallas_call(
        functools.partial(spread_kernel, size, lanes),
        out_shape=[jax.ShapeDtypeStruct((size, rows, width), values.dtype)]
        + [jax.ShapeDtypeStruct(v.shape, v.dtype) for v in sides],
        in_specs=[space] * (1 + len(sides)),
        out_specs=[space] * (1 + len(sides)),
        scratch_shapes=[
            pltpu.SemaphoreType.DMA,
            pltpu.SemaphoreType.DMA((count,)),
            pltpu.SemaphoreType.DMA((count,)),
        ]
        + (swap_sems(lanes) if lanes else []),
        compiler_params=pltpu.CompilerParams(
            collective_id=4 if lanes else 0, has_side_effects=True, vmem_limit_bytes=32 << 20
        ),
        cost_estimate=pl.CostEstimate(
            flops=0, bytes_accessed=size * rows * width * 16, transcendentals=0
        ),
        name="spread",
    )(values, *sides)
    whole = out[0].reshape(size * rows, width)
    return (whole, out[1]) if lanes else whole


def settle_kernel(size, lanes, *refs):
    if lanes:
        parts_ref, side_ref, sum_ref, there_ref, came, kept, send_sem, recv_sem, *sems = refs
    else:
        parts_ref, sum_ref, came, kept, send_sem, recv_sem = refs
    me = lax.axis_index("gy")
    orders = tuple(order[::-1] for order in bit_orders(size))
    half = sum_ref.shape[0] // 2
    strip = 16
    greet(me, orders[0], lanes)
    swapped = swap_start(lanes, side_ref, there_ref, sems) if lanes else []
    slot = {}
    for h in range(2):
        held = list(range(size))
        for step, bit in enumerate(orders[h]):
            held = [r for r in held if not r & bit]
            for r in held:
                slot[h, step, r] = len(slot)
    copies = {}

    def view(h, step, r):
        if step == 0:
            return parts_ref.at[flip_all(me, r), pl.ds(h * half, half)]
        return kept.at[h, r]

    def send(h, step):
        bit = orders[h][step]
        gone = set()
        for b in orders[h][:step]:
            gone.add(b)
        for r in range(size):
            if r & bit and not any(r & b for b in gone):
                n = slot[h, step, r ^ bit]
                made = pltpu.make_async_remote_copy(
                    src_ref=view(h, step, r),
                    dst_ref=came.at[n],
                    send_sem=send_sem.at[n],
                    recv_sem=recv_sem.at[n],
                    device_id={"gy": flip(me, bit)},
                    device_id_type=MESH,
                )
                copies[h, step, r ^ bit] = made
                made.start()

    def gather(h, step, r, last):
        n = slot[h, step, r]
        copies[h, step, r].wait_recv()

        @pl.loop(0, half // strip)
        def _(i):
            rows = pl.ds(i * strip, strip)
            total = view(h, step, r)[rows].astype(F32) + came[n, rows].astype(F32)
            if last:
                sum_ref[pl.ds(h * half + i * strip, strip)] = total
            else:
                kept[h, r, rows] = total.astype(BF)

    steps = len(orders[0])
    for h in range(2):
        send(h, 0)
    for step in range(steps):
        for h in range(2):
            bits = orders[h][: step + 1]
            later = orders[h][step + 1] if step + 1 < steps else 0
            left = [r for r in range(size) if not any(r & b for b in bits)]
            for r in left:
                if r & later:
                    gather(h, step, r, False)
            if later:
                send(h, step + 1)
            for r in left:
                if not r & later:
                    gather(h, step, r, step == steps - 1)
    for made in copies.values():
        made.wait_send()
    for copy in swapped:
        copy.wait()


def settle(parts, side=None):
    size = lax.axis_size("gy")
    parts = parts.astype(BF)
    total, width = parts.shape
    rows = total // size
    count = 2 * (size - 1)
    sides = [] if side is None else [side]
    lanes = 0 if side is None else side.shape[0]
    space = pl.BlockSpec(memory_space=pltpu.VMEM)
    out = pl.pallas_call(
        functools.partial(settle_kernel, size, lanes),
        out_shape=[jax.ShapeDtypeStruct((rows, width), F32)]
        + [jax.ShapeDtypeStruct(v.shape, v.dtype) for v in sides],
        in_specs=[space] * (1 + len(sides)),
        out_specs=[space] * (1 + len(sides)),
        scratch_shapes=[
            pltpu.VMEM((count, rows // 2, width), BF),
            pltpu.VMEM((2, size, rows // 2, width), BF),
            pltpu.SemaphoreType.DMA((count,)),
            pltpu.SemaphoreType.DMA((count,)),
        ]
        + (swap_sems(lanes) if lanes else []),
        compiler_params=pltpu.CompilerParams(
            collective_id=5 if lanes else 1, has_side_effects=True, vmem_limit_bytes=32 << 20
        ),
        cost_estimate=pl.CostEstimate(
            flops=0, bytes_accessed=total * width * 16, transcendentals=0
        ),
        name="settle",
    )(parts.reshape(size, rows, width), *sides)
    return out if lanes else out[0]


def tally_kernel(size, own_ref, sum_ref, came, send_sem, recv_sem):
    me = lax.axis_index("gy")
    barrier = pltpu.get_barrier_semaphore()
    for d in range(1, size):
        pl.semaphore_signal(
            barrier, inc=1, device_id={"gy": (me + d) % size}, device_id_type=MESH
        )
    pl.semaphore_wait(barrier, size - 1)
    copies = []
    for d in range(1, size):
        made = pltpu.make_async_remote_copy(
            src_ref=own_ref,
            dst_ref=came.at[d],
            send_sem=send_sem.at[d],
            recv_sem=recv_sem.at[d],
            device_id={"gy": (me + d) % size},
            device_id_type=MESH,
        )
        made.start()
        copies.append(made)
    total = own_ref[...]
    for d in range(1, size):
        copies[d - 1].wait_recv()
        total = total + came[d]
    sum_ref[...] = total
    for made in copies:
        made.wait_send()


def tally(values, size):
    return pl.pallas_call(
        functools.partial(tally_kernel, size),
        out_shape=jax.ShapeDtypeStruct(values.shape, F32),
        in_specs=[pl.BlockSpec(memory_space=pltpu.VMEM)],
        out_specs=pl.BlockSpec(memory_space=pltpu.VMEM),
        scratch_shapes=[
            pltpu.VMEM((size,) + values.shape, F32),
            pltpu.SemaphoreType.DMA((size,)),
            pltpu.SemaphoreType.DMA((size,)),
        ],
        compiler_params=pltpu.CompilerParams(collective_id=2, has_side_effects=True),
        name="tally",
    )(values)


def make_shards(nx, ny):
    blocks = [((b // ny) * ny + b % ny, (b % nx) * ny + b // nx) for b in range(nx * ny)]

    def shards(
        inputs,
        segment_ids,
        qkv_weight,
        out_weight,
        gate_up_weight,
        down_weight,
        first_gain,
        second_gain,
        third_gain,
        fourth_gain,
        cotangent,
    ):
        width = inputs.shape[1]

        gains = thirds(jnp.stack([first_gain, second_gain, third_gain, fourth_gain]))
        rows_in = to_whole_rows(inputs, nx, gains)
        own = inputs.shape[0] // nx
        heads = qkv_weight.shape[1]
        x_rows = rows_in[:own].astype(F32)
        gains = join_thirds(rows_in[own:])[:, None, :]
        both_w = lax.all_gather(
            jnp.concatenate([qkv_weight, out_weight.T], axis=1), "gx", axis=0, tiled=True
        )
        gate_up_w = lax.all_gather(gate_up_weight, "gx", axis=0, tiled=True)
        down_w = lax.all_gather(down_weight.T, "gx", axis=0, tiled=True)
        qkv_w, out_w = both_w[:, :heads], both_w[:, heads:]

        segment_row = lax.ppermute(segment_ids[0], ("gx", "gy"), blocks)
        position, allowed = block_layout(segment_row)
        layout = (allowed,) + rope_tables(position)

        scale_one = inverse_rms(x_rows)
        unit_one = x_rows * scale_one
        normed_one = spread(unit_one * gains[0])
        rows = product("td,dc->tc", normed_one, qkv_w).astype(BF)
        rows = lax.all_to_all(rows, "gy", split_axis=0, concat_axis=1, tiled=True)
        mixing_rows, saved = attention_forward(rows, layout)
        mixed = lax.all_to_all(mixing_rows, "gy", split_axis=1, concat_axis=0, tiled=True)
        attn_branch = settle(product("tc,dc->td", mixed, out_w))
        scale_two = inverse_rms(attn_branch)
        unit_two = attn_branch * scale_two
        attn_term = unit_two * gains[1]
        middle = x_rows + attn_term
        scale_three = inverse_rms(middle)
        unit_three = middle * scale_three
        normed_two = spread(unit_three * gains[2])
        pre_gate = product("td,df->tf", normed_two, gate_up_w[:, 0, :])
        up_part = product("td,df->tf", normed_two, gate_up_w[:, 1, :])
        value, slope = gelu_parts(pre_gate)
        hidden = (value * up_part).astype(BF)
        ff_branch, cot_parts = settle(
            product("tf,df->td", hidden, down_w), cotangent.astype(BF).reshape(nx, own, width)
        )
        cot_rows = cot_parts.transpose(1, 0, 2).reshape(own, nx * width).astype(F32)
        scale_four = inverse_rms(ff_branch)
        unit_four = ff_branch * scale_four
        delta = (attn_term + unit_four * gains[3]).astype(BF)
        ff_grad, delta = spread(
            norm_back(cot_rows, unit_four, scale_four, gains[3]),
            delta.reshape(own, nx, width).transpose(1, 0, 2),
        )
        outputs = inputs + delta.reshape(inputs.shape).astype(F32)

        down_sum = product("td,tf->df", ff_grad, hidden).astype(BF)
        down_sum, ff_grad = lax.optimization_barrier((down_sum, ff_grad))
        down_done = lax.psum_scatter(down_sum, "gx", scatter_dimension=0, tiled=True)
        hidden_grad = product("td,df->tf", ff_grad, down_w)
        gate_grad = (hidden_grad * up_part * slope).astype(BF)
        up_grad = (hidden_grad * value).astype(BF)
        gate_up_sum = jnp.stack(
            [
                product("td,tf->df", normed_two, gate_grad).astype(BF),
                product("td,tf->df", normed_two, up_grad).astype(BF),
            ],
            axis=1,
        )
        gate_up_sum, gate_grad, up_grad = lax.optimization_barrier(
            (gate_up_sum, gate_grad, up_grad)
        )
        gate_up_done = lax.psum_scatter(gate_up_sum, "gx", scatter_dimension=0, tiled=True)
        normed_two_grad = settle(
            product("tf,df->td", gate_grad, gate_up_w[:, 0, :])
            + product("tf,df->td", up_grad, gate_up_w[:, 1, :])
        )
        middle_delta = norm_back(normed_two_grad, unit_three, scale_three, gains[2])
        middle_grad = cot_rows + middle_delta
        branch_grad = spread(norm_back(middle_grad, unit_two, scale_two, gains[1]))
        out_sum = product("td,tc->dc", branch_grad, mixed).astype(BF)
        mixing_gradient = product("td,dc->tc", branch_grad, out_w).astype(BF)
        mixing_gradient = lax.all_to_all(
            mixing_gradient, "gy", split_axis=0, concat_axis=1, tiled=True
        )
        qkv_grad_rows = attention_backward(mixing_gradient, mixing_rows, saved, layout)
        qkv_grad_rows, down_done = lax.optimization_barrier((qkv_grad_rows, down_done))
        qkv_grad_rows = lax.all_to_all(
            qkv_grad_rows, "gy", split_axis=1, concat_axis=0, tiled=True
        )
        normed_one_grad = settle(product("tc,dc->td", qkv_grad_rows, qkv_w))
        both_sum = jnp.concatenate(
            [product("td,tc->dc", normed_one, qkv_grad_rows).astype(BF), out_sum], axis=1
        )
        terms = jnp.stack(
            [
                jnp.sum(normed_one_grad * unit_one, axis=0),
                jnp.sum(middle_grad * unit_two, axis=0),
                jnp.sum(normed_two_grad * unit_three, axis=0),
                jnp.sum(cot_rows * unit_four, axis=0),
            ]
        )
        delta = to_width_blocks(
            middle_delta + norm_back(normed_one_grad, unit_one, scale_one, gains[0]),
            nx,
            thirds(tally(terms, ny)),
        )
        down_grad = down_done.astype(F32).T
        gate_up_done, both_sum, delta, down_grad = lax.optimization_barrier(
            (gate_up_done, both_sum, delta, down_grad)
        )
        both_done = lax.psum_scatter(both_sum, "gx", scatter_dimension=0, tiled=True)
        gate_up_grad = gate_up_done.astype(F32)
        input_grad = cotangent + delta[:, :own].reshape(inputs.shape).astype(F32)
        terms = jnp.sum(join_thirds(delta[:, own:]), axis=0)
        qkv_grad = both_done[:, :heads].astype(F32)
        out_grad = both_done[:, heads:].astype(F32).T
        return (outputs, input_grad, qkv_grad, out_grad, gate_up_grad, down_grad) + tuple(
            terms[i] for i in range(4)
        )

    return shards


def solution(mesh):
    placed = (
        P("gy", "gx"),
        P(("gx", "gy"), None),
        P("gx", "gy"),
        P("gy", "gx"),
        P("gx", None, "gy"),
        P("gy", "gx"),
        P("gx"),
        P("gx"),
        P("gx"),
        P("gx"),
        P("gy", "gx"),
    )
    return jax.shard_map(
        make_shards(mesh.shape["gx"], mesh.shape["gy"]),
        mesh=mesh,
        in_specs=placed,
        out_specs=(
            P("gy", "gx"),
            P("gy", "gx"),
            P("gx", "gy"),
            P("gy", "gx"),
            P("gx", None, "gy"),
            P("gy", "gx"),
            P("gx"),
            P("gx"),
            P("gx"),
            P("gx"),
        ),
        check_vma=False,
    )
```

```python
import functools
import math

import jax
import jax.numpy as jnp
from jax import lax
from jax.experimental import pallas as pl
from jax.experimental.pallas import tpu as pltpu
from jax.sharding import PartitionSpec as P

QUERY_HEADS = 8
KEY_VALUE_HEADS = 4
HEAD_SIZE = 256


EPSILON = 1e-06
SOFT_CAP = 50.0
GELU_COEF = 0.7978845608028654
CUBIC_COEF = 0.044715

BF = jnp.bfloat16
F32 = jnp.float32
MESH = pl.DeviceIdType.MESH


def product(form, left, right):
    return jnp.einsum(form, left, right, preferred_element_type=F32)


def gelu_parts(pre_gate):
    inner_arg = GELU_COEF * (pre_gate + CUBIC_COEF * pre_gate * pre_gate * pre_gate)
    tanh_value = jnp.tanh(inner_arg)
    activated = 0.5 * pre_gate * (1.0 + tanh_value)
    derivative = 0.5 * (1.0 + tanh_value) + 0.5 * pre_gate * (
        1.0 - tanh_value * tanh_value
    ) * GELU_COEF * (1.0 + 3.0 * CUBIC_COEF * pre_gate * pre_gate)
    return (activated, derivative)


def block_layout(segment_row):
    length_total = segment_row.shape[0]
    places = jnp.arange(length_total, dtype=jnp.int32)
    same_doc = segment_row[:, None] == segment_row[None, :]
    starts = jnp.min(jnp.where(same_doc, places[None, :], length_total), axis=1)
    allowed = jnp.logical_and(same_doc, places[None, :] <= places[:, None])
    return (places - starts, allowed)


def rope_tables(position):
    half_dim = HEAD_SIZE // 2
    freq_steps = jnp.arange(half_dim, dtype=F32)
    frequency = jnp.exp(freq_steps * (-2.0 * math.log(10000.0) / HEAD_SIZE))
    angles = position.astype(F32)[:, None] * frequency[None, :]
    return (jnp.cos(angles)[:, None, :], jnp.sin(angles)[:, None, :])


def rotate(values, cos_table, sin_table, direction):
    half_dim = values.shape[-1] // 2
    leading = values[..., :half_dim]
    trailing = values[..., half_dim:]
    return jnp.concatenate(
        [
            leading * cos_table - direction * trailing * sin_table,
            trailing * cos_table + direction * leading * sin_table,
        ],
        axis=-1,
    )


def capped_scores(rotated_query, k_rot):
    token_rows = rotated_query.shape[0]
    query_groups = rotated_query.reshape(
        token_rows, KEY_VALUE_HEADS, QUERY_HEADS // KEY_VALUE_HEADS, HEAD_SIZE
    )
    raw_scores = product("tkgd,skd->kgts", query_groups, k_rot) * HEAD_SIZE ** (-0.5)
    return SOFT_CAP * jnp.tanh(raw_scores / SOFT_CAP)


def attention_forward(rows, layout):
    token_rows = rows.shape[0]
    query_span_width = QUERY_HEADS * HEAD_SIZE
    key_value_width = KEY_VALUE_HEADS * HEAD_SIZE
    allowed, cos_table, sin_table = layout
    query_part = (
        rows[:, :query_span_width].astype(F32).reshape(token_rows, QUERY_HEADS, HEAD_SIZE)
    )
    key_slice = (
        rows[:, query_span_width : query_span_width + key_value_width]
        .astype(F32)
        .reshape(token_rows, KEY_VALUE_HEADS, HEAD_SIZE)
    )
    value_slice = rows[:, query_span_width + key_value_width :].reshape(
        token_rows, KEY_VALUE_HEADS, HEAD_SIZE
    )
    rotated_query = rotate(query_part, cos_table, sin_table, 1.0).astype(BF)
    k_rot = rotate(key_slice, cos_table, sin_table, 1.0).astype(BF)
    capped = capped_scores(rotated_query, k_rot)
    log_total = jnp.log(jnp.sum(jnp.where(allowed, jnp.exp(capped), 0.0), axis=-1))
    weights_f = jnp.where(allowed, jnp.exp(capped - log_total[..., None]), 0.0)
    mixing_rows = product("kgts,skd->tkgd", weights_f.astype(BF), value_slice)
    mixing_rows = mixing_rows.astype(BF).reshape(token_rows, query_span_width)
    return (mixing_rows, (rotated_query, k_rot, value_slice, log_total))


def attention_backward(mixing_gradient, mixing_rows, saved, layout):
    rotated_query, k_rot, value_slice, log_total = saved
    token_rows = mixing_gradient.shape[0]
    heads_per_group = QUERY_HEADS // KEY_VALUE_HEADS
    allowed, cos_table, sin_table = layout
    capped = capped_scores(rotated_query, k_rot)
    weights_f = jnp.where(allowed, jnp.exp(capped - log_total[..., None]), 0.0)
    gradient_by_group = mixing_gradient.reshape(
        token_rows, KEY_VALUE_HEADS, heads_per_group, HEAD_SIZE
    )
    output_by_group = mixing_rows.reshape(token_rows, KEY_VALUE_HEADS, heads_per_group, HEAD_SIZE)
    row_delta = product("tkgd,tkgd->kgt", gradient_by_group, output_by_group)
    value_gradient = product("maew,emaq->wmq", weights_f.astype(BF), gradient_by_group)
    weight_grad = product("tkgd,skd->kgts", gradient_by_group, value_slice)
    score_gradient = (
        weights_f
        * (weight_grad - row_delta[..., None])
        * (1.0 - (capped / SOFT_CAP) ** 2)
        * HEAD_SIZE ** (-0.5)
    )
    score_gradient = score_gradient.astype(BF)
    query_gradient = product("kgts,skd->tkgd", score_gradient, k_rot).reshape(
        token_rows, QUERY_HEADS, HEAD_SIZE
    )
    key_gradient = product(
        "maew,emaq->wmq",
        score_gradient,
        rotated_query.reshape(token_rows, KEY_VALUE_HEADS, heads_per_group, HEAD_SIZE),
    )
    query_gradient = rotate(query_gradient, cos_table, sin_table, -1.0)
    key_gradient = rotate(key_gradient, cos_table, sin_table, -1.0)
    return jnp.concatenate(
        [
            query_gradient.reshape(token_rows, QUERY_HEADS * HEAD_SIZE),
            key_gradient.reshape(token_rows, KEY_VALUE_HEADS * HEAD_SIZE),
            value_gradient.reshape(token_rows, KEY_VALUE_HEADS * HEAD_SIZE),
        ],
        axis=1,
    ).astype(BF)


def inverse_rms(values):
    return lax.rsqrt(jnp.mean(values * values, axis=1, keepdims=True) + EPSILON)


def norm_back(grad_rows, unit_rows, scale_rows, gain):
    scaled = grad_rows * gain
    return scale_rows * (scaled - unit_rows * jnp.mean(scaled * unit_rows, axis=1, keepdims=True))


def thirds(values):
    high = lax.reduce_precision(values, 8, 7)
    rest = values - high
    middle = lax.reduce_precision(rest, 8, 7)
    return jnp.concatenate([high, middle, rest - middle], axis=0).astype(BF)


def join_thirds(rows):
    count = rows.shape[-2] // 3
    rows = rows.astype(F32)
    return rows[..., :count, :] + rows[..., count : 2 * count, :] + rows[..., 2 * count :, :]


def to_whole_rows(values, nx, extra=None):
    width = values.shape[1]
    parts = values.astype(BF).reshape(nx, -1, width)
    if extra is not None:
        parts = jnp.concatenate(
            [parts, jnp.broadcast_to(extra[None], (nx,) + extra.shape)], axis=1
        )
    parts = lax.all_to_all(parts, "gx", split_axis=0, concat_axis=0, tiled=True)
    return parts.transpose(1, 0, 2).reshape(-1, nx * width)


def to_width_blocks(values, nx, extra=None):
    values = values.astype(BF)
    if extra is not None:
        values = jnp.concatenate([values, extra], axis=0)
    rows, whole = values.shape
    parts = values.reshape(rows, nx, whole // nx).transpose(1, 0, 2)
    return lax.all_to_all(parts, "gx", split_axis=0, concat_axis=0, tiled=True)


def flip(index, mask):
    return index + mask - 2 * mask * ((index // mask) % 2)


def flip_all(index, masks):
    bit = 1
    while bit <= masks:
        if masks & bit:
            index = flip(index, bit)
        bit *= 2
    return index


def greet(me, bits, lanes=0):
    barrier = pltpu.get_barrier_semaphore()
    for bit in bits:
        pl.semaphore_signal(barrier, inc=1, device_id={"gy": flip(me, bit)}, device_id_type=MESH)
    for d in range(1, lanes):
        other = (lax.axis_index("gx") + d) % lanes
        pl.semaphore_signal(barrier, inc=1, device_id={"gx": other}, device_id_type=MESH)
    pl.semaphore_wait(barrier, len(bits) + max(lanes - 1, 0))


def bit_orders(size):
    bits = []
    bit = 2
    while bit < size:
        bits.append(bit)
        bit *= 2
    return (bits + [1], bits[::-1] + [1])


def swap_start(lanes, side_ref, there_ref, sems):
    me = lax.axis_index("gx")
    own, send_sem, recv_sem = sems
    made = [pltpu.make_async_copy(side_ref.at[me], there_ref.at[me], own)]
    for d in range(1, lanes):
        other = (me + d) % lanes
        made.append(
            pltpu.make_async_remote_copy(
                src_ref=side_ref.at[other],
                dst_ref=there_ref.at[me],
                send_sem=send_sem.at[d],
                recv_sem=recv_sem.at[d],
                device_id={"gx": other},
                device_id_type=MESH,
            )
        )
    for copy in made:
        copy.start()
    return made


def swap_sems(lanes):
    return [
        pltpu.SemaphoreType.DMA,
        pltpu.SemaphoreType.DMA((lanes,)),
        pltpu.SemaphoreType.DMA((lanes,)),
    ]


def spread_kernel(size, lanes, *refs):
    if lanes:
        own_ref, side_ref, all_ref, there_ref, local_sem, send_sem, recv_sem, *sems = refs
    else:
        own_ref, all_ref, local_sem, send_sem, recv_sem = refs
    me = lax.axis_index("gy")
    orders = bit_orders(size)
    half = own_ref.shape[0] // 2
    greet(me, orders[0], lanes)
    swapped = swap_start(lanes, side_ref, there_ref, sems) if lanes else []
    keep = pltpu.make_async_copy(own_ref, all_ref.at[me], local_sem)
    keep.start()
    copies = {}
    arrival = {}

    def copy(h, bit, r):
        n = len(copies)
        rows = pl.ds(h * half, half)
        where = flip_all(me, r)
        source = own_ref.at[rows] if r == 0 else all_ref.at[where, rows]
        made = pltpu.make_async_remote_copy(
            src_ref=source,
            dst_ref=all_ref.at[where, rows],
            send_sem=send_sem.at[n],
            recv_sem=recv_sem.at[n],
            device_id={"gy": flip(me, bit)},
            device_id_type=MESH,
        )
        copies[h, bit, r] = made
        arrival[h, r ^ bit] = made
        made.start()

    for step in range(len(orders[0])):
        for h in range(2):
            copy(h, orders[h][step], 0)
    landed = set()

    def land(h, r):
        if (h, r) not in landed:
            landed.add((h, r))
            arrival[h, r].wait_recv()

    held = [[0], [0]]
    for step in range(len(orders[0])):
        for h in range(2):
            bit = orders[h][step]
            for r in held[h]:
                if r:
                    land(h, r)
                    copy(h, bit, r)
        for h in range(2):
            held[h] = held[h] + [r ^ orders[h][step] for r in held[h]]
    for h in range(2):
        for r in range(1, size):
            land(h, r)
    for made in copies.values():
        made.wait_send()
    for copy in [keep] + swapped:
        copy.wait()


def spread(values, side=None):
    size = lax.axis_size("gy")
    values = values.astype(BF)
    rows, width = values.shape
    count = 2 * (size - 1)
    sides = [] if side is None else [side]
    lanes = 0 if side is None else side.shape[0]
    space = pl.BlockSpec(memory_space=pltpu.VMEM)
    out = pl.pallas_call(
        functools.partial(spread_kernel, size, lanes),
        out_shape=[jax.ShapeDtypeStruct((size, rows, width), values.dtype)]
        + [jax.ShapeDtypeStruct(v.shape, v.dtype) for v in sides],
        in_specs=[space] * (1 + len(sides)),
        out_specs=[space] * (1 + len(sides)),
        scratch_shapes=[
            pltpu.SemaphoreType.DMA,
            pltpu.SemaphoreType.DMA((count,)),
            pltpu.SemaphoreType.DMA((count,)),
        ]
        + (swap_sems(lanes) if lanes else []),
        compiler_params=pltpu.CompilerParams(
            collective_id=4 if lanes else 0, has_side_effects=True, vmem_limit_bytes=32 << 20
        ),
        cost_estimate=pl.CostEstimate(
            flops=0, bytes_accessed=size * rows * width * 16, transcendentals=0
        ),
        name="spread",
    )(values, *sides)
    whole = out[0].reshape(size * rows, width)
    return (whole, out[1]) if lanes else whole


def settle_kernel(size, lanes, *refs):
    if lanes:
        parts_ref, side_ref, sum_ref, there_ref, came, kept, send_sem, recv_sem, *sems = refs
    else:
        parts_ref, sum_ref, came, kept, send_sem, recv_sem = refs
    me = lax.axis_index("gy")
    orders = tuple(order[::-1] for order in bit_orders(size))
    half = sum_ref.shape[0] // 2
    strip = 16
    greet(me, orders[0], lanes)
    swapped = swap_start(lanes, side_ref, there_ref, sems) if lanes else []
    slot = {}
    for h in range(2):
        held = list(range(size))
        for step, bit in enumerate(orders[h]):
            held = [r for r in held if not r & bit]
            for r in held:
                slot[h, step, r] = len(slot)
    copies = {}

    def view(h, step, r):
        if step == 0:
            return parts_ref.at[flip_all(me, r), pl.ds(h * half, half)]
        return kept.at[h, r]

    def send(h, step):
        bit = orders[h][step]
        gone = set()
        for b in orders[h][:step]:
            gone.add(b)
        for r in range(size):
            if r & bit and not any(r & b for b in gone):
                n = slot[h, step, r ^ bit]
                made = pltpu.make_async_remote_copy(
                    src_ref=view(h, step, r),
                    dst_ref=came.at[n],
                    send_sem=send_sem.at[n],
                    recv_sem=recv_sem.at[n],
                    device_id={"gy": flip(me, bit)},
                    device_id_type=MESH,
                )
                copies[h, step, r ^ bit] = made
                made.start()

    def gather(h, step, r, last):
        n = slot[h, step, r]
        copies[h, step, r].wait_recv()

        @pl.loop(0, half // strip)
        def _(i):
            rows = pl.ds(i * strip, strip)
            total = view(h, step, r)[rows].astype(F32) + came[n, rows].astype(F32)
            if last:
                sum_ref[pl.ds(h * half + i * strip, strip)] = total
            else:
                kept[h, r, rows] = total.astype(BF)

    steps = len(orders[0])
    for h in range(2):
        send(h, 0)
    for step in range(steps):
        for h in range(2):
            bits = orders[h][: step + 1]
            later = orders[h][step + 1] if step + 1 < steps else 0
            left = [r for r in range(size) if not any(r & b for b in bits)]
            for r in left:
                if r & later:
                    gather(h, step, r, False)
            if later:
                send(h, step + 1)
            for r in left:
                if not r & later:
                    gather(h, step, r, step == steps - 1)
    for made in copies.values():
        made.wait_send()
    for copy in swapped:
        copy.wait()


def settle(parts, side=None):
    size = lax.axis_size("gy")
    parts = parts.astype(BF)
    total, width = parts.shape
    rows = total // size
    count = 2 * (size - 1)
    sides = [] if side is None else [side]
    lanes = 0 if side is None else side.shape[0]
    space = pl.BlockSpec(memory_space=pltpu.VMEM)
    out = pl.pallas_call(
        functools.partial(settle_kernel, size, lanes),
        out_shape=[jax.ShapeDtypeStruct((rows, width), F32)]
        + [jax.ShapeDtypeStruct(v.shape, v.dtype) for v in sides],
        in_specs=[space] * (1 + len(sides)),
        out_specs=[space] * (1 + len(sides)),
        scratch_shapes=[
            pltpu.VMEM((count, rows // 2, width), BF),
            pltpu.VMEM((2, size, rows // 2, width), BF),
            pltpu.SemaphoreType.DMA((count,)),
            pltpu.SemaphoreType.DMA((count,)),
        ]
        + (swap_sems(lanes) if lanes else []),
        compiler_params=pltpu.CompilerParams(
            collective_id=5 if lanes else 1, has_side_effects=True, vmem_limit_bytes=32 << 20
        ),
        cost_estimate=pl.CostEstimate(
            flops=0, bytes_accessed=total * width * 16, transcendentals=0
        ),
        name="settle",
    )(parts.reshape(size, rows, width), *sides)
    return out if lanes else out[0]


def tally_kernel(size, own_ref, sum_ref, came, send_sem, recv_sem):
    me = lax.axis_index("gy")
    barrier = pltpu.get_barrier_semaphore()
    for d in range(1, size):
        pl.semaphore_signal(
            barrier, inc=1, device_id={"gy": (me + d) % size}, device_id_type=MESH
        )
    pl.semaphore_wait(barrier, size - 1)
    copies = []
    for d in range(1, size):
        made = pltpu.make_async_remote_copy(
            src_ref=own_ref,
            dst_ref=came.at[d],
            send_sem=send_sem.at[d],
            recv_sem=recv_sem.at[d],
            device_id={"gy": (me + d) % size},
            device_id_type=MESH,
        )
        made.start()
        copies.append(made)
    total = own_ref[...]
    for d in range(1, size):
        copies[d - 1].wait_recv()
        total = total + came[d]
    sum_ref[...] = total
    for made in copies:
        made.wait_send()


def tally(values, size):
    return pl.pallas_call(
        functools.partial(tally_kernel, size),
        out_shape=jax.ShapeDtypeStruct(values.shape, F32),
        in_specs=[pl.BlockSpec(memory_space=pltpu.VMEM)],
        out_specs=pl.BlockSpec(memory_space=pltpu.VMEM),
        scratch_shapes=[
            pltpu.VMEM((size,) + values.shape, F32),
            pltpu.SemaphoreType.DMA((size,)),
            pltpu.SemaphoreType.DMA((size,)),
        ],
        compiler_params=pltpu.CompilerParams(collective_id=2, has_side_effects=True),
        name="tally",
    )(values)


def feed_forward(rows, weight):
    pre_gate = product("td,df->tf", rows, weight[:, 0, :])
    up_part = product("td,df->tf", rows, weight[:, 1, :])
    value, slope = gelu_parts(pre_gate)
    return ((value * up_part).astype(BF), value, slope, up_part)


def feed_back(hidden_grad, kept):
    _, value, slope, up_part = kept
    return ((hidden_grad * up_part * slope).astype(BF), (hidden_grad * value).astype(BF))


def spend(pair, weight):
    return product("tf,df->td", pair[0], weight[:, 0, :]) + product(
        "tf,df->td", pair[1], weight[:, 1, :]
    )


class Fold:
    def __init__(self, nx):
        half = nx // 2
        self.active = half == 2 and nx % 2 == 0
        self.half = half
        self.inward = [(half - 2, half - 1), (half + 1, half)]
        self.outward = [(b, a) for a, b in self.inward]
        self.across = [(half - 1, half), (half, half - 1)]

    def places(self):
        me = lax.axis_index("gx")
        first = me == self.half - 1
        return (first, jnp.logical_or(first, me == self.half))

    def hop_in(self, values):
        return lax.ppermute(values, "gx", self.inward)

    def hop_out(self, values):
        return lax.ppermute(values, "gx", self.outward)

    def hop_across(self, values):
        return lax.ppermute(values, "gx", self.across)

    def fetch(self, own):
        first, middle = self.places()
        outer = self.hop_in(own)
        other_own = self.hop_across(own)
        other_outer = self.hop_across(outer)
        mine = jnp.where(middle, own, jnp.zeros_like(own))
        return jnp.concatenate(
            [
                jnp.where(first, outer, other_outer),
                jnp.where(first, mine, other_own),
                jnp.where(first, other_own, mine),
                jnp.where(first, other_outer, outer),
            ],
            axis=0,
        )

    def trade(self, sums):
        first, _ = self.places()
        blocks = jnp.split(sums, 4, axis=0)
        got_own = self.hop_across(jnp.where(first, blocks[2], blocks[1]))
        got_outer = self.hop_across(jnp.where(first, blocks[3], blocks[0]))
        return (got_own, got_outer)

    def give_back(self, sums, got):
        first, middle = self.places()
        blocks = jnp.split(sums, 4, axis=0)
        own = jnp.where(first, blocks[1], blocks[2]).astype(F32) + got[0].astype(F32)
        outer = jnp.where(first, blocks[0], blocks[3]).astype(F32) + got[1].astype(F32)
        return jnp.where(middle, own.astype(BF), self.hop_out(outer.astype(BF)))


def make_shards(nx, ny):
    fold = Fold(nx)
    blocks = [((b // ny) * ny + b % ny, (b % nx) * ny + b // nx) for b in range(nx * ny)]

    def shards(
        inputs,
        segment_ids,
        qkv_weight,
        out_weight,
        gate_up_weight,
        down_weight,
        first_gain,
        second_gain,
        third_gain,
        fourth_gain,
        cotangent,
    ):
        width = inputs.shape[1]

        gains = thirds(jnp.stack([first_gain, second_gain, third_gain, fourth_gain]))
        rows_in = to_whole_rows(inputs, nx, gains)
        own = inputs.shape[0] // nx
        heads = qkv_weight.shape[1]
        x_rows = rows_in[:own].astype(F32)
        gains = join_thirds(rows_in[own:])[:, None, :]
        both_w = lax.all_gather(
            jnp.concatenate([qkv_weight, out_weight.T], axis=1), "gx", axis=0, tiled=True
        )
        hid = down_weight.shape[0]
        near = hid - hid // 3 if fold.active else hid
        down_t = down_weight.T
        gate_up_w = lax.all_gather(gate_up_weight[:, :, :near], "gx", axis=0, tiled=True)
        down_w = lax.all_gather(down_t[:, :near], "gx", axis=0, tiled=True)
        if fold.active:
            gate_up_f = fold.fetch(gate_up_weight[:, :, near:])
            down_f = fold.fetch(down_t[:, near:])
        qkv_w, out_w = both_w[:, :heads], both_w[:, heads:]

        segment_row = lax.ppermute(segment_ids[0], ("gx", "gy"), blocks)
        position, allowed = block_layout(segment_row)
        layout = (allowed,) + rope_tables(position)

        scale_one = inverse_rms(x_rows)
        unit_one = x_rows * scale_one
        normed_one = spread(unit_one * gains[0])
        rows = product("td,dc->tc", normed_one, qkv_w).astype(BF)
        rows = lax.all_to_all(rows, "gy", split_axis=0, concat_axis=1, tiled=True)
        mixing_rows, saved = attention_forward(rows, layout)
        mixed = lax.all_to_all(mixing_rows, "gy", split_axis=1, concat_axis=0, tiled=True)
        attn_branch = settle(product("tc,dc->td", mixed, out_w))
        scale_two = inverse_rms(attn_branch)
        unit_two = attn_branch * scale_two
        attn_term = unit_two * gains[1]
        middle = x_rows + attn_term
        scale_three = inverse_rms(middle)
        unit_three = middle * scale_three
        two_rows = (unit_three * gains[2]).astype(BF)
        if fold.active:
            outer_rows = fold.hop_in(two_rows)
        normed_two = spread(two_rows)
        ours = feed_forward(normed_two, gate_up_w)
        partial = product("tf,df->td", ours[0], down_w)
        if fold.active:
            normed_out = spread(outer_rows)
            ours_f = feed_forward(normed_two, gate_up_f)
            theirs = feed_forward(normed_out, gate_up_f)
            outer_branch = fold.hop_out(settle(product("tf,df->td", theirs[0], down_f)).astype(BF))
            partial = partial + product("tf,df->td", ours_f[0], down_f)
        ff_branch, cot_parts = settle(partial, cotangent.astype(BF).reshape(nx, own, width))
        if fold.active:
            ff_branch = ff_branch + outer_branch.astype(F32)
        cot_rows = cot_parts.transpose(1, 0, 2).reshape(own, nx * width).astype(F32)
        scale_four = inverse_rms(ff_branch)
        unit_four = ff_branch * scale_four
        delta = (attn_term + unit_four * gains[3]).astype(BF)
        four_rows = norm_back(cot_rows, unit_four, scale_four, gains[3]).astype(BF)
        if fold.active:
            outer_rows = fold.hop_in(four_rows)
        ff_grad, delta = spread(four_rows, delta.reshape(own, nx, width).transpose(1, 0, 2))
        outputs = inputs + delta.reshape(inputs.shape).astype(F32)

        hidden = ours[0]
        down_sum = product("td,tf->df", ff_grad, hidden).astype(BF)
        down_sum, ff_grad = lax.optimization_barrier((down_sum, ff_grad))
        down_done = lax.psum_scatter(down_sum, "gx", scatter_dimension=0, tiled=True)
        pair = feed_back(product("td,df->tf", ff_grad, down_w), ours)
        gate_up_sum = jnp.stack(
            [product("td,tf->df", normed_two, g).astype(BF) for g in pair], axis=1
        )
        gate_up_sum, pair = lax.optimization_barrier((gate_up_sum, pair))
        gate_up_done = lax.psum_scatter(gate_up_sum, "gx", scatter_dimension=0, tiled=True)
        partial = spend(pair, gate_up_w)
        if fold.active:
            ff_out = spread(outer_rows)
            pair_f = feed_back(product("td,df->tf", ff_grad, down_f), ours_f)
            pair_o = feed_back(product("td,df->tf", ff_out, down_f), theirs)
            outer_grad = settle(spend(pair_o, gate_up_f)).astype(BF)
            partial = (partial + spend(pair_f, gate_up_f)).astype(BF)
            outer_grad, partial = lax.optimization_barrier((outer_grad, partial))
            outer_grad = fold.hop_out(outer_grad)
        normed_two_grad = settle(partial)
        if fold.active:
            normed_two_grad = normed_two_grad + outer_grad.astype(F32)
            down_far = (
                product("td,tf->df", ff_grad, ours_f[0]) + product("td,tf->df", ff_out, theirs[0])
            ).astype(BF)
            gate_up_far = jnp.stack(
                [
                    (
                        product("td,tf->df", normed_two, pair_f[i])
                        + product("td,tf->df", normed_out, pair_o[i])
                    ).astype(BF)
                    for i in range(2)
                ],
                axis=1,
            )
        middle_delta = norm_back(normed_two_grad, unit_three, scale_three, gains[2])
        middle_grad = cot_rows + middle_delta
        branch_grad = spread(norm_back(middle_grad, unit_two, scale_two, gains[1]))
        out_sum = product("td,tc->dc", branch_grad, mixed).astype(BF)
        mixing_gradient = product("td,dc->tc", branch_grad, out_w).astype(BF)
        mixing_gradient = lax.all_to_all(
            mixing_gradient, "gy", split_axis=0, concat_axis=1, tiled=True
        )
        if fold.active:
            mixing_gradient, down_far, gate_up_far = lax.optimization_barrier(
                (mixing_gradient, down_far, gate_up_far)
            )
            traded = fold.trade(gate_up_far), fold.trade(down_far)
        qkv_grad_rows = attention_backward(mixing_gradient, mixing_rows, saved, layout)
        qkv_grad_rows, down_done = lax.optimization_barrier((qkv_grad_rows, down_done))
        qkv_grad_rows = lax.all_to_all(
            qkv_grad_rows, "gy", split_axis=1, concat_axis=0, tiled=True
        )
        normed_one_grad = settle(product("tc,dc->td", qkv_grad_rows, qkv_w))
        if fold.active:
            normed_one_grad, traded = lax.optimization_barrier((normed_one_grad, traded))
            gate_up_far = fold.give_back(gate_up_far, traded[0])
            down_far = fold.give_back(down_far, traded[1])
        both_sum = jnp.concatenate(
            [product("td,tc->dc", normed_one, qkv_grad_rows).astype(BF), out_sum], axis=1
        )
        terms = jnp.stack(
            [
                jnp.sum(normed_one_grad * unit_one, axis=0),
                jnp.sum(middle_grad * unit_two, axis=0),
                jnp.sum(normed_two_grad * unit_three, axis=0),
                jnp.sum(cot_rows * unit_four, axis=0),
            ]
        )
        delta = to_width_blocks(
            middle_delta + norm_back(normed_one_grad, unit_one, scale_one, gains[0]),
            nx,
            thirds(tally(terms, ny)),
        )
        if fold.active:
            down_done = jnp.concatenate([down_done, down_far], axis=1)
        down_grad = down_done.astype(F32).T
        gate_up_done, both_sum, delta, down_grad = lax.optimization_barrier(
            (gate_up_done, both_sum, delta, down_grad)
        )
        both_done = lax.psum_scatter(both_sum, "gx", scatter_dimension=0, tiled=True)
        if fold.active:
            gate_up_done = jnp.concatenate([gate_up_done, gate_up_far], axis=2)
        gate_up_grad = gate_up_done.astype(F32)
        input_grad = cotangent + delta[:, :own].reshape(inputs.shape).astype(F32)
        terms = jnp.sum(join_thirds(delta[:, own:]), axis=0)
        qkv_grad = both_done[:, :heads].astype(F32)
        out_grad = both_done[:, heads:].astype(F32).T
        return (outputs, input_grad, qkv_grad, out_grad, gate_up_grad, down_grad) + tuple(
            terms[i] for i in range(4)
        )

    return shards


def solution(mesh):
    placed = (
        P("gy", "gx"),
        P(("gx", "gy"), None),
        P("gx", "gy"),
        P("gy", "gx"),
        P("gx", None, "gy"),
        P("gy", "gx"),
        P("gx"),
        P("gx"),
        P("gx"),
        P("gx"),
        P("gy", "gx"),
    )
    return jax.shard_map(
        make_shards(mesh.shape["gx"], mesh.shape["gy"]),
        mesh=mesh,
        in_specs=placed,
        out_specs=(
            P("gy", "gx"),
            P("gy", "gx"),
            P("gx", "gy"),
            P("gy", "gx"),
            P("gx", None, "gy"),
            P("gy", "gx"),
            P("gx"),
            P("gx"),
            P("gx"),
            P("gx"),
        ),
        check_vma=False,
    )
```

```python
import functools
import math

import jax
import jax.numpy as jnp
from jax import lax
from jax.experimental import pallas as pl
from jax.experimental.pallas import tpu as pltpu
from jax.sharding import PartitionSpec as P

QUERY_HEADS = 8
KEY_VALUE_HEADS = 4
HEAD_SIZE = 256


EPSILON = 1e-06
SOFT_CAP = 50.0
GELU_COEF = 0.7978845608028654
CUBIC_COEF = 0.044715

BF = jnp.bfloat16
F32 = jnp.float32
MESH = pl.DeviceIdType.MESH


def product(form, left, right):
    return jnp.einsum(form, left, right, preferred_element_type=F32)


def gelu_parts(pre_gate):
    inner_arg = GELU_COEF * (pre_gate + CUBIC_COEF * pre_gate * pre_gate * pre_gate)
    tanh_value = jnp.tanh(inner_arg)
    activated = 0.5 * pre_gate * (1.0 + tanh_value)
    derivative = 0.5 * (1.0 + tanh_value) + 0.5 * pre_gate * (
        1.0 - tanh_value * tanh_value
    ) * GELU_COEF * (1.0 + 3.0 * CUBIC_COEF * pre_gate * pre_gate)
    return (activated, derivative)


def block_layout(segment_row):
    length_total = segment_row.shape[0]
    places = jnp.arange(length_total, dtype=jnp.int32)
    same_doc = segment_row[:, None] == segment_row[None, :]
    starts = jnp.min(jnp.where(same_doc, places[None, :], length_total), axis=1)
    allowed = jnp.logical_and(same_doc, places[None, :] <= places[:, None])
    return (places - starts, allowed)


def rope_tables(position):
    half_dim = HEAD_SIZE // 2
    freq_steps = jnp.arange(half_dim, dtype=F32)
    frequency = jnp.exp(freq_steps * (-2.0 * math.log(10000.0) / HEAD_SIZE))
    angles = position.astype(F32)[:, None] * frequency[None, :]
    return (jnp.cos(angles)[:, None, :], jnp.sin(angles)[:, None, :])


def rotate(values, cos_table, sin_table, direction):
    half_dim = values.shape[-1] // 2
    leading = values[..., :half_dim]
    trailing = values[..., half_dim:]
    return jnp.concatenate(
        [
            leading * cos_table - direction * trailing * sin_table,
            trailing * cos_table + direction * leading * sin_table,
        ],
        axis=-1,
    )


def capped_scores(rotated_query, k_rot):
    token_rows = rotated_query.shape[0]
    query_groups = rotated_query.reshape(
        token_rows, KEY_VALUE_HEADS, QUERY_HEADS // KEY_VALUE_HEADS, HEAD_SIZE
    )
    raw_scores = product("tkgd,skd->kgts", query_groups, k_rot) * HEAD_SIZE ** (-0.5)
    return SOFT_CAP * jnp.tanh(raw_scores / SOFT_CAP)


def attention_forward(rows, layout):
    token_rows = rows.shape[0]
    query_span_width = QUERY_HEADS * HEAD_SIZE
    key_value_width = KEY_VALUE_HEADS * HEAD_SIZE
    allowed, cos_table, sin_table = layout
    query_part = (
        rows[:, :query_span_width].astype(F32).reshape(token_rows, QUERY_HEADS, HEAD_SIZE)
    )
    key_slice = (
        rows[:, query_span_width : query_span_width + key_value_width]
        .astype(F32)
        .reshape(token_rows, KEY_VALUE_HEADS, HEAD_SIZE)
    )
    value_slice = rows[:, query_span_width + key_value_width :].reshape(
        token_rows, KEY_VALUE_HEADS, HEAD_SIZE
    )
    rotated_query = rotate(query_part, cos_table, sin_table, 1.0).astype(BF)
    k_rot = rotate(key_slice, cos_table, sin_table, 1.0).astype(BF)
    capped = capped_scores(rotated_query, k_rot)
    log_total = jnp.log(jnp.sum(jnp.where(allowed, jnp.exp(capped), 0.0), axis=-1))
    weights_f = jnp.where(allowed, jnp.exp(capped - log_total[..., None]), 0.0)
    mixing_rows = product("kgts,skd->tkgd", weights_f.astype(BF), value_slice)
    mixing_rows = mixing_rows.astype(BF).reshape(token_rows, query_span_width)
    return (mixing_rows, (rotated_query, k_rot, value_slice, log_total))


def attention_backward(mixing_gradient, mixing_rows, saved, layout):
    rotated_query, k_rot, value_slice, log_total = saved
    token_rows = mixing_gradient.shape[0]
    heads_per_group = QUERY_HEADS // KEY_VALUE_HEADS
    allowed, cos_table, sin_table = layout
    capped = capped_scores(rotated_query, k_rot)
    weights_f = jnp.where(allowed, jnp.exp(capped - log_total[..., None]), 0.0)
    gradient_by_group = mixing_gradient.reshape(
        token_rows, KEY_VALUE_HEADS, heads_per_group, HEAD_SIZE
    )
    output_by_group = mixing_rows.reshape(token_rows, KEY_VALUE_HEADS, heads_per_group, HEAD_SIZE)
    row_delta = product("tkgd,tkgd->kgt", gradient_by_group, output_by_group)
    value_gradient = product("maew,emaq->wmq", weights_f.astype(BF), gradient_by_group)
    weight_grad = product("tkgd,skd->kgts", gradient_by_group, value_slice)
    score_gradient = (
        weights_f
        * (weight_grad - row_delta[..., None])
        * (1.0 - (capped / SOFT_CAP) ** 2)
        * HEAD_SIZE ** (-0.5)
    )
    score_gradient = score_gradient.astype(BF)
    query_gradient = product("kgts,skd->tkgd", score_gradient, k_rot).reshape(
        token_rows, QUERY_HEADS, HEAD_SIZE
    )
    key_gradient = product(
        "maew,emaq->wmq",
        score_gradient,
        rotated_query.reshape(token_rows, KEY_VALUE_HEADS, heads_per_group, HEAD_SIZE),
    )
    query_gradient = rotate(query_gradient, cos_table, sin_table, -1.0)
    key_gradient = rotate(key_gradient, cos_table, sin_table, -1.0)
    return jnp.concatenate(
        [
            query_gradient.reshape(token_rows, QUERY_HEADS * HEAD_SIZE),
            key_gradient.reshape(token_rows, KEY_VALUE_HEADS * HEAD_SIZE),
            value_gradient.reshape(token_rows, KEY_VALUE_HEADS * HEAD_SIZE),
        ],
        axis=1,
    ).astype(BF)


def inverse_rms(values):
    return lax.rsqrt(jnp.mean(values * values, axis=1, keepdims=True) + EPSILON)


def norm_back(grad_rows, unit_rows, scale_rows, gain):
    scaled = grad_rows * gain
    return scale_rows * (scaled - unit_rows * jnp.mean(scaled * unit_rows, axis=1, keepdims=True))


def thirds(values):
    high = lax.reduce_precision(values, 8, 7)
    rest = values - high
    middle = lax.reduce_precision(rest, 8, 7)
    return jnp.concatenate([high, middle, rest - middle], axis=0).astype(BF)


def join_thirds(rows):
    count = rows.shape[-2] // 3
    rows = rows.astype(F32)
    return rows[..., :count, :] + rows[..., count : 2 * count, :] + rows[..., 2 * count :, :]


def to_whole_rows(values, nx, extra=None):
    width = values.shape[1]
    parts = values.astype(BF).reshape(nx, -1, width)
    if extra is not None:
        parts = jnp.concatenate(
            [parts, jnp.broadcast_to(extra[None], (nx,) + extra.shape)], axis=1
        )
    parts = lax.all_to_all(parts, "gx", split_axis=0, concat_axis=0, tiled=True)
    return parts.transpose(1, 0, 2).reshape(-1, nx * width)


def to_width_blocks(values, nx, extra=None):
    values = values.astype(BF)
    if extra is not None:
        values = jnp.concatenate([values, extra], axis=0)
    rows, whole = values.shape
    parts = values.reshape(rows, nx, whole // nx).transpose(1, 0, 2)
    return lax.all_to_all(parts, "gx", split_axis=0, concat_axis=0, tiled=True)


def flip(index, mask):
    return index + mask - 2 * mask * ((index // mask) % 2)


def flip_all(index, masks):
    bit = 1
    while bit <= masks:
        if masks & bit:
            index = flip(index, bit)
        bit *= 2
    return index


def greet(me, bits, lanes=0):
    barrier = pltpu.get_barrier_semaphore()
    for bit in bits:
        pl.semaphore_signal(barrier, inc=1, device_id={"gy": flip(me, bit)}, device_id_type=MESH)
    for d in range(1, lanes):
        other = (lax.axis_index("gx") + d) % lanes
        pl.semaphore_signal(barrier, inc=1, device_id={"gx": other}, device_id_type=MESH)
    pl.semaphore_wait(barrier, len(bits) + max(lanes - 1, 0))


def bit_orders(size):
    bits = []
    bit = 2
    while bit < size:
        bits.append(bit)
        bit *= 2
    return (bits + [1], bits[::-1] + [1])


def swap_start(lanes, side_ref, there_ref, sems):
    me = lax.axis_index("gx")
    own, send_sem, recv_sem = sems
    made = [pltpu.make_async_copy(side_ref.at[me], there_ref.at[me], own)]
    for d in range(1, lanes):
        other = (me + d) % lanes
        made.append(
            pltpu.make_async_remote_copy(
                src_ref=side_ref.at[other],
                dst_ref=there_ref.at[me],
                send_sem=send_sem.at[d],
                recv_sem=recv_sem.at[d],
                device_id={"gx": other},
                device_id_type=MESH,
            )
        )
    for copy in made:
        copy.start()
    return made


def swap_sems(lanes):
    return [
        pltpu.SemaphoreType.DMA,
        pltpu.SemaphoreType.DMA((lanes,)),
        pltpu.SemaphoreType.DMA((lanes,)),
    ]


def spread_kernel(size, lanes, *refs):
    if lanes:
        own_ref, side_ref, all_ref, there_ref, local_sem, send_sem, recv_sem, *sems = refs
    else:
        own_ref, all_ref, local_sem, send_sem, recv_sem = refs
    me = lax.axis_index("gy")
    orders = bit_orders(size)
    half = own_ref.shape[0] // 2
    greet(me, orders[0], lanes)
    swapped = swap_start(lanes, side_ref, there_ref, sems) if lanes else []
    keep = pltpu.make_async_copy(own_ref, all_ref.at[me], local_sem)
    keep.start()
    copies = {}
    arrival = {}

    def copy(h, bit, r):
        n = len(copies)
        rows = pl.ds(h * half, half)
        where = flip_all(me, r)
        source = own_ref.at[rows] if r == 0 else all_ref.at[where, rows]
        made = pltpu.make_async_remote_copy(
            src_ref=source,
            dst_ref=all_ref.at[where, rows],
            send_sem=send_sem.at[n],
            recv_sem=recv_sem.at[n],
            device_id={"gy": flip(me, bit)},
            device_id_type=MESH,
        )
        copies[h, bit, r] = made
        arrival[h, r ^ bit] = made
        made.start()

    for step in range(len(orders[0])):
        for h in range(2):
            copy(h, orders[h][step], 0)
    landed = set()

    def land(h, r):
        if (h, r) not in landed:
            landed.add((h, r))
            arrival[h, r].wait_recv()

    held = [[0], [0]]
    for step in range(len(orders[0])):
        for h in range(2):
            bit = orders[h][step]
            for r in held[h]:
                if r:
                    land(h, r)
                    copy(h, bit, r)
        for h in range(2):
            held[h] = held[h] + [r ^ orders[h][step] for r in held[h]]
    for h in range(2):
        for r in range(1, size):
            land(h, r)
    for made in copies.values():
        made.wait_send()
    for copy in [keep] + swapped:
        copy.wait()


def spread(values, side=None):
    size = lax.axis_size("gy")
    values = values.astype(BF)
    rows, width = values.shape
    count = 2 * (size - 1)
    sides = [] if side is None else [side]
    lanes = 0 if side is None else side.shape[0]
    space = pl.BlockSpec(memory_space=pltpu.VMEM)
    out = pl.pallas_call(
        functools.partial(spread_kernel, size, lanes),
        out_shape=[jax.ShapeDtypeStruct((size, rows, width), values.dtype)]
        + [jax.ShapeDtypeStruct(v.shape, v.dtype) for v in sides],
        in_specs=[space] * (1 + len(sides)),
        out_specs=[space] * (1 + len(sides)),
        scratch_shapes=[
            pltpu.SemaphoreType.DMA,
            pltpu.SemaphoreType.DMA((count,)),
            pltpu.SemaphoreType.DMA((count,)),
        ]
        + (swap_sems(lanes) if lanes else []),
        compiler_params=pltpu.CompilerParams(
            collective_id=4 if lanes else 0, has_side_effects=True, vmem_limit_bytes=32 << 20
        ),
        cost_estimate=pl.CostEstimate(
            flops=0, bytes_accessed=size * rows * width * 16, transcendentals=0
        ),
        name="spread",
    )(values, *sides)
    whole = out[0].reshape(size * rows, width)
    return (whole, out[1]) if lanes else whole


def settle_kernel(size, lanes, *refs):
    if lanes:
        parts_ref, side_ref, sum_ref, there_ref, came, kept, send_sem, recv_sem, *sems = refs
    else:
        parts_ref, sum_ref, came, kept, send_sem, recv_sem = refs
    me = lax.axis_index("gy")
    orders = tuple(order[::-1] for order in bit_orders(size))
    half = sum_ref.shape[0] // 2
    strip = 16
    greet(me, orders[0], lanes)
    swapped = swap_start(lanes, side_ref, there_ref, sems) if lanes else []
    slot = {}
    for h in range(2):
        held = list(range(size))
        for step, bit in enumerate(orders[h]):
            held = [r for r in held if not r & bit]
            for r in held:
                slot[h, step, r] = len(slot)
    copies = {}

    def view(h, step, r):
        if step == 0:
            return parts_ref.at[flip_all(me, r), pl.ds(h * half, half)]
        return kept.at[h, r]

    def send(h, step):
        bit = orders[h][step]
        gone = set()
        for b in orders[h][:step]:
            gone.add(b)
        for r in range(size):
            if r & bit and not any(r & b for b in gone):
                n = slot[h, step, r ^ bit]
                made = pltpu.make_async_remote_copy(
                    src_ref=view(h, step, r),
                    dst_ref=came.at[n],
                    send_sem=send_sem.at[n],
                    recv_sem=recv_sem.at[n],
                    device_id={"gy": flip(me, bit)},
                    device_id_type=MESH,
                )
                copies[h, step, r ^ bit] = made
                made.start()

    def gather(h, step, r, last):
        n = slot[h, step, r]
        copies[h, step, r].wait_recv()

        @pl.loop(0, half // strip)
        def _(i):
            rows = pl.ds(i * strip, strip)
            total = view(h, step, r)[rows].astype(F32) + came[n, rows].astype(F32)
            if last:
                sum_ref[pl.ds(h * half + i * strip, strip)] = total
            else:
                kept[h, r, rows] = total.astype(BF)

    steps = len(orders[0])
    for h in range(2):
        send(h, 0)
    for step in range(steps):
        for h in range(2):
            bits = orders[h][: step + 1]
            later = orders[h][step + 1] if step + 1 < steps else 0
            left = [r for r in range(size) if not any(r & b for b in bits)]
            for r in left:
                if r & later:
                    gather(h, step, r, False)
            if later:
                send(h, step + 1)
            for r in left:
                if not r & later:
                    gather(h, step, r, step == steps - 1)
    for made in copies.values():
        made.wait_send()
    for copy in swapped:
        copy.wait()


def settle(parts, side=None, call=1):
    size = lax.axis_size("gy")
    parts = parts.astype(BF)
    total, width = parts.shape
    rows = total // size
    count = 2 * (size - 1)
    sides = [] if side is None else [side]
    lanes = 0 if side is None else side.shape[0]
    space = pl.BlockSpec(memory_space=pltpu.VMEM)
    out = pl.pallas_call(
        functools.partial(settle_kernel, size, lanes),
        out_shape=[jax.ShapeDtypeStruct((rows, width), F32)]
        + [jax.ShapeDtypeStruct(v.shape, v.dtype) for v in sides],
        in_specs=[space] * (1 + len(sides)),
        out_specs=[space] * (1 + len(sides)),
        scratch_shapes=[
            pltpu.VMEM((count, rows // 2, width), BF),
            pltpu.VMEM((2, size, rows // 2, width), BF),
            pltpu.SemaphoreType.DMA((count,)),
            pltpu.SemaphoreType.DMA((count,)),
        ]
        + (swap_sems(lanes) if lanes else []),
        compiler_params=pltpu.CompilerParams(
            collective_id=call, has_side_effects=True, vmem_limit_bytes=32 << 20
        ),
        cost_estimate=pl.CostEstimate(
            flops=0, bytes_accessed=total * width * 16, transcendentals=0
        ),
        name="settle",
    )(parts.reshape(size, rows, width), *sides)
    return out if lanes else out[0]


def tally_kernel(size, own_ref, sum_ref, came, send_sem, recv_sem):
    me = lax.axis_index("gy")
    barrier = pltpu.get_barrier_semaphore()
    for d in range(1, size):
        pl.semaphore_signal(
            barrier, inc=1, device_id={"gy": (me + d) % size}, device_id_type=MESH
        )
    pl.semaphore_wait(barrier, size - 1)
    copies = []
    for d in range(1, size):
        made = pltpu.make_async_remote_copy(
            src_ref=own_ref,
            dst_ref=came.at[d],
            send_sem=send_sem.at[d],
            recv_sem=recv_sem.at[d],
            device_id={"gy": (me + d) % size},
            device_id_type=MESH,
        )
        made.start()
        copies.append(made)
    total = own_ref[...]
    for d in range(1, size):
        copies[d - 1].wait_recv()
        total = total + came[d]
    sum_ref[...] = total
    for made in copies:
        made.wait_send()


def tally(values, size):
    return pl.pallas_call(
        functools.partial(tally_kernel, size),
        out_shape=jax.ShapeDtypeStruct(values.shape, F32),
        in_specs=[pl.BlockSpec(memory_space=pltpu.VMEM)],
        out_specs=pl.BlockSpec(memory_space=pltpu.VMEM),
        scratch_shapes=[
            pltpu.VMEM((size,) + values.shape, F32),
            pltpu.SemaphoreType.DMA((size,)),
            pltpu.SemaphoreType.DMA((size,)),
        ],
        compiler_params=pltpu.CompilerParams(collective_id=2, has_side_effects=True),
        name="tally",
    )(values)


def to_parts(rows, nx, part):
    count = rows.shape[0]
    return rows.reshape(count, nx, -1, part).transpose(0, 2, 1, 3).reshape(count, -1)


def make_shards(nx, ny):
    blocks = [((b // ny) * ny + b % ny, (b % nx) * ny + b // nx) for b in range(nx * ny)]

    def shards(
        inputs,
        segment_ids,
        qkv_weight,
        out_weight,
        gate_up_weight,
        down_weight,
        first_gain,
        second_gain,
        third_gain,
        fourth_gain,
        cotangent,
    ):
        width = inputs.shape[1]

        gains = thirds(jnp.stack([first_gain, second_gain, third_gain, fourth_gain]))
        rows_in = to_whole_rows(inputs, nx, gains)
        own = inputs.shape[0] // nx
        heads = qkv_weight.shape[1]
        x_rows = rows_in[:own].astype(F32)
        gains = join_thirds(rows_in[own:])[:, None, :]
        both_w = lax.all_gather(
            jnp.concatenate([qkv_weight, out_weight.T], axis=1), "gx", axis=0, tiled=True
        )
        gate_up_w = lax.all_gather(gate_up_weight, "gx", axis=0, tiled=True)
        part = width // 2
        down_first = lax.all_gather(down_weight.T[:part], "gx", axis=0, tiled=True)
        down_last = lax.all_gather(down_weight.T[part:], "gx", axis=0, tiled=True)
        split = nx * part
        qkv_w, out_w = both_w[:, :heads], both_w[:, heads:]

        segment_row = lax.ppermute(segment_ids[0], ("gx", "gy"), blocks)
        position, allowed = block_layout(segment_row)
        layout = (allowed,) + rope_tables(position)

        scale_one = inverse_rms(x_rows)
        unit_one = x_rows * scale_one
        normed_one = spread(unit_one * gains[0])
        rows = product("td,dc->tc", normed_one, qkv_w).astype(BF)
        rows = lax.all_to_all(rows, "gy", split_axis=0, concat_axis=1, tiled=True)
        mixing_rows, saved = attention_forward(rows, layout)
        mixed = lax.all_to_all(mixing_rows, "gy", split_axis=1, concat_axis=0, tiled=True)
        attn_branch = settle(product("tc,dc->td", mixed, out_w))
        scale_two = inverse_rms(attn_branch)
        unit_two = attn_branch * scale_two
        attn_term = unit_two * gains[1]
        middle = x_rows + attn_term
        scale_three = inverse_rms(middle)
        unit_three = middle * scale_three
        normed_two = spread(unit_three * gains[2])
        pre_gate = product("td,df->tf", normed_two, gate_up_w[:, 0, :])
        up_part = product("td,df->tf", normed_two, gate_up_w[:, 1, :])
        value, slope = gelu_parts(pre_gate)
        hidden = (value * up_part).astype(BF)
        first_branch, cot_parts = settle(
            product("tf,df->td", hidden, down_first), cotangent.astype(BF).reshape(nx, own, width), 5
        )
        cot_rows = cot_parts.transpose(1, 0, 2).reshape(own, nx * width).astype(F32)
        cot_mixed = to_parts(cot_rows, nx, part)
        term_mixed = to_parts(attn_term, nx, part)
        gain_mixed = to_parts(gains[3], nx, part)
        (cot_mixed, term_mixed, gain_mixed), down_last = lax.optimization_barrier(
            ((cot_mixed, term_mixed, gain_mixed), down_last)
        )
        last_branch = settle(product("tf,df->td", hidden, down_last), call=6)
        ff_branch = jnp.concatenate([first_branch, last_branch], axis=1)
        scale_four = inverse_rms(ff_branch)
        unit_four = ff_branch * scale_four
        delta = (term_mixed + unit_four * gain_mixed).astype(BF).reshape(own, -1, nx, part)
        ff_grad, delta = spread(
            norm_back(cot_mixed, unit_four, scale_four, gain_mixed),
            delta.transpose(2, 0, 1, 3).reshape(nx, own, width),
        )
        outputs = inputs + delta.reshape(inputs.shape).astype(F32)

        first_sum = product("td,tf->df", ff_grad[:, :split], hidden).astype(BF)
        first_sum, ff_grad = lax.optimization_barrier((first_sum, ff_grad))
        first_done = lax.psum_scatter(first_sum, "gx", scatter_dimension=0, tiled=True)
        last_sum = product("td,tf->df", ff_grad[:, split:], hidden).astype(BF)
        last_sum, ff_grad = lax.optimization_barrier((last_sum, ff_grad))
        last_done = lax.psum_scatter(last_sum, "gx", scatter_dimension=0, tiled=True)
        down_w = jnp.concatenate([down_first, down_last], axis=0)
        hidden_grad = product("td,df->tf", ff_grad, down_w)
        gate_grad = (hidden_grad * up_part * slope).astype(BF)
        up_grad = (hidden_grad * value).astype(BF)
        gate_up_sum = jnp.stack(
            [
                product("td,tf->df", normed_two, gate_grad).astype(BF),
                product("td,tf->df", normed_two, up_grad).astype(BF),
            ],
            axis=1,
        )
        gate_up_sum, gate_grad, up_grad = lax.optimization_barrier(
            (gate_up_sum, gate_grad, up_grad)
        )
        gate_up_done = lax.psum_scatter(gate_up_sum, "gx", scatter_dimension=0, tiled=True)
        normed_two_grad = settle(
            product("tf,df->td", gate_grad, gate_up_w[:, 0, :])
            + product("tf,df->td", up_grad, gate_up_w[:, 1, :])
        )
        middle_delta = norm_back(normed_two_grad, unit_three, scale_three, gains[2])
        middle_grad = cot_rows + middle_delta
        branch_grad = spread(norm_back(middle_grad, unit_two, scale_two, gains[1]))
        out_sum = product("td,tc->dc", branch_grad, mixed).astype(BF)
        mixing_gradient = product("td,dc->tc", branch_grad, out_w).astype(BF)
        mixing_gradient = lax.all_to_all(
            mixing_gradient, "gy", split_axis=0, concat_axis=1, tiled=True
        )
        qkv_grad_rows = attention_backward(mixing_gradient, mixing_rows, saved, layout)
        qkv_grad_rows, first_done, last_done = lax.optimization_barrier(
            (qkv_grad_rows, first_done, last_done)
        )
        qkv_grad_rows = lax.all_to_all(
            qkv_grad_rows, "gy", split_axis=1, concat_axis=0, tiled=True
        )
        normed_one_grad = settle(product("tc,dc->td", qkv_grad_rows, qkv_w))
        both_sum = jnp.concatenate(
            [product("td,tc->dc", normed_one, qkv_grad_rows).astype(BF), out_sum], axis=1
        )
        terms = jnp.stack(
            [
                jnp.sum(normed_one_grad * unit_one, axis=0),
                jnp.sum(middle_grad * unit_two, axis=0),
                jnp.sum(normed_two_grad * unit_three, axis=0),
                jnp.sum(cot_mixed * unit_four, axis=0)
                .reshape(-1, nx, part)
                .transpose(1, 0, 2)
                .reshape(-1),
            ]
        )
        delta = to_width_blocks(
            middle_delta + norm_back(normed_one_grad, unit_one, scale_one, gains[0]),
            nx,
            thirds(tally(terms, ny)),
        )
        down_grad = jnp.concatenate([first_done, last_done], axis=0).astype(F32).T
        gate_up_done, both_sum, delta, down_grad = lax.optimization_barrier(
            (gate_up_done, both_sum, delta, down_grad)
        )
        both_done = lax.psum_scatter(both_sum, "gx", scatter_dimension=0, tiled=True)
        gate_up_grad = gate_up_done.astype(F32)
        input_grad = cotangent + delta[:, :own].reshape(inputs.shape).astype(F32)
        terms = jnp.sum(join_thirds(delta[:, own:]), axis=0)
        qkv_grad = both_done[:, :heads].astype(F32)
        out_grad = both_done[:, heads:].astype(F32).T
        return (outputs, input_grad, qkv_grad, out_grad, gate_up_grad, down_grad) + tuple(
            terms[i] for i in range(4)
        )

    return shards


def solution(mesh):
    placed = (
        P("gy", "gx"),
        P(("gx", "gy"), None),
        P("gx", "gy"),
        P("gy", "gx"),
        P("gx", None, "gy"),
        P("gy", "gx"),
        P("gx"),
        P("gx"),
        P("gx"),
        P("gx"),
        P("gy", "gx"),
    )
    return jax.shard_map(
        make_shards(mesh.shape["gx"], mesh.shape["gy"]),
        mesh=mesh,
        in_specs=placed,
        out_specs=(
            P("gy", "gx"),
            P("gy", "gx"),
            P("gx", "gy"),
            P("gy", "gx"),
            P("gx", None, "gy"),
            P("gy", "gx"),
            P("gx"),
            P("gx"),
            P("gx"),
            P("gx"),
        ),
        check_vma=False,
    )
```

```python
import functools
import math

import jax
import jax.numpy as jnp
from jax import lax
from jax.experimental import pallas as pl
from jax.experimental.pallas import tpu as pltpu
from jax.sharding import PartitionSpec as P

QUERY_HEADS = 8
KEY_VALUE_HEADS = 4
HEAD_SIZE = 256


EPSILON = 1e-06
SOFT_CAP = 50.0
GELU_COEF = 0.7978845608028654
CUBIC_COEF = 0.044715

BF = jnp.bfloat16
F32 = jnp.float32
MESH = pl.DeviceIdType.MESH


def product(form, left, right):
    return jnp.einsum(form, left, right, preferred_element_type=F32)


def gelu_parts(pre_gate):
    inner_arg = GELU_COEF * (pre_gate + CUBIC_COEF * pre_gate * pre_gate * pre_gate)
    tanh_value = jnp.tanh(inner_arg)
    activated = 0.5 * pre_gate * (1.0 + tanh_value)
    derivative = 0.5 * (1.0 + tanh_value) + 0.5 * pre_gate * (
        1.0 - tanh_value * tanh_value
    ) * GELU_COEF * (1.0 + 3.0 * CUBIC_COEF * pre_gate * pre_gate)
    return (activated, derivative)


def block_layout(segment_row):
    length_total = segment_row.shape[0]
    places = jnp.arange(length_total, dtype=jnp.int32)
    same_doc = segment_row[:, None] == segment_row[None, :]
    starts = jnp.min(jnp.where(same_doc, places[None, :], length_total), axis=1)
    allowed = jnp.logical_and(same_doc, places[None, :] <= places[:, None])
    return (places - starts, allowed)


def rope_tables(position):
    half_dim = HEAD_SIZE // 2
    freq_steps = jnp.arange(half_dim, dtype=F32)
    frequency = jnp.exp(freq_steps * (-2.0 * math.log(10000.0) / HEAD_SIZE))
    angles = position.astype(F32)[:, None] * frequency[None, :]
    return (jnp.cos(angles)[:, None, :], jnp.sin(angles)[:, None, :])


def rotate(values, cos_table, sin_table, direction):
    half_dim = values.shape[-1] // 2
    leading = values[..., :half_dim]
    trailing = values[..., half_dim:]
    return jnp.concatenate(
        [
            leading * cos_table - direction * trailing * sin_table,
            trailing * cos_table + direction * leading * sin_table,
        ],
        axis=-1,
    )


def capped_scores(rotated_query, k_rot):
    token_rows = rotated_query.shape[0]
    query_groups = rotated_query.reshape(
        token_rows, KEY_VALUE_HEADS, QUERY_HEADS // KEY_VALUE_HEADS, HEAD_SIZE
    )
    raw_scores = product("tkgd,skd->kgts", query_groups, k_rot) * HEAD_SIZE ** (-0.5)
    return SOFT_CAP * jnp.tanh(raw_scores / SOFT_CAP)


def attention_forward(rows, layout):
    token_rows = rows.shape[0]
    query_span_width = QUERY_HEADS * HEAD_SIZE
    key_value_width = KEY_VALUE_HEADS * HEAD_SIZE
    allowed, cos_table, sin_table = layout
    query_part = (
        rows[:, :query_span_width].astype(F32).reshape(token_rows, QUERY_HEADS, HEAD_SIZE)
    )
    key_slice = (
        rows[:, query_span_width : query_span_width + key_value_width]
        .astype(F32)
        .reshape(token_rows, KEY_VALUE_HEADS, HEAD_SIZE)
    )
    value_slice = rows[:, query_span_width + key_value_width :].reshape(
        token_rows, KEY_VALUE_HEADS, HEAD_SIZE
    )
    rotated_query = rotate(query_part, cos_table, sin_table, 1.0).astype(BF)
    k_rot = rotate(key_slice, cos_table, sin_table, 1.0).astype(BF)
    capped = capped_scores(rotated_query, k_rot)
    log_total = jnp.log(jnp.sum(jnp.where(allowed, jnp.exp(capped), 0.0), axis=-1))
    weights_f = jnp.where(allowed, jnp.exp(capped - log_total[..., None]), 0.0)
    mixing_rows = product("kgts,skd->tkgd", weights_f.astype(BF), value_slice)
    mixing_rows = mixing_rows.astype(BF).reshape(token_rows, query_span_width)
    return (mixing_rows, (rotated_query, k_rot, value_slice, log_total))


def attention_backward(mixing_gradient, mixing_rows, saved, layout):
    rotated_query, k_rot, value_slice, log_total = saved
    token_rows = mixing_gradient.shape[0]
    heads_per_group = QUERY_HEADS // KEY_VALUE_HEADS
    allowed, cos_table, sin_table = layout
    capped = capped_scores(rotated_query, k_rot)
    weights_f = jnp.where(allowed, jnp.exp(capped - log_total[..., None]), 0.0)
    gradient_by_group = mixing_gradient.reshape(
        token_rows, KEY_VALUE_HEADS, heads_per_group, HEAD_SIZE
    )
    output_by_group = mixing_rows.reshape(token_rows, KEY_VALUE_HEADS, heads_per_group, HEAD_SIZE)
    row_delta = product("tkgd,tkgd->kgt", gradient_by_group, output_by_group)
    value_gradient = product("maew,emaq->wmq", weights_f.astype(BF), gradient_by_group)
    weight_grad = product("tkgd,skd->kgts", gradient_by_group, value_slice)
    score_gradient = (
        weights_f
        * (weight_grad - row_delta[..., None])
        * (1.0 - (capped / SOFT_CAP) ** 2)
        * HEAD_SIZE ** (-0.5)
    )
    score_gradient = score_gradient.astype(BF)
    query_gradient = product("kgts,skd->tkgd", score_gradient, k_rot).reshape(
        token_rows, QUERY_HEADS, HEAD_SIZE
    )
    key_gradient = product(
        "maew,emaq->wmq",
        score_gradient,
        rotated_query.reshape(token_rows, KEY_VALUE_HEADS, heads_per_group, HEAD_SIZE),
    )
    query_gradient = rotate(query_gradient, cos_table, sin_table, -1.0)
    key_gradient = rotate(key_gradient, cos_table, sin_table, -1.0)
    return jnp.concatenate(
        [
            query_gradient.reshape(token_rows, QUERY_HEADS * HEAD_SIZE),
            key_gradient.reshape(token_rows, KEY_VALUE_HEADS * HEAD_SIZE),
            value_gradient.reshape(token_rows, KEY_VALUE_HEADS * HEAD_SIZE),
        ],
        axis=1,
    ).astype(BF)


def inverse_rms(values):
    return lax.rsqrt(jnp.mean(values * values, axis=1, keepdims=True) + EPSILON)


def norm_back(grad_rows, unit_rows, scale_rows, gain):
    scaled = grad_rows * gain
    return scale_rows * (scaled - unit_rows * jnp.mean(scaled * unit_rows, axis=1, keepdims=True))


def thirds(values):
    high = lax.reduce_precision(values, 8, 7)
    rest = values - high
    middle = lax.reduce_precision(rest, 8, 7)
    return jnp.concatenate([high, middle, rest - middle], axis=0).astype(BF)


def join_thirds(rows):
    count = rows.shape[-2] // 3
    rows = rows.astype(F32)
    return rows[..., :count, :] + rows[..., count : 2 * count, :] + rows[..., 2 * count :, :]


def to_whole_rows(values, nx, extra=None):
    width = values.shape[1]
    parts = values.astype(BF).reshape(nx, -1, width)
    if extra is not None:
        parts = jnp.concatenate(
            [parts, jnp.broadcast_to(extra[None], (nx,) + extra.shape)], axis=1
        )
    parts = lax.all_to_all(parts, "gx", split_axis=0, concat_axis=0, tiled=True)
    return parts.transpose(1, 0, 2).reshape(-1, nx * width)


def to_width_blocks(values, nx, extra=None):
    values = values.astype(BF)
    if extra is not None:
        values = jnp.concatenate([values, extra], axis=0)
    rows, whole = values.shape
    parts = values.reshape(rows, nx, whole // nx).transpose(1, 0, 2)
    return lax.all_to_all(parts, "gx", split_axis=0, concat_axis=0, tiled=True)


def flip(index, mask):
    return index + mask - 2 * mask * ((index // mask) % 2)


def flip_all(index, masks):
    bit = 1
    while bit <= masks:
        if masks & bit:
            index = flip(index, bit)
        bit *= 2
    return index


def greet(me, bits, lanes=0):
    barrier = pltpu.get_barrier_semaphore()
    for bit in bits:
        pl.semaphore_signal(barrier, inc=1, device_id={"gy": flip(me, bit)}, device_id_type=MESH)
    for d in range(1, lanes):
        other = (lax.axis_index("gx") + d) % lanes
        pl.semaphore_signal(barrier, inc=1, device_id={"gx": other}, device_id_type=MESH)
    pl.semaphore_wait(barrier, len(bits) + max(lanes - 1, 0))


def bit_orders(size):
    bits = []
    bit = 2
    while bit < size:
        bits.append(bit)
        bit *= 2
    return (bits + [1], bits[::-1] + [1])


def lay_out(rows_ref, blocks_ref, strip):
    lanes, count, width = blocks_ref.shape

    @pl.loop(0, count // strip)
    def _(i):
        rows = pl.ds(i * strip, strip)
        for k in range(lanes):
            rows_ref[rows, k * width : (k + 1) * width] = blocks_ref[k, rows].astype(F32)


def cut_up(blocks_ref, rows_ref, strip):
    lanes, count, width = blocks_ref.shape

    @pl.loop(0, count // strip)
    def _(i):
        rows = pl.ds(i * strip, strip)
        for k in range(lanes):
            blocks_ref[k, rows] = rows_ref[rows, k * width : (k + 1) * width].astype(BF)


def swap_start(lanes, side_ref, there_ref, sems):
    me = lax.axis_index("gx")
    own, send_sem, recv_sem = sems
    made = [pltpu.make_async_copy(side_ref.at[me], there_ref.at[me], own)]
    for d in range(1, lanes):
        other = (me + d) % lanes
        made.append(
            pltpu.make_async_remote_copy(
                src_ref=side_ref.at[other],
                dst_ref=there_ref.at[me],
                send_sem=send_sem.at[d],
                recv_sem=recv_sem.at[d],
                device_id={"gx": other},
                device_id_type=MESH,
            )
        )
    for copy in made:
        copy.start()
    return made


def swap_sems(lanes):
    return [
        pltpu.SemaphoreType.DMA,
        pltpu.SemaphoreType.DMA((lanes,)),
        pltpu.SemaphoreType.DMA((lanes,)),
    ]


def spread_kernel(size, lanes, *refs):
    if lanes:
        own_ref, rows_ref, all_ref, there_ref, local_sem, send_sem, recv_sem, *rest = refs
        side_ref, *sems = rest
    else:
        own_ref, all_ref, local_sem, send_sem, recv_sem = refs
    me = lax.axis_index("gy")
    orders = bit_orders(size)
    half = own_ref.shape[0] // 2
    greet(me, orders[0], lanes)
    keep = pltpu.make_async_copy(own_ref, all_ref.at[me], local_sem)
    keep.start()
    copies = {}
    arrival = {}

    def copy(h, bit, r):
        n = len(copies)
        rows = pl.ds(h * half, half)
        where = flip_all(me, r)
        source = own_ref.at[rows] if r == 0 else all_ref.at[where, rows]
        made = pltpu.make_async_remote_copy(
            src_ref=source,
            dst_ref=all_ref.at[where, rows],
            send_sem=send_sem.at[n],
            recv_sem=recv_sem.at[n],
            device_id={"gy": flip(me, bit)},
            device_id_type=MESH,
        )
        copies[h, bit, r] = made
        arrival[h, r ^ bit] = made
        made.start()

    for step in range(len(orders[0])):
        for h in range(2):
            copy(h, orders[h][step], 0)
    swapped = []
    if lanes:
        cut_up(side_ref, rows_ref, 16)
        swapped = swap_start(lanes, side_ref, there_ref, sems)
    landed = set()

    def land(h, r):
        if (h, r) not in landed:
            landed.add((h, r))
            arrival[h, r].wait_recv()

    held = [[0], [0]]
    for step in range(len(orders[0])):
        for h in range(2):
            bit = orders[h][step]
            for r in held[h]:
                if r:
                    land(h, r)
                    copy(h, bit, r)
        for h in range(2):
            held[h] = held[h] + [r ^ orders[h][step] for r in held[h]]
    for h in range(2):
        for r in range(1, size):
            land(h, r)
    for made in copies.values():
        made.wait_send()
    for copy in [keep] + swapped:
        copy.wait()


def spread(values, side=None):
    size = lax.axis_size("gy")
    values = values.astype(BF)
    rows, width = values.shape
    count = 2 * (size - 1)
    sides = [] if side is None else [side]
    lanes = 0 if side is None else lax.axis_size("gx")
    blocks = (lanes, rows, width // max(lanes, 1))
    space = pl.BlockSpec(memory_space=pltpu.VMEM)
    out = pl.pallas_call(
        functools.partial(spread_kernel, size, lanes),
        out_shape=[jax.ShapeDtypeStruct((size, rows, width), values.dtype)]
        + [jax.ShapeDtypeStruct(blocks, BF) for v in sides],
        in_specs=[space] * (1 + len(sides)),
        out_specs=[pl.BlockSpec(memory_space=pltpu.HBM)] * (1 + len(sides)),
        scratch_shapes=[
            pltpu.SemaphoreType.DMA,
            pltpu.SemaphoreType.DMA((count,)),
            pltpu.SemaphoreType.DMA((count,)),
        ]
        + ([pltpu.VMEM(blocks, BF)] + swap_sems(lanes) if lanes else []),
        compiler_params=pltpu.CompilerParams(
            collective_id=4 if lanes else 0, has_side_effects=True, vmem_limit_bytes=32 << 20
        ),
        cost_estimate=pl.CostEstimate(
            flops=0, bytes_accessed=size * rows * width * 16, transcendentals=0
        ),
        name="spread",
    )(values, *sides)
    whole = out[0].reshape(size * rows, width)
    return (whole, out[1]) if lanes else whole


def settle_kernel(size, lanes, *refs):
    if lanes:
        parts_ref, side_ref, sum_ref, rows_ref, came, kept, send_sem, recv_sem, *rest = refs
        there_ref, *sems = rest
    else:
        parts_ref, sum_ref, came, kept, send_sem, recv_sem = refs
    me = lax.axis_index("gy")
    orders = tuple(order[::-1] for order in bit_orders(size))
    half = sum_ref.shape[0] // 2
    strip = 16
    greet(me, orders[0], lanes)
    swapped = swap_start(lanes, side_ref, there_ref, sems) if lanes else []
    slot = {}
    for h in range(2):
        held = list(range(size))
        for step, bit in enumerate(orders[h]):
            held = [r for r in held if not r & bit]
            for r in held:
                slot[h, step, r] = len(slot)
    copies = {}

    def view(h, step, r):
        if step == 0:
            return parts_ref.at[flip_all(me, r), pl.ds(h * half, half)]
        return kept.at[h, r]

    def send(h, step):
        bit = orders[h][step]
        gone = set()
        for b in orders[h][:step]:
            gone.add(b)
        for r in range(size):
            if r & bit and not any(r & b for b in gone):
                n = slot[h, step, r ^ bit]
                made = pltpu.make_async_remote_copy(
                    src_ref=view(h, step, r),
                    dst_ref=came.at[n],
                    send_sem=send_sem.at[n],
                    recv_sem=recv_sem.at[n],
                    device_id={"gy": flip(me, bit)},
                    device_id_type=MESH,
                )
                copies[h, step, r ^ bit] = made
                made.start()

    def gather(h, step, r, last):
        n = slot[h, step, r]
        copies[h, step, r].wait_recv()

        @pl.loop(0, half // strip)
        def _(i):
            rows = pl.ds(i * strip, strip)
            total = view(h, step, r)[rows].astype(F32) + came[n, rows].astype(F32)
            if last:
                sum_ref[pl.ds(h * half + i * strip, strip)] = total
            else:
                kept[h, r, rows] = total.astype(BF)

    steps = len(orders[0])
    for h in range(2):
        send(h, 0)
    for step in range(steps):
        if lanes and step == steps - 1:
            for copy in swapped:
                copy.wait()
            lay_out(rows_ref, there_ref, strip)
        for h in range(2):
            bits = orders[h][: step + 1]
            later = orders[h][step + 1] if step + 1 < steps else 0
            left = [r for r in range(size) if not any(r & b for b in bits)]
            for r in left:
                if r & later:
                    gather(h, step, r, False)
            if later:
                send(h, step + 1)
            for r in left:
                if not r & later:
                    gather(h, step, r, step == steps - 1)
    for made in copies.values():
        made.wait_send()


def settle(parts, side=None):
    size = lax.axis_size("gy")
    parts = parts.astype(BF)
    total, width = parts.shape
    rows = total // size
    count = 2 * (size - 1)
    sides = [] if side is None else [side]
    lanes = 0 if side is None else side.shape[0]
    space = pl.BlockSpec(memory_space=pltpu.VMEM)
    out = pl.pallas_call(
        functools.partial(settle_kernel, size, lanes),
        out_shape=[jax.ShapeDtypeStruct((rows, width), F32)]
        + [jax.ShapeDtypeStruct((rows, width), F32) for v in sides],
        in_specs=[space] * (1 + len(sides)),
        out_specs=[space] * (1 + len(sides)),
        scratch_shapes=[
            pltpu.VMEM((count, rows // 2, width), BF),
            pltpu.VMEM((2, size, rows // 2, width), BF),
            pltpu.SemaphoreType.DMA((count,)),
            pltpu.SemaphoreType.DMA((count,)),
        ]
        + ([pltpu.VMEM(side.shape, side.dtype)] + swap_sems(lanes) if lanes else []),
        compiler_params=pltpu.CompilerParams(
            collective_id=5 if lanes else 1, has_side_effects=True, vmem_limit_bytes=32 << 20
        ),
        cost_estimate=pl.CostEstimate(
            flops=0, bytes_accessed=total * width * 16, transcendentals=0
        ),
        name="settle",
    )(parts.reshape(size, rows, width), *sides)
    return out if lanes else out[0]


def tally_kernel(size, own_ref, sum_ref, came, send_sem, recv_sem):
    me = lax.axis_index("gy")
    barrier = pltpu.get_barrier_semaphore()
    for d in range(1, size):
        pl.semaphore_signal(
            barrier, inc=1, device_id={"gy": (me + d) % size}, device_id_type=MESH
        )
    pl.semaphore_wait(barrier, size - 1)
    copies = []
    for d in range(1, size):
        made = pltpu.make_async_remote_copy(
            src_ref=own_ref,
            dst_ref=came.at[d],
            send_sem=send_sem.at[d],
            recv_sem=recv_sem.at[d],
            device_id={"gy": (me + d) % size},
            device_id_type=MESH,
        )
        made.start()
        copies.append(made)
    total = own_ref[...]
    for d in range(1, size):
        copies[d - 1].wait_recv()
        total = total + came[d]
    sum_ref[...] = total
    for made in copies:
        made.wait_send()


def tally(values, size):
    return pl.pallas_call(
        functools.partial(tally_kernel, size),
        out_shape=jax.ShapeDtypeStruct(values.shape, F32),
        in_specs=[pl.BlockSpec(memory_space=pltpu.VMEM)],
        out_specs=pl.BlockSpec(memory_space=pltpu.VMEM),
        scratch_shapes=[
            pltpu.VMEM((size,) + values.shape, F32),
            pltpu.SemaphoreType.DMA((size,)),
            pltpu.SemaphoreType.DMA((size,)),
        ],
        compiler_params=pltpu.CompilerParams(collective_id=2, has_side_effects=True),
        name="tally",
    )(values)


def make_shards(nx, ny):
    blocks = [((b // ny) * ny + b % ny, (b % nx) * ny + b // nx) for b in range(nx * ny)]

    def shards(
        inputs,
        segment_ids,
        qkv_weight,
        out_weight,
        gate_up_weight,
        down_weight,
        first_gain,
        second_gain,
        third_gain,
        fourth_gain,
        cotangent,
    ):
        width = inputs.shape[1]

        gains = thirds(jnp.stack([first_gain, second_gain, third_gain, fourth_gain]))
        rows_in = to_whole_rows(inputs, nx, gains)
        rows_in, down_weight, segment_ids = lax.optimization_barrier(
            (rows_in, down_weight, segment_ids)
        )
        own = inputs.shape[0] // nx
        heads = qkv_weight.shape[1]
        x_rows = rows_in[:own].astype(F32)
        gains = join_thirds(rows_in[own:])[:, None, :]
        both_w = lax.all_gather(
            jnp.concatenate([qkv_weight, out_weight.T], axis=1), "gx", axis=0, tiled=True
        )
        gate_up_w = lax.all_gather(gate_up_weight, "gx", axis=0, tiled=True)
        down_w = lax.all_gather(down_weight.T, "gx", axis=0, tiled=True)
        qkv_w, out_w = both_w[:, :heads], both_w[:, heads:]

        segment_row = lax.ppermute(segment_ids[0], ("gx", "gy"), blocks)
        position, allowed = block_layout(segment_row)
        layout = (allowed,) + rope_tables(position)

        scale_one = inverse_rms(x_rows)
        unit_one = x_rows * scale_one
        normed_one = spread(unit_one * gains[0])
        rows = product("td,dc->tc", normed_one, qkv_w).astype(BF)
        rows = lax.all_to_all(rows, "gy", split_axis=0, concat_axis=1, tiled=True)
        mixing_rows, saved = attention_forward(rows, layout)
        mixed = lax.all_to_all(mixing_rows, "gy", split_axis=1, concat_axis=0, tiled=True)
        attn_branch = settle(product("tc,dc->td", mixed, out_w))
        scale_two = inverse_rms(attn_branch)
        unit_two = attn_branch * scale_two
        attn_term = unit_two * gains[1]
        middle = x_rows + attn_term
        scale_three = inverse_rms(middle)
        unit_three = middle * scale_three
        normed_two = spread(unit_three * gains[2])
        pre_gate = product("td,df->tf", normed_two, gate_up_w[:, 0, :])
        up_part = product("td,df->tf", normed_two, gate_up_w[:, 1, :])
        value, slope = gelu_parts(pre_gate)
        hidden = (value * up_part).astype(BF)
        ff_branch, cot_rows = settle(
            product("tf,df->td", hidden, down_w), cotangent.astype(BF).reshape(nx, own, width)
        )
        scale_four = inverse_rms(ff_branch)
        unit_four = ff_branch * scale_four
        ff_grad, delta = spread(
            norm_back(cot_rows, unit_four, scale_four, gains[3]),
            attn_term + unit_four * gains[3],
        )
        outputs = inputs + delta.reshape(inputs.shape).astype(F32)

        down_sum = product("td,tf->df", ff_grad, hidden).astype(BF)
        down_sum, ff_grad = lax.optimization_barrier((down_sum, ff_grad))
        down_done = lax.psum_scatter(down_sum, "gx", scatter_dimension=0, tiled=True)
        hidden_grad = product("td,df->tf", ff_grad, down_w)
        gate_grad = (hidden_grad * up_part * slope).astype(BF)
        up_grad = (hidden_grad * value).astype(BF)
        gate_up_sum = jnp.stack(
            [
                product("td,tf->df", normed_two, gate_grad).astype(BF),
                product("td,tf->df", normed_two, up_grad).astype(BF),
            ],
            axis=1,
        )
        gate_up_sum, gate_grad, up_grad = lax.optimization_barrier(
            (gate_up_sum, gate_grad, up_grad)
        )
        gate_up_done = lax.psum_scatter(gate_up_sum, "gx", scatter_dimension=0, tiled=True)
        normed_two_grad = settle(
            product("tf,df->td", gate_grad, gate_up_w[:, 0, :])
            + product("tf,df->td", up_grad, gate_up_w[:, 1, :])
        )
        middle_delta = norm_back(normed_two_grad, unit_three, scale_three, gains[2])
        middle_grad = cot_rows + middle_delta
        branch_grad = spread(norm_back(middle_grad, unit_two, scale_two, gains[1]))
        out_sum = product("td,tc->dc", branch_grad, mixed).astype(BF)
        mixing_gradient = product("td,dc->tc", branch_grad, out_w).astype(BF)
        mixing_gradient = lax.all_to_all(
            mixing_gradient, "gy", split_axis=0, concat_axis=1, tiled=True
        )
        qkv_grad_rows = attention_backward(mixing_gradient, mixing_rows, saved, layout)
        qkv_grad_rows, down_done = lax.optimization_barrier((qkv_grad_rows, down_done))
        qkv_grad_rows = lax.all_to_all(
            qkv_grad_rows, "gy", split_axis=1, concat_axis=0, tiled=True
        )
        normed_one_grad = settle(product("tc,dc->td", qkv_grad_rows, qkv_w))
        both_sum = jnp.concatenate(
            [product("td,tc->dc", normed_one, qkv_grad_rows).astype(BF), out_sum], axis=1
        )
        terms = jnp.stack(
            [
                jnp.sum(normed_one_grad * unit_one, axis=0),
                jnp.sum(middle_grad * unit_two, axis=0),
                jnp.sum(normed_two_grad * unit_three, axis=0),
                jnp.sum(cot_rows * unit_four, axis=0),
            ]
        )
        delta = to_width_blocks(
            middle_delta + norm_back(normed_one_grad, unit_one, scale_one, gains[0]),
            nx,
            thirds(tally(terms, ny)),
        )
        down_grad = down_done.astype(F32).T
        gate_up_done, both_sum, delta, down_grad = lax.optimization_barrier(
            (gate_up_done, both_sum, delta, down_grad)
        )
        both_done = lax.psum_scatter(both_sum, "gx", scatter_dimension=0, tiled=True)
        gate_up_grad = gate_up_done.astype(F32)
        input_grad = cotangent + delta[:, :own].reshape(inputs.shape).astype(F32)
        terms = jnp.sum(join_thirds(delta[:, own:]), axis=0)
        qkv_grad = both_done[:, :heads].astype(F32)
        out_grad = both_done[:, heads:].astype(F32).T
        return (outputs, input_grad, qkv_grad, out_grad, gate_up_grad, down_grad) + tuple(
            terms[i] for i in range(4)
        )

    return shards


def solution(mesh):
    placed = (
        P("gy", "gx"),
        P(("gx", "gy"), None),
        P("gx", "gy"),
        P("gy", "gx"),
        P("gx", None, "gy"),
        P("gy", "gx"),
        P("gx"),
        P("gx"),
        P("gx"),
        P("gx"),
        P("gy", "gx"),
    )
    return jax.shard_map(
        make_shards(mesh.shape["gx"], mesh.shape["gy"]),
        mesh=mesh,
        in_specs=placed,
        out_specs=(
            P("gy", "gx"),
            P("gy", "gx"),
            P("gx", "gy"),
            P("gy", "gx"),
            P("gx", None, "gy"),
            P("gy", "gx"),
            P("gx"),
            P("gx"),
            P("gx"),
            P("gx"),
        ),
        check_vma=False,
    )
```

```python
import functools
import math

import jax
import jax.numpy as jnp
from jax import lax
from jax.experimental import pallas as pl
from jax.experimental.layout import Layout, with_layout_constraint
from jax.experimental.pallas import tpu as pltpu
from jax.sharding import PartitionSpec as P

QUERY_HEADS = 8
KEY_VALUE_HEADS = 4
HEAD_SIZE = 256


EPSILON = 1e-06
SOFT_CAP = 50.0
GELU_COEF = 0.7978845608028654
CUBIC_COEF = 0.044715

BF = jnp.bfloat16
F32 = jnp.float32
MESH = pl.DeviceIdType.MESH
PARTS = 4


def product(form, left, right):
    return jnp.einsum(form, left, right, preferred_element_type=F32)


def gelu_parts(pre_gate):
    inner_arg = GELU_COEF * (pre_gate + CUBIC_COEF * pre_gate * pre_gate * pre_gate)
    tanh_value = jnp.tanh(inner_arg)
    activated = 0.5 * pre_gate * (1.0 + tanh_value)
    derivative = 0.5 * (1.0 + tanh_value) + 0.5 * pre_gate * (
        1.0 - tanh_value * tanh_value
    ) * GELU_COEF * (1.0 + 3.0 * CUBIC_COEF * pre_gate * pre_gate)
    return (activated, derivative)


def block_layout(segment_row):
    length_total = segment_row.shape[0]
    places = jnp.arange(length_total, dtype=jnp.int32)
    same_doc = segment_row[:, None] == segment_row[None, :]
    starts = jnp.min(jnp.where(same_doc, places[None, :], length_total), axis=1)
    allowed = jnp.logical_and(same_doc, places[None, :] <= places[:, None])
    return (places - starts, allowed)


def rope_tables(position):
    half_dim = HEAD_SIZE // 2
    freq_steps = jnp.arange(half_dim, dtype=F32)
    frequency = jnp.exp(freq_steps * (-2.0 * math.log(10000.0) / HEAD_SIZE))
    angles = position.astype(F32)[:, None] * frequency[None, :]
    return (jnp.cos(angles)[:, None, :], jnp.sin(angles)[:, None, :])


def rotate(values, cos_table, sin_table, direction):
    half_dim = values.shape[-1] // 2
    leading = values[..., :half_dim]
    trailing = values[..., half_dim:]
    return jnp.concatenate(
        [
            leading * cos_table - direction * trailing * sin_table,
            trailing * cos_table + direction * leading * sin_table,
        ],
        axis=-1,
    )


def capped_scores(rotated_query, k_rot):
    token_rows = rotated_query.shape[0]
    query_groups = rotated_query.reshape(
        token_rows, KEY_VALUE_HEADS, QUERY_HEADS // KEY_VALUE_HEADS, HEAD_SIZE
    )
    raw_scores = product("tkgd,skd->kgts", query_groups, k_rot) * HEAD_SIZE ** (-0.5)
    return SOFT_CAP * jnp.tanh(raw_scores / SOFT_CAP)


def attention_forward(rows, layout):
    token_rows = rows.shape[0]
    query_span_width = QUERY_HEADS * HEAD_SIZE
    key_value_width = KEY_VALUE_HEADS * HEAD_SIZE
    allowed, cos_table, sin_table = layout
    query_part = (
        rows[:, :query_span_width].astype(F32).reshape(token_rows, QUERY_HEADS, HEAD_SIZE)
    )
    key_slice = (
        rows[:, query_span_width : query_span_width + key_value_width]
        .astype(F32)
        .reshape(token_rows, KEY_VALUE_HEADS, HEAD_SIZE)
    )
    value_slice = rows[:, query_span_width + key_value_width :].reshape(
        token_rows, KEY_VALUE_HEADS, HEAD_SIZE
    )
    rotated_query = rotate(query_part, cos_table, sin_table, 1.0).astype(BF)
    k_rot = rotate(key_slice, cos_table, sin_table, 1.0).astype(BF)
    capped = capped_scores(rotated_query, k_rot)
    log_total = jnp.log(jnp.sum(jnp.where(allowed, jnp.exp(capped), 0.0), axis=-1))
    weights_f = jnp.where(allowed, jnp.exp(capped - log_total[..., None]), 0.0)
    mixing_rows = product("kgts,skd->tkgd", weights_f.astype(BF), value_slice)
    mixing_rows = mixing_rows.astype(BF).reshape(token_rows, query_span_width)
    return (mixing_rows, (rotated_query, k_rot, value_slice, log_total))


def attention_backward(mixing_gradient, mixing_rows, saved, layout):
    rotated_query, k_rot, value_slice, log_total = saved
    token_rows = mixing_gradient.shape[0]
    heads_per_group = QUERY_HEADS // KEY_VALUE_HEADS
    allowed, cos_table, sin_table = layout
    capped = capped_scores(rotated_query, k_rot)
    weights_f = jnp.where(allowed, jnp.exp(capped - log_total[..., None]), 0.0)
    gradient_by_group = mixing_gradient.reshape(
        token_rows, KEY_VALUE_HEADS, heads_per_group, HEAD_SIZE
    )
    output_by_group = mixing_rows.reshape(token_rows, KEY_VALUE_HEADS, heads_per_group, HEAD_SIZE)
    row_delta = product("tkgd,tkgd->kgt", gradient_by_group, output_by_group)
    value_gradient = product("maew,emaq->wmq", weights_f.astype(BF), gradient_by_group)
    weight_grad = product("tkgd,skd->kgts", gradient_by_group, value_slice)
    score_gradient = (
        weights_f
        * (weight_grad - row_delta[..., None])
        * (1.0 - (capped / SOFT_CAP) ** 2)
        * HEAD_SIZE ** (-0.5)
    )
    score_gradient = score_gradient.astype(BF)
    query_gradient = product("kgts,skd->tkgd", score_gradient, k_rot).reshape(
        token_rows, QUERY_HEADS, HEAD_SIZE
    )
    key_gradient = product(
        "maew,emaq->wmq",
        score_gradient,
        rotated_query.reshape(token_rows, KEY_VALUE_HEADS, heads_per_group, HEAD_SIZE),
    )
    query_gradient = rotate(query_gradient, cos_table, sin_table, -1.0)
    key_gradient = rotate(key_gradient, cos_table, sin_table, -1.0)
    return jnp.concatenate(
        [
            query_gradient.reshape(token_rows, QUERY_HEADS * HEAD_SIZE),
            key_gradient.reshape(token_rows, KEY_VALUE_HEADS * HEAD_SIZE),
            value_gradient.reshape(token_rows, KEY_VALUE_HEADS * HEAD_SIZE),
        ],
        axis=1,
    ).astype(BF)


def inverse_rms(values):
    return lax.rsqrt(jnp.mean(values * values, axis=1, keepdims=True) + EPSILON)


def norm_back(grad_rows, unit_rows, scale_rows, gain):
    scaled = grad_rows * gain
    return scale_rows * (scaled - unit_rows * jnp.mean(scaled * unit_rows, axis=1, keepdims=True))


def thirds(values):
    high = lax.reduce_precision(values, 8, 7)
    rest = values - high
    middle = lax.reduce_precision(rest, 8, 7)
    return jnp.concatenate([high, middle, rest - middle], axis=0).astype(BF)


def join_thirds(rows):
    count = rows.shape[-2] // 3
    rows = rows.astype(F32)
    return rows[..., :count, :] + rows[..., count : 2 * count, :] + rows[..., 2 * count :, :]


def to_whole_rows(values, nx, extra=None):
    width = values.shape[1]
    parts = values.astype(BF).reshape(nx, -1, width)
    if extra is not None:
        parts = jnp.concatenate(
            [parts, jnp.broadcast_to(extra[None], (nx,) + extra.shape)], axis=1
        )
    parts = lax.all_to_all(parts, "gx", split_axis=0, concat_axis=0, tiled=True)
    return parts.transpose(1, 0, 2).reshape(-1, nx * width)


def to_width_blocks(values, nx, extra=None):
    values = values.astype(BF)
    if extra is not None:
        values = jnp.concatenate([values, extra], axis=0)
    rows, whole = values.shape
    parts = values.reshape(rows, nx, whole // nx).transpose(1, 0, 2)
    return lax.all_to_all(parts, "gx", split_axis=0, concat_axis=0, tiled=True)


def flip(index, mask):
    return index + mask - 2 * mask * ((index // mask) % 2)


def flip_all(index, masks):
    bit = 1
    while bit <= masks:
        if masks & bit:
            index = flip(index, bit)
        bit *= 2
    return index


def greet(me, bits, lanes=0):
    barrier = pltpu.get_barrier_semaphore()
    for bit in bits:
        pl.semaphore_signal(barrier, inc=1, device_id={"gy": flip(me, bit)}, device_id_type=MESH)
    for d in range(1, lanes):
        other = (lax.axis_index("gx") + d) % lanes
        pl.semaphore_signal(barrier, inc=1, device_id={"gx": other}, device_id_type=MESH)
    pl.semaphore_wait(barrier, len(bits) + max(lanes - 1, 0))


def bit_orders(size):
    bits = []
    bit = 2
    while bit < size:
        bits.append(bit)
        bit *= 2
    return (bits + [1], bits[::-1] + [1])


def lay_out(rows_ref, blocks_ref, strip):
    lanes, count, width = blocks_ref.shape

    @pl.loop(0, count // strip)
    def _(i):
        rows = pl.ds(i * strip, strip)
        for k in range(lanes):
            rows_ref[rows, k * width : (k + 1) * width] = blocks_ref[k, rows].astype(F32)


def cut_up(blocks_ref, rows_ref, strip):
    lanes, count, width = blocks_ref.shape

    @pl.loop(0, count // strip)
    def _(i):
        rows = pl.ds(i * strip, strip)
        for k in range(lanes):
            blocks_ref[k, rows] = rows_ref[rows, k * width : (k + 1) * width].astype(BF)


def swap_start(lanes, side_ref, there_ref, sems):
    me = lax.axis_index("gx")
    own, send_sem, recv_sem = sems
    made = [pltpu.make_async_copy(side_ref.at[me], there_ref.at[me], own)]
    for d in range(1, lanes):
        other = (me + d) % lanes
        made.append(
            pltpu.make_async_remote_copy(
                src_ref=side_ref.at[other],
                dst_ref=there_ref.at[me],
                send_sem=send_sem.at[d],
                recv_sem=recv_sem.at[d],
                device_id={"gx": other},
                device_id_type=MESH,
            )
        )
    for copy in made:
        copy.start()
    return made


def swap_sems(lanes):
    return [
        pltpu.SemaphoreType.DMA,
        pltpu.SemaphoreType.DMA((lanes,)),
        pltpu.SemaphoreType.DMA((lanes,)),
    ]


def spread_kernel(size, lanes, *refs):
    if lanes:
        own_ref, rows_ref, all_ref, there_ref, local_sem, send_sem, recv_sem, *rest = refs
        side_ref, *sems = rest
    else:
        own_ref, all_ref, local_sem, send_sem, recv_sem = refs
    me = lax.axis_index("gy")
    orders = bit_orders(size)
    half = own_ref.shape[0] // 2
    greet(me, orders[0], lanes)
    keep = pltpu.make_async_copy(own_ref, all_ref.at[me], local_sem)
    keep.start()
    copies = {}
    arrival = {}

    def copy(h, bit, r):
        n = len(copies)
        rows = pl.ds(h * half, half)
        where = flip_all(me, r)
        source = own_ref.at[rows] if r == 0 else all_ref.at[where, rows]
        made = pltpu.make_async_remote_copy(
            src_ref=source,
            dst_ref=all_ref.at[where, rows],
            send_sem=send_sem.at[n],
            recv_sem=recv_sem.at[n],
            device_id={"gy": flip(me, bit)},
            device_id_type=MESH,
        )
        copies[h, bit, r] = made
        arrival[h, r ^ bit] = made
        made.start()

    for step in range(len(orders[0])):
        for h in range(2):
            copy(h, orders[h][step], 0)
    swapped = []
    if lanes:
        cut_up(side_ref, rows_ref, 16)
        swapped = swap_start(lanes, side_ref, there_ref, sems)
    landed = set()

    def land(h, r):
        if (h, r) not in landed:
            landed.add((h, r))
            arrival[h, r].wait_recv()

    held = [[0], [0]]
    for step in range(len(orders[0])):
        for h in range(2):
            bit = orders[h][step]
            for r in held[h]:
                if r:
                    land(h, r)
                    copy(h, bit, r)
        for h in range(2):
            held[h] = held[h] + [r ^ orders[h][step] for r in held[h]]
    for h in range(2):
        for r in range(1, size):
            land(h, r)
    for made in copies.values():
        made.wait_send()
    for copy in [keep] + swapped:
        copy.wait()


def spread(values, side=None):
    size = lax.axis_size("gy")
    values = values.astype(BF)
    rows, width = values.shape
    count = 2 * (size - 1)
    sides = [] if side is None else [side]
    lanes = 0 if side is None else lax.axis_size("gx")
    blocks = (lanes, rows, width // max(lanes, 1))
    space = pl.BlockSpec(memory_space=pltpu.VMEM)
    out = pl.pallas_call(
        functools.partial(spread_kernel, size, lanes),
        out_shape=[jax.ShapeDtypeStruct((size, rows, width), values.dtype)]
        + [jax.ShapeDtypeStruct(blocks, BF) for v in sides],
        in_specs=[space] * (1 + len(sides)),
        out_specs=[pl.BlockSpec(memory_space=pltpu.HBM)] * (1 + len(sides)),
        scratch_shapes=[
            pltpu.SemaphoreType.DMA,
            pltpu.SemaphoreType.DMA((count,)),
            pltpu.SemaphoreType.DMA((count,)),
        ]
        + ([pltpu.VMEM(blocks, BF)] + swap_sems(lanes) if lanes else []),
        compiler_params=pltpu.CompilerParams(
            collective_id=4 if lanes else 0, has_side_effects=True, vmem_limit_bytes=32 << 20
        ),
        cost_estimate=pl.CostEstimate(
            flops=0, bytes_accessed=size * rows * width * 16, transcendentals=0
        ),
        name="spread",
    )(values, *sides)
    whole = out[0].reshape(size * rows, width)
    return (whole, out[1]) if lanes else whole


def settle_kernel(size, lanes, *refs):
    if lanes:
        parts_ref, side_ref, sum_ref, rows_ref, came, kept, send_sem, recv_sem, *rest = refs
        there_ref, *sems = rest
    else:
        parts_ref, sum_ref, came, kept, send_sem, recv_sem = refs
    me = lax.axis_index("gy")
    orders = tuple(order[::-1] for order in bit_orders(size)) * (PARTS // 2)
    half = sum_ref.shape[0] // PARTS
    strip = 16
    greet(me, orders[0], lanes)
    swapped = swap_start(lanes, side_ref, there_ref, sems) if lanes else []
    slot = {}
    for h in range(PARTS):
        held = list(range(size))
        for step, bit in enumerate(orders[h]):
            held = [r for r in held if not r & bit]
            for r in held:
                slot[h, step, r] = len(slot)
    copies = {}

    def view(h, step, r):
        if step == 0:
            return parts_ref.at[flip_all(me, r), pl.ds(h * half, half)]
        return kept.at[h, r]

    def send(h, step):
        bit = orders[h][step]
        gone = set()
        for b in orders[h][:step]:
            gone.add(b)
        for r in range(size):
            if r & bit and not any(r & b for b in gone):
                n = slot[h, step, r ^ bit]
                made = pltpu.make_async_remote_copy(
                    src_ref=view(h, step, r),
                    dst_ref=came.at[n],
                    send_sem=send_sem.at[n],
                    recv_sem=recv_sem.at[n],
                    device_id={"gy": flip(me, bit)},
                    device_id_type=MESH,
                )
                copies[h, step, r ^ bit] = made
                made.start()

    def gather(h, step, r, last):
        n = slot[h, step, r]
        copies[h, step, r].wait_recv()

        @pl.loop(0, half // strip)
        def _(i):
            rows = pl.ds(i * strip, strip)
            total = view(h, step, r)[rows].astype(F32) + came[n, rows].astype(F32)
            if last:
                sum_ref[pl.ds(h * half + i * strip, strip)] = total
            else:
                kept[h, r, rows] = total.astype(BF)

    steps = len(orders[0])
    for h in range(PARTS):
        send(h, 0)
    for step in range(steps):
        if lanes and step == steps - 1:
            for copy in swapped:
                copy.wait()
            lay_out(rows_ref, there_ref, strip)
        for h in range(PARTS):
            bits = orders[h][: step + 1]
            later = orders[h][step + 1] if step + 1 < steps else 0
            left = [r for r in range(size) if not any(r & b for b in bits)]
            for r in left:
                if r & later:
                    gather(h, step, r, False)
            if later:
                send(h, step + 1)
            for r in left:
                if not r & later:
                    gather(h, step, r, step == steps - 1)
    for made in copies.values():
        made.wait_send()


def settle(parts, side=None):
    size = lax.axis_size("gy")
    parts = parts.astype(BF)
    total, width = parts.shape
    rows = total // size
    count = PARTS * (size - 1)
    sides = [] if side is None else [side]
    lanes = 0 if side is None else side.shape[0]
    space = pl.BlockSpec(memory_space=pltpu.VMEM)
    out = pl.pallas_call(
        functools.partial(settle_kernel, size, lanes),
        out_shape=[jax.ShapeDtypeStruct((rows, width), F32)]
        + [jax.ShapeDtypeStruct((rows, width), F32) for v in sides],
        in_specs=[space] * (1 + len(sides)),
        out_specs=[space] * (1 + len(sides)),
        scratch_shapes=[
            pltpu.VMEM((count, rows // PARTS, width), BF),
            pltpu.VMEM((PARTS, size, rows // PARTS, width), BF),
            pltpu.SemaphoreType.DMA((count,)),
            pltpu.SemaphoreType.DMA((count,)),
        ]
        + ([pltpu.VMEM(side.shape, side.dtype)] + swap_sems(lanes) if lanes else []),
        compiler_params=pltpu.CompilerParams(
            collective_id=5 if lanes else 1, has_side_effects=True, vmem_limit_bytes=32 << 20
        ),
        cost_estimate=pl.CostEstimate(
            flops=0, bytes_accessed=total * width * 16, transcendentals=0
        ),
        name="settle",
    )(parts.reshape(size, rows, width), *sides)
    return out if lanes else out[0]


def tally_kernel(size, own_ref, sum_ref, came, send_sem, recv_sem):
    me = lax.axis_index("gy")
    barrier = pltpu.get_barrier_semaphore()
    for d in range(1, size):
        pl.semaphore_signal(
            barrier, inc=1, device_id={"gy": (me + d) % size}, device_id_type=MESH
        )
    pl.semaphore_wait(barrier, size - 1)
    copies = []
    for d in range(1, size):
        made = pltpu.make_async_remote_copy(
            src_ref=own_ref,
            dst_ref=came.at[d],
            send_sem=send_sem.at[d],
            recv_sem=recv_sem.at[d],
            device_id={"gy": (me + d) % size},
            device_id_type=MESH,
        )
        made.start()
        copies.append(made)
    total = own_ref[...]
    for d in range(1, size):
        copies[d - 1].wait_recv()
        total = total + came[d]
    sum_ref[...] = total
    for made in copies:
        made.wait_send()


def tally(values, size):
    return pl.pallas_call(
        functools.partial(tally_kernel, size),
        out_shape=jax.ShapeDtypeStruct(values.shape, F32),
        in_specs=[pl.BlockSpec(memory_space=pltpu.VMEM)],
        out_specs=pl.BlockSpec(memory_space=pltpu.VMEM),
        scratch_shapes=[
            pltpu.VMEM((size,) + values.shape, F32),
            pltpu.SemaphoreType.DMA((size,)),
            pltpu.SemaphoreType.DMA((size,)),
        ],
        compiler_params=pltpu.CompilerParams(collective_id=2, has_side_effects=True),
        name="tally",
    )(values)


def make_shards(nx, ny):
    blocks = [((b // ny) * ny + b % ny, (b % nx) * ny + b // nx) for b in range(nx * ny)]

    def shards(
        inputs,
        segment_ids,
        qkv_weight,
        out_weight,
        gate_up_weight,
        down_weight,
        first_gain,
        second_gain,
        third_gain,
        fourth_gain,
        cotangent,
    ):
        width = inputs.shape[1]

        gains = thirds(jnp.stack([first_gain, second_gain, third_gain, fourth_gain]))
        rows_in = to_whole_rows(inputs, nx, gains)
        rows_in, down_weight, segment_ids = lax.optimization_barrier(
            (rows_in, down_weight, segment_ids)
        )
        own = inputs.shape[0] // nx
        heads = qkv_weight.shape[1]
        x_rows = rows_in[:own].astype(F32)
        gains = join_thirds(rows_in[own:])[:, None, :]
        both_w = lax.all_gather(
            jnp.concatenate([qkv_weight, out_weight.T], axis=1), "gx", axis=0, tiled=True
        )
        gate_up_w = lax.all_gather(gate_up_weight, "gx", axis=0, tiled=True)
        down_w = lax.all_gather(down_weight.T, "gx", axis=0, tiled=True)
        qkv_w, out_w = both_w[:, :heads], both_w[:, heads:]

        segment_row = lax.ppermute(segment_ids[0], ("gx", "gy"), blocks)
        position, allowed = block_layout(segment_row)
        layout = (allowed,) + rope_tables(position)

        scale_one = inverse_rms(x_rows)
        unit_one = x_rows * scale_one
        normed_one = spread(unit_one * gains[0])
        rows = product("td,dc->tc", normed_one, qkv_w).astype(BF)
        rows = lax.all_to_all(rows, "gy", split_axis=0, concat_axis=1, tiled=True)
        mixing_rows, saved = attention_forward(rows, layout)
        mixed = lax.all_to_all(mixing_rows, "gy", split_axis=1, concat_axis=0, tiled=True)
        attn_branch = settle(product("tc,dc->td", mixed, out_w))
        scale_two = inverse_rms(attn_branch)
        unit_two = attn_branch * scale_two
        attn_term = unit_two * gains[1]
        middle = x_rows + attn_term
        scale_three = inverse_rms(middle)
        unit_three = middle * scale_three
        normed_two = spread(unit_three * gains[2])
        pre_gate = product("td,df->tf", normed_two, gate_up_w[:, 0, :])
        up_part = product("td,df->tf", normed_two, gate_up_w[:, 1, :])
        value, slope = gelu_parts(pre_gate)
        hidden = (value * up_part).astype(BF)
        ff_branch, cot_rows = settle(
            product("tf,df->td", hidden, down_w), cotangent.astype(BF).reshape(nx, own, width)
        )
        scale_four = inverse_rms(ff_branch)
        unit_four = ff_branch * scale_four
        ff_grad, delta = spread(
            norm_back(cot_rows, unit_four, scale_four, gains[3]),
            attn_term + unit_four * gains[3],
        )
        outputs = inputs + delta.reshape(inputs.shape).astype(F32)

        down_sum = product("td,tf->df", ff_grad, hidden).astype(BF)
        down_sum, ff_grad = lax.optimization_barrier((down_sum, ff_grad))
        down_done = lax.psum_scatter(down_sum, "gx", scatter_dimension=0, tiled=True)
        hidden_grad = product("td,df->tf", ff_grad, down_w)
        gate_grad = (hidden_grad * up_part * slope).astype(BF)
        up_grad = (hidden_grad * value).astype(BF)
        gate_up_sum = jnp.stack(
            [
                product("td,tf->df", normed_two, gate_grad).astype(BF),
                product("td,tf->df", normed_two, up_grad).astype(BF),
            ],
            axis=1,
        )
        gate_up_sum, gate_grad, up_grad = lax.optimization_barrier(
            (gate_up_sum, gate_grad, up_grad)
        )
        gate_up_done = lax.psum_scatter(gate_up_sum, "gx", scatter_dimension=0, tiled=True)
        normed_two_grad = settle(
            product("tf,df->td", gate_grad, gate_up_w[:, 0, :])
            + product("tf,df->td", up_grad, gate_up_w[:, 1, :])
        )
        middle_delta = norm_back(normed_two_grad, unit_three, scale_three, gains[2])
        middle_grad = cot_rows + middle_delta
        branch_grad = spread(norm_back(middle_grad, unit_two, scale_two, gains[1]))
        out_sum = product("td,tc->dc", branch_grad, mixed).astype(BF)
        mixing_gradient = product("td,dc->tc", branch_grad, out_w).astype(BF)
        mixing_gradient = lax.all_to_all(
            mixing_gradient, "gy", split_axis=0, concat_axis=1, tiled=True
        )
        qkv_grad_rows = attention_backward(mixing_gradient, mixing_rows, saved, layout)
        qkv_grad_rows, down_done = lax.optimization_barrier((qkv_grad_rows, down_done))
        qkv_grad_rows = lax.all_to_all(
            qkv_grad_rows, "gy", split_axis=1, concat_axis=0, tiled=True
        )
        normed_one_grad = settle(product("tc,dc->td", qkv_grad_rows, qkv_w))
        both_sum = jnp.concatenate(
            [product("td,tc->dc", normed_one, qkv_grad_rows).astype(BF), out_sum], axis=1
        )
        terms = jnp.stack(
            [
                jnp.sum(normed_one_grad * unit_one, axis=0),
                jnp.sum(middle_grad * unit_two, axis=0),
                jnp.sum(normed_two_grad * unit_three, axis=0),
                jnp.sum(cot_rows * unit_four, axis=0),
            ]
        )
        delta = to_width_blocks(
            middle_delta + norm_back(normed_one_grad, unit_one, scale_one, gains[0]),
            nx,
            thirds(tally(terms, ny)),
        )
        down_grad = down_done.astype(F32).T
        both_sum = with_layout_constraint(both_sum, Layout((0, 1)))
        gate_up_done, both_sum, delta, down_grad = lax.optimization_barrier(
            (gate_up_done, both_sum, delta, down_grad)
        )
        both_done = lax.psum_scatter(both_sum, "gx", scatter_dimension=0, tiled=True)
        gate_up_grad = gate_up_done.astype(F32)
        input_grad = cotangent + delta[:, :own].reshape(inputs.shape).astype(F32)
        terms = jnp.sum(join_thirds(delta[:, own:]), axis=0)
        qkv_grad = both_done[:, :heads].astype(F32)
        out_grad = both_done[:, heads:].astype(F32).T
        return (outputs, input_grad, qkv_grad, out_grad, gate_up_grad, down_grad) + tuple(
            terms[i] for i in range(4)
        )

    return shards


def solution(mesh):
    placed = (
        P("gy", "gx"),
        P(("gx", "gy"), None),
        P("gx", "gy"),
        P("gy", "gx"),
        P("gx", None, "gy"),
        P("gy", "gx"),
        P("gx"),
        P("gx"),
        P("gx"),
        P("gx"),
        P("gy", "gx"),
    )
    return jax.shard_map(
        make_shards(mesh.shape["gx"], mesh.shape["gy"]),
        mesh=mesh,
        in_specs=placed,
        out_specs=(
            P("gy", "gx"),
            P("gy", "gx"),
            P("gx", "gy"),
            P("gy", "gx"),
            P("gx", None, "gy"),
            P("gy", "gx"),
            P("gx"),
            P("gx"),
            P("gx"),
            P("gx"),
        ),
        check_vma=False,
    )
```

```python
import functools
import math

import jax
import jax.numpy as jnp
from jax import lax
from jax.experimental import pallas as pl
from jax.experimental.layout import Layout, with_layout_constraint
from jax.experimental.pallas import tpu as pltpu
from jax.sharding import PartitionSpec as P

QUERY_HEADS = 8
KEY_VALUE_HEADS = 4
HEAD_SIZE = 256


EPSILON = 1e-06
SOFT_CAP = 50.0
GELU_COEF = 0.7978845608028654
CUBIC_COEF = 0.044715

BF = jnp.bfloat16
F32 = jnp.float32
MESH = pl.DeviceIdType.MESH
PARTS = 4


def product(form, left, right):
    return jnp.einsum(form, left, right, preferred_element_type=F32)


def gelu_parts(pre_gate):
    inner_arg = GELU_COEF * (pre_gate + CUBIC_COEF * pre_gate * pre_gate * pre_gate)
    tanh_value = jnp.tanh(inner_arg)
    activated = 0.5 * pre_gate * (1.0 + tanh_value)
    derivative = 0.5 * (1.0 + tanh_value) + 0.5 * pre_gate * (
        1.0 - tanh_value * tanh_value
    ) * GELU_COEF * (1.0 + 3.0 * CUBIC_COEF * pre_gate * pre_gate)
    return (activated, derivative)


def block_layout(segment_row):
    length_total = segment_row.shape[0]
    places = jnp.arange(length_total, dtype=jnp.int32)
    same_doc = segment_row[:, None] == segment_row[None, :]
    starts = jnp.min(jnp.where(same_doc, places[None, :], length_total), axis=1)
    allowed = jnp.logical_and(same_doc, places[None, :] <= places[:, None])
    return (places - starts, allowed)


def rope_tables(position):
    half_dim = HEAD_SIZE // 2
    freq_steps = jnp.arange(half_dim, dtype=F32)
    frequency = jnp.exp(freq_steps * (-2.0 * math.log(10000.0) / HEAD_SIZE))
    angles = position.astype(F32)[:, None] * frequency[None, :]
    return (jnp.cos(angles)[:, None, :], jnp.sin(angles)[:, None, :])


def rotate(values, cos_table, sin_table, direction):
    half_dim = values.shape[-1] // 2
    leading = values[..., :half_dim]
    trailing = values[..., half_dim:]
    return jnp.concatenate(
        [
            leading * cos_table - direction * trailing * sin_table,
            trailing * cos_table + direction * leading * sin_table,
        ],
        axis=-1,
    )


def capped_scores(rotated_query, k_rot):
    token_rows = rotated_query.shape[0]
    query_groups = rotated_query.reshape(
        token_rows, KEY_VALUE_HEADS, QUERY_HEADS // KEY_VALUE_HEADS, HEAD_SIZE
    )
    raw_scores = product("tkgd,skd->kgts", query_groups, k_rot) * HEAD_SIZE ** (-0.5)
    return SOFT_CAP * jnp.tanh(raw_scores / SOFT_CAP)


def attention_forward(rows, layout):
    token_rows = rows.shape[0]
    query_span_width = QUERY_HEADS * HEAD_SIZE
    key_value_width = KEY_VALUE_HEADS * HEAD_SIZE
    allowed, cos_table, sin_table = layout
    query_part = (
        rows[:, :query_span_width].astype(F32).reshape(token_rows, QUERY_HEADS, HEAD_SIZE)
    )
    key_slice = (
        rows[:, query_span_width : query_span_width + key_value_width]
        .astype(F32)
        .reshape(token_rows, KEY_VALUE_HEADS, HEAD_SIZE)
    )
    value_slice = rows[:, query_span_width + key_value_width :].reshape(
        token_rows, KEY_VALUE_HEADS, HEAD_SIZE
    )
    rotated_query = rotate(query_part, cos_table, sin_table, 1.0).astype(BF)
    k_rot = rotate(key_slice, cos_table, sin_table, 1.0).astype(BF)
    capped = capped_scores(rotated_query, k_rot)
    log_total = jnp.log(jnp.sum(jnp.where(allowed, jnp.exp(capped), 0.0), axis=-1))
    weights_f = jnp.where(allowed, jnp.exp(capped - log_total[..., None]), 0.0)
    mixing_rows = product("kgts,skd->tkgd", weights_f.astype(BF), value_slice)
    mixing_rows = mixing_rows.astype(BF).reshape(token_rows, query_span_width)
    return (mixing_rows, (rotated_query, k_rot, value_slice, log_total))


def attention_backward(mixing_gradient, mixing_rows, saved, layout):
    rotated_query, k_rot, value_slice, log_total = saved
    token_rows = mixing_gradient.shape[0]
    heads_per_group = QUERY_HEADS // KEY_VALUE_HEADS
    allowed, cos_table, sin_table = layout
    capped = capped_scores(rotated_query, k_rot)
    weights_f = jnp.where(allowed, jnp.exp(capped - log_total[..., None]), 0.0)
    gradient_by_group = mixing_gradient.reshape(
        token_rows, KEY_VALUE_HEADS, heads_per_group, HEAD_SIZE
    )
    output_by_group = mixing_rows.reshape(token_rows, KEY_VALUE_HEADS, heads_per_group, HEAD_SIZE)
    row_delta = product("tkgd,tkgd->kgt", gradient_by_group, output_by_group)
    value_gradient = product("maew,emaq->wmq", weights_f.astype(BF), gradient_by_group)
    weight_grad = product("tkgd,skd->kgts", gradient_by_group, value_slice)
    score_gradient = (
        weights_f
        * (weight_grad - row_delta[..., None])
        * (1.0 - (capped / SOFT_CAP) ** 2)
        * HEAD_SIZE ** (-0.5)
    )
    score_gradient = score_gradient.astype(BF)
    query_gradient = product("kgts,skd->tkgd", score_gradient, k_rot).reshape(
        token_rows, QUERY_HEADS, HEAD_SIZE
    )
    key_gradient = product(
        "maew,emaq->wmq",
        score_gradient,
        rotated_query.reshape(token_rows, KEY_VALUE_HEADS, heads_per_group, HEAD_SIZE),
    )
    query_gradient = rotate(query_gradient, cos_table, sin_table, -1.0)
    key_gradient = rotate(key_gradient, cos_table, sin_table, -1.0)
    return jnp.concatenate(
        [
            query_gradient.reshape(token_rows, QUERY_HEADS * HEAD_SIZE),
            key_gradient.reshape(token_rows, KEY_VALUE_HEADS * HEAD_SIZE),
            value_gradient.reshape(token_rows, KEY_VALUE_HEADS * HEAD_SIZE),
        ],
        axis=1,
    ).astype(BF)


def inverse_rms(values):
    return lax.rsqrt(jnp.mean(values * values, axis=1, keepdims=True) + EPSILON)


def norm_back(grad_rows, unit_rows, scale_rows, gain):
    scaled = grad_rows * gain
    return scale_rows * (scaled - unit_rows * jnp.mean(scaled * unit_rows, axis=1, keepdims=True))


def flip(index, mask):
    return index + mask - 2 * mask * ((index // mask) % 2)


def flip_all(index, masks):
    bit = 1
    while bit <= masks:
        if masks & bit:
            index = flip(index, bit)
        bit *= 2
    return index


def greet(me, bits, lanes=0):
    barrier = pltpu.get_barrier_semaphore()
    for bit in bits:
        pl.semaphore_signal(barrier, inc=1, device_id={"gy": flip(me, bit)}, device_id_type=MESH)
    for d in range(1, lanes):
        other = (lax.axis_index("gx") + d) % lanes
        pl.semaphore_signal(barrier, inc=1, device_id={"gx": other}, device_id_type=MESH)
    pl.semaphore_wait(barrier, len(bits) + max(lanes - 1, 0))


def bit_orders(size):
    bits = []
    bit = 2
    while bit < size:
        bits.append(bit)
        bit *= 2
    return (bits + [1], bits[::-1] + [1])


def lay_out(rows_ref, blocks_ref, strip):
    lanes, count, width = blocks_ref.shape

    @pl.loop(0, count // strip)
    def _(i):
        rows = pl.ds(i * strip, strip)
        for k in range(lanes):
            rows_ref[rows, k * width : (k + 1) * width] = blocks_ref[k, rows].astype(F32)


def cut_up(blocks_ref, rows_ref, strip):
    lanes, count, width = blocks_ref.shape

    @pl.loop(0, count // strip)
    def _(i):
        rows = pl.ds(i * strip, strip)
        for k in range(lanes):
            blocks_ref[k, rows] = rows_ref[rows, k * width : (k + 1) * width].astype(BF)


def swap_start(lanes, side_ref, there_ref, sems):
    me = lax.axis_index("gx")
    own, send_sem, recv_sem = sems
    made = [pltpu.make_async_copy(side_ref.at[me], there_ref.at[me], own)]
    for d in range(1, lanes):
        other = (me + d) % lanes
        made.append(
            pltpu.make_async_remote_copy(
                src_ref=side_ref.at[other],
                dst_ref=there_ref.at[me],
                send_sem=send_sem.at[d],
                recv_sem=recv_sem.at[d],
                device_id={"gx": other},
                device_id_type=MESH,
            )
        )
    for copy in made:
        copy.start()
    return made


def swap_sems(lanes):
    return [
        pltpu.SemaphoreType.DMA,
        pltpu.SemaphoreType.DMA((lanes,)),
        pltpu.SemaphoreType.DMA((lanes,)),
    ]


def greet_lanes(lanes):
    barrier = pltpu.get_barrier_semaphore()
    for d in range(1, lanes):
        other = (lax.axis_index("gx") + d) % lanes
        pl.semaphore_signal(barrier, inc=1, device_id={"gx": other}, device_id_type=MESH)
    pl.semaphore_wait(barrier, lanes - 1)


def gather_rows_kernel(lanes, native_ref, small_ref, rows_ref, wide_ref, *scratch):
    send_ref, there_ref, small_all, *sems = scratch
    big_sems, small_sems = sems[:3], sems[3:]
    fold, pair = send_ref.shape[1:]
    width = pair // 2
    strip = 16
    for j in range(lanes):
        for side in range(2):

            @pl.loop(0, fold // strip)
            def _(i):
                rows = pl.ds((2 * j + side) * fold + i * strip, strip)
                send_ref[j, pl.ds(i * strip, strip), side * width : (side + 1) * width] = (
                    native_ref[rows].astype(BF)
                )

    greet_lanes(lanes)
    copies = swap_start(lanes, send_ref, there_ref, big_sems)
    copies += hand_round(lanes, small_ref, small_all, small_sems)
    for copy in copies:
        copy.wait()
    for k in range(lanes):
        columns = slice(k * width, (k + 1) * width)
        wide_ref[:, columns] = small_all[k]
        for side in range(2):

            @pl.loop(0, fold // strip)
            def _(i):
                rows_ref[pl.ds(side * fold + i * strip, strip), columns] = there_ref[
                    k, pl.ds(i * strip, strip), side * width : (side + 1) * width
                ].astype(F32)


def scatter_rows_kernel(lanes, rows_ref, wide_ref, native_ref, small_ref, *scratch):
    send_ref, there_ref, small_send, small_all, *sems = scratch
    big_sems, small_sems = sems[:3], sems[3:]
    fold, pair = send_ref.shape[1:]
    width = pair // 2
    strip = 16
    for j in range(lanes):
        columns = slice(j * width, (j + 1) * width)
        small_send[j] = wide_ref[:, columns]
        for side in range(2):

            @pl.loop(0, fold // strip)
            def _(i):
                send_ref[j, pl.ds(i * strip, strip), side * width : (side + 1) * width] = rows_ref[
                    pl.ds(side * fold + i * strip, strip), columns
                ].astype(BF)

    greet_lanes(lanes)
    copies = swap_start(lanes, send_ref, there_ref, big_sems)
    copies += swap_start(lanes, small_send, small_all, small_sems)
    for copy in copies:
        copy.wait()
    total = small_all[0]
    for k in range(1, lanes):
        total = total + small_all[k]
    small_ref[...] = total
    for k in range(lanes):
        for side in range(2):

            @pl.loop(0, fold // strip)
            def _(i):
                rows = pl.ds((2 * k + side) * fold + i * strip, strip)
                native_ref[rows] = there_ref[
                    k, pl.ds(i * strip, strip), side * width : (side + 1) * width
                ].astype(F32)


def hand_round(lanes, own_ref, all_ref, sems):
    me = lax.axis_index("gx")
    own, send_sem, recv_sem = sems
    made = [pltpu.make_async_copy(own_ref, all_ref.at[me], own)]
    for d in range(1, lanes):
        made.append(
            pltpu.make_async_remote_copy(
                src_ref=own_ref,
                dst_ref=all_ref.at[me],
                send_sem=send_sem.at[d],
                recv_sem=recv_sem.at[d],
                device_id={"gx": (me + d) % lanes},
                device_id_type=MESH,
            )
        )
    for copy in made:
        copy.start()
    return made


def exchange(kernel, lanes, big, small, outs, extra, call):
    total, width = big.shape
    space = pl.BlockSpec(memory_space=pltpu.VMEM)
    count = total * width // (lanes * outs[2])
    block = (lanes, count // 2, 2 * outs[2])
    cut = (lanes, small.shape[0], outs[2])
    return pl.pallas_call(
        functools.partial(kernel, lanes),
        out_shape=[jax.ShapeDtypeStruct(v, F32) for v in outs[:2]],
        in_specs=[space] * 2,
        out_specs=[space] * 2,
        scratch_shapes=[pltpu.VMEM(block, BF), pltpu.VMEM(block, BF)]
        + [pltpu.VMEM(cut, F32)] * (1 + extra)
        + swap_sems(lanes)
        + swap_sems(lanes),
        compiler_params=pltpu.CompilerParams(
            collective_id=call, has_side_effects=True, vmem_limit_bytes=32 << 20
        ),
        cost_estimate=pl.CostEstimate(
            flops=0, bytes_accessed=total * width * 16, transcendentals=0
        ),
        name="exchange",
    )(big, small)


def to_whole_rows(values, small, lanes):
    total, width = values.shape
    outs = ((total // lanes, lanes * width), (small.shape[0], lanes * width), width)
    return exchange(gather_rows_kernel, lanes, values, small, outs, 0, 9)


def to_width_blocks(rows, small, lanes):
    count, whole = rows.shape
    width = whole // lanes
    outs = ((count * lanes, width), (small.shape[0], width), width)
    return exchange(scatter_rows_kernel, lanes, rows, small, outs, 1, 10)


def spread_kernel(size, lanes, *refs):
    if lanes:
        own_ref, rows_ref, all_ref, there_ref, local_sem, send_sem, recv_sem, *rest = refs
        side_ref, *sems = rest
    else:
        own_ref, all_ref, local_sem, send_sem, recv_sem = refs
    me = lax.axis_index("gy")
    orders = bit_orders(size)
    half = own_ref.shape[0] // 2
    greet(me, orders[0], lanes)
    keep = pltpu.make_async_copy(own_ref, all_ref.at[me], local_sem)
    keep.start()
    copies = {}
    arrival = {}

    def copy(h, bit, r):
        n = len(copies)
        rows = pl.ds(h * half, half)
        where = flip_all(me, r)
        source = own_ref.at[rows] if r == 0 else all_ref.at[where, rows]
        made = pltpu.make_async_remote_copy(
            src_ref=source,
            dst_ref=all_ref.at[where, rows],
            send_sem=send_sem.at[n],
            recv_sem=recv_sem.at[n],
            device_id={"gy": flip(me, bit)},
            device_id_type=MESH,
        )
        copies[h, bit, r] = made
        arrival[h, r ^ bit] = made
        made.start()

    for step in range(len(orders[0])):
        for h in range(2):
            copy(h, orders[h][step], 0)
    swapped = []
    if lanes:
        cut_up(side_ref, rows_ref, 16)
        swapped = swap_start(lanes, side_ref, there_ref, sems)
    landed = set()

    def land(h, r):
        if (h, r) not in landed:
            landed.add((h, r))
            arrival[h, r].wait_recv()

    held = [[0], [0]]
    for step in range(len(orders[0])):
        for h in range(2):
            bit = orders[h][step]
            for r in held[h]:
                if r:
                    land(h, r)
                    copy(h, bit, r)
        for h in range(2):
            held[h] = held[h] + [r ^ orders[h][step] for r in held[h]]
    for h in range(2):
        for r in range(1, size):
            land(h, r)
    for made in copies.values():
        made.wait_send()
    for copy in [keep] + swapped:
        copy.wait()


def spread(values, side=None):
    size = lax.axis_size("gy")
    values = values.astype(BF)
    rows, width = values.shape
    count = 2 * (size - 1)
    sides = [] if side is None else [side]
    lanes = 0 if side is None else lax.axis_size("gx")
    blocks = (lanes, rows, width // max(lanes, 1))
    space = pl.BlockSpec(memory_space=pltpu.VMEM)
    out = pl.pallas_call(
        functools.partial(spread_kernel, size, lanes),
        out_shape=[jax.ShapeDtypeStruct((size, rows, width), values.dtype)]
        + [jax.ShapeDtypeStruct(blocks, BF) for v in sides],
        in_specs=[space] * (1 + len(sides)),
        out_specs=[pl.BlockSpec(memory_space=pltpu.HBM)] * (1 + len(sides)),
        scratch_shapes=[
            pltpu.SemaphoreType.DMA,
            pltpu.SemaphoreType.DMA((count,)),
            pltpu.SemaphoreType.DMA((count,)),
        ]
        + ([pltpu.VMEM(blocks, BF)] + swap_sems(lanes) if lanes else []),
        compiler_params=pltpu.CompilerParams(
            collective_id=4 if lanes else 0, has_side_effects=True, vmem_limit_bytes=32 << 20
        ),
        cost_estimate=pl.CostEstimate(
            flops=0, bytes_accessed=size * rows * width * 16, transcendentals=0
        ),
        name="spread",
    )(values, *sides)
    whole = out[0].reshape(size * rows, width)
    return (whole, out[1]) if lanes else whole


def settle_kernel(size, lanes, *refs):
    if lanes:
        parts_ref, side_ref, sum_ref, rows_ref, came, kept, send_sem, recv_sem, *rest = refs
        there_ref, *sems = rest
    else:
        parts_ref, sum_ref, came, kept, send_sem, recv_sem = refs
    me = lax.axis_index("gy")
    orders = tuple(order[::-1] for order in bit_orders(size)) * (PARTS // 2)
    half = sum_ref.shape[0] // PARTS
    strip = 16
    greet(me, orders[0], lanes)
    swapped = swap_start(lanes, side_ref, there_ref, sems) if lanes else []
    slot = {}
    for h in range(PARTS):
        held = list(range(size))
        for step, bit in enumerate(orders[h]):
            held = [r for r in held if not r & bit]
            for r in held:
                slot[h, step, r] = len(slot)
    copies = {}

    def view(h, step, r):
        if step == 0:
            return parts_ref.at[flip_all(me, r), pl.ds(h * half, half)]
        return kept.at[h, r]

    def send(h, step):
        bit = orders[h][step]
        gone = set()
        for b in orders[h][:step]:
            gone.add(b)
        for r in range(size):
            if r & bit and not any(r & b for b in gone):
                n = slot[h, step, r ^ bit]
                made = pltpu.make_async_remote_copy(
                    src_ref=view(h, step, r),
                    dst_ref=came.at[n],
                    send_sem=send_sem.at[n],
                    recv_sem=recv_sem.at[n],
                    device_id={"gy": flip(me, bit)},
                    device_id_type=MESH,
                )
                copies[h, step, r ^ bit] = made
                made.start()

    def gather(h, step, r, last):
        n = slot[h, step, r]
        copies[h, step, r].wait_recv()

        @pl.loop(0, half // strip)
        def _(i):
            rows = pl.ds(i * strip, strip)
            total = view(h, step, r)[rows].astype(F32) + came[n, rows].astype(F32)
            if last:
                sum_ref[pl.ds(h * half + i * strip, strip)] = total
            else:
                kept[h, r, rows] = total.astype(BF)

    steps = len(orders[0])
    for h in range(PARTS):
        send(h, 0)
    for step in range(steps):
        if lanes and step == steps - 1:
            for copy in swapped:
                copy.wait()
            lay_out(rows_ref, there_ref, strip)
        for h in range(PARTS):
            bits = orders[h][: step + 1]
            later = orders[h][step + 1] if step + 1 < steps else 0
            left = [r for r in range(size) if not any(r & b for b in bits)]
            for r in left:
                if r & later:
                    gather(h, step, r, False)
            if later:
                send(h, step + 1)
            for r in left:
                if not r & later:
                    gather(h, step, r, step == steps - 1)
    for made in copies.values():
        made.wait_send()


def settle(parts, side=None):
    size = lax.axis_size("gy")
    parts = parts.astype(BF)
    total, width = parts.shape
    rows = total // size
    count = PARTS * (size - 1)
    sides = [] if side is None else [side]
    lanes = 0 if side is None else side.shape[0]
    space = pl.BlockSpec(memory_space=pltpu.VMEM)
    out = pl.pallas_call(
        functools.partial(settle_kernel, size, lanes),
        out_shape=[jax.ShapeDtypeStruct((rows, width), F32)]
        + [jax.ShapeDtypeStruct((rows, width), F32) for v in sides],
        in_specs=[space] * (1 + len(sides)),
        out_specs=[space] * (1 + len(sides)),
        scratch_shapes=[
            pltpu.VMEM((count, rows // PARTS, width), BF),
            pltpu.VMEM((PARTS, size, rows // PARTS, width), BF),
            pltpu.SemaphoreType.DMA((count,)),
            pltpu.SemaphoreType.DMA((count,)),
        ]
        + ([pltpu.VMEM(side.shape, side.dtype)] + swap_sems(lanes) if lanes else []),
        compiler_params=pltpu.CompilerParams(
            collective_id=5 if lanes else 1, has_side_effects=True, vmem_limit_bytes=32 << 20
        ),
        cost_estimate=pl.CostEstimate(
            flops=0, bytes_accessed=total * width * 16, transcendentals=0
        ),
        name="settle",
    )(parts.reshape(size, rows, width), *sides)
    return out if lanes else out[0]


def tally_kernel(size, own_ref, sum_ref, came, send_sem, recv_sem):
    me = lax.axis_index("gy")
    barrier = pltpu.get_barrier_semaphore()
    for d in range(1, size):
        pl.semaphore_signal(
            barrier, inc=1, device_id={"gy": (me + d) % size}, device_id_type=MESH
        )
    pl.semaphore_wait(barrier, size - 1)
    copies = []
    for d in range(1, size):
        made = pltpu.make_async_remote_copy(
            src_ref=own_ref,
            dst_ref=came.at[d],
            send_sem=send_sem.at[d],
            recv_sem=recv_sem.at[d],
            device_id={"gy": (me + d) % size},
            device_id_type=MESH,
        )
        made.start()
        copies.append(made)
    total = own_ref[...]
    for d in range(1, size):
        copies[d - 1].wait_recv()
        total = total + came[d]
    sum_ref[...] = total
    for made in copies:
        made.wait_send()


def tally(values, size):
    return pl.pallas_call(
        functools.partial(tally_kernel, size),
        out_shape=jax.ShapeDtypeStruct(values.shape, F32),
        in_specs=[pl.BlockSpec(memory_space=pltpu.VMEM)],
        out_specs=pl.BlockSpec(memory_space=pltpu.VMEM),
        scratch_shapes=[
            pltpu.VMEM((size,) + values.shape, F32),
            pltpu.SemaphoreType.DMA((size,)),
            pltpu.SemaphoreType.DMA((size,)),
        ],
        compiler_params=pltpu.CompilerParams(collective_id=2, has_side_effects=True),
        name="tally",
    )(values)


def make_shards(nx, ny):
    blocks = [((b // ny) * ny + b % ny, (b % nx) * ny + b // nx) for b in range(nx * ny)]

    def shards(
        inputs,
        segment_ids,
        qkv_weight,
        out_weight,
        gate_up_weight,
        down_weight,
        first_gain,
        second_gain,
        third_gain,
        fourth_gain,
        cotangent,
    ):
        width = inputs.shape[1]

        gains = jnp.stack([first_gain, second_gain, third_gain, fourth_gain])
        x_rows, gains = to_whole_rows(inputs, gains, nx)
        x_rows, down_weight, segment_ids = lax.optimization_barrier(
            (x_rows, down_weight, segment_ids)
        )
        own = inputs.shape[0] // nx
        heads = qkv_weight.shape[1]
        gains = gains[:, None, :]
        both_w = lax.all_gather(
            jnp.concatenate([qkv_weight, out_weight.T], axis=1), "gx", axis=0, tiled=True
        )
        gate_up_w = lax.all_gather(gate_up_weight, "gx", axis=0, tiled=True)
        down_w = lax.all_gather(down_weight.T, "gx", axis=0, tiled=True)
        qkv_w, out_w = both_w[:, :heads], both_w[:, heads:]

        segment_row = lax.ppermute(segment_ids[0], ("gx", "gy"), blocks)
        position, allowed = block_layout(segment_row)
        layout = (allowed,) + rope_tables(position)

        scale_one = inverse_rms(x_rows)
        unit_one = x_rows * scale_one
        normed_one = spread(unit_one * gains[0])
        rows = product("td,dc->tc", normed_one, qkv_w).astype(BF)
        rows = lax.all_to_all(rows, "gy", split_axis=0, concat_axis=1, tiled=True)
        mixing_rows, saved = attention_forward(rows, layout)
        mixed = lax.all_to_all(mixing_rows, "gy", split_axis=1, concat_axis=0, tiled=True)
        attn_branch = settle(product("tc,dc->td", mixed, out_w))
        scale_two = inverse_rms(attn_branch)
        unit_two = attn_branch * scale_two
        attn_term = unit_two * gains[1]
        middle = x_rows + attn_term
        scale_three = inverse_rms(middle)
        unit_three = middle * scale_three
        normed_two = spread(unit_three * gains[2])
        pre_gate = product("td,df->tf", normed_two, gate_up_w[:, 0, :])
        up_part = product("td,df->tf", normed_two, gate_up_w[:, 1, :])
        value, slope = gelu_parts(pre_gate)
        hidden = (value * up_part).astype(BF)
        ff_branch, cot_rows = settle(
            product("tf,df->td", hidden, down_w), cotangent.astype(BF).reshape(nx, own, width)
        )
        scale_four = inverse_rms(ff_branch)
        unit_four = ff_branch * scale_four
        ff_grad, delta = spread(
            norm_back(cot_rows, unit_four, scale_four, gains[3]),
            attn_term + unit_four * gains[3],
        )
        outputs = inputs + delta.reshape(inputs.shape).astype(F32)

        down_sum = product("td,tf->df", ff_grad, hidden).astype(BF)
        down_sum, ff_grad = lax.optimization_barrier((down_sum, ff_grad))
        down_done = lax.psum_scatter(down_sum, "gx", scatter_dimension=0, tiled=True)
        hidden_grad = product("td,df->tf", ff_grad, down_w)
        gate_grad = (hidden_grad * up_part * slope).astype(BF)
        up_grad = (hidden_grad * value).astype(BF)
        gate_up_sum = jnp.stack(
            [
                product("td,tf->df", normed_two, gate_grad).astype(BF),
                product("td,tf->df", normed_two, up_grad).astype(BF),
            ],
            axis=1,
        )
        gate_up_sum, gate_grad, up_grad = lax.optimization_barrier(
            (gate_up_sum, gate_grad, up_grad)
        )
        gate_up_done = lax.psum_scatter(gate_up_sum, "gx", scatter_dimension=0, tiled=True)
        normed_two_grad = settle(
            product("tf,df->td", gate_grad, gate_up_w[:, 0, :])
            + product("tf,df->td", up_grad, gate_up_w[:, 1, :])
        )
        middle_delta = norm_back(normed_two_grad, unit_three, scale_three, gains[2])
        middle_grad = cot_rows + middle_delta
        branch_grad = spread(norm_back(middle_grad, unit_two, scale_two, gains[1]))
        out_sum = product("td,tc->dc", branch_grad, mixed).astype(BF)
        mixing_gradient = product("td,dc->tc", branch_grad, out_w).astype(BF)
        mixing_gradient = lax.all_to_all(
            mixing_gradient, "gy", split_axis=0, concat_axis=1, tiled=True
        )
        qkv_grad_rows = attention_backward(mixing_gradient, mixing_rows, saved, layout)
        qkv_grad_rows, down_done = lax.optimization_barrier((qkv_grad_rows, down_done))
        qkv_grad_rows = lax.all_to_all(
            qkv_grad_rows, "gy", split_axis=1, concat_axis=0, tiled=True
        )
        normed_one_grad = settle(product("tc,dc->td", qkv_grad_rows, qkv_w))
        both_sum = jnp.concatenate(
            [product("td,tc->dc", normed_one, qkv_grad_rows).astype(BF), out_sum], axis=1
        )
        terms = jnp.stack(
            [
                jnp.sum(normed_one_grad * unit_one, axis=0),
                jnp.sum(middle_grad * unit_two, axis=0),
                jnp.sum(normed_two_grad * unit_three, axis=0),
                jnp.sum(cot_rows * unit_four, axis=0),
            ]
        )
        delta, terms = to_width_blocks(
            middle_delta + norm_back(normed_one_grad, unit_one, scale_one, gains[0]),
            tally(terms, ny),
            nx,
        )
        down_grad = down_done.astype(F32).T
        both_sum = with_layout_constraint(both_sum, Layout((0, 1)))
        gate_up_done, both_sum, delta, down_grad = lax.optimization_barrier(
            (gate_up_done, both_sum, delta, down_grad)
        )
        both_done = lax.psum_scatter(both_sum, "gx", scatter_dimension=0, tiled=True)
        gate_up_grad = gate_up_done.astype(F32)
        input_grad = cotangent + delta
        qkv_grad = both_done[:, :heads].astype(F32)
        out_grad = both_done[:, heads:].astype(F32).T
        return (outputs, input_grad, qkv_grad, out_grad, gate_up_grad, down_grad) + tuple(
            terms[i] for i in range(4)
        )

    return shards


def solution(mesh):
    placed = (
        P("gy", "gx"),
        P(("gx", "gy"), None),
        P("gx", "gy"),
        P("gy", "gx"),
        P("gx", None, "gy"),
        P("gy", "gx"),
        P("gx"),
        P("gx"),
        P("gx"),
        P("gx"),
        P("gy", "gx"),
    )
    return jax.shard_map(
        make_shards(mesh.shape["gx"], mesh.shape["gy"]),
        mesh=mesh,
        in_specs=placed,
        out_specs=(
            P("gy", "gx"),
            P("gy", "gx"),
            P("gx", "gy"),
            P("gy", "gx"),
            P("gx", None, "gy"),
            P("gy", "gx"),
            P("gx"),
            P("gx"),
            P("gx"),
            P("gx"),
        ),
        check_vma=False,
    )
```

```python
import functools
import math

import jax
import jax.numpy as jnp
from jax import lax
from jax.experimental import pallas as pl
from jax.experimental.layout import Layout, with_layout_constraint
from jax.experimental.pallas import tpu as pltpu
from jax.sharding import PartitionSpec as P

QUERY_HEADS = 8
KEY_VALUE_HEADS = 4
HEAD_SIZE = 256


EPSILON = 1e-06
SOFT_CAP = 50.0
GELU_COEF = 0.7978845608028654
CUBIC_COEF = 0.044715

BF = jnp.bfloat16
F32 = jnp.float32
MESH = pl.DeviceIdType.MESH
PARTS = 4
TILE = 256


def product(form, left, right):
    return jnp.einsum(form, left, right, preferred_element_type=F32)


def gelu_parts(pre_gate):
    inner_arg = GELU_COEF * (pre_gate + CUBIC_COEF * pre_gate * pre_gate * pre_gate)
    tanh_value = jnp.tanh(inner_arg)
    activated = 0.5 * pre_gate * (1.0 + tanh_value)
    derivative = 0.5 * (1.0 + tanh_value) + 0.5 * pre_gate * (
        1.0 - tanh_value * tanh_value
    ) * GELU_COEF * (1.0 + 3.0 * CUBIC_COEF * pre_gate * pre_gate)
    return (activated, derivative)


def block_layout(segment_row):
    length_total = segment_row.shape[0]
    places = jnp.arange(length_total, dtype=jnp.int32)
    same_doc = segment_row[:, None] == segment_row[None, :]
    starts = jnp.min(jnp.where(same_doc, places[None, :], length_total), axis=1)
    allowed = jnp.logical_and(same_doc, places[None, :] <= places[:, None])
    return (places - starts, allowed)


def rope_tables(position):
    half_dim = HEAD_SIZE // 2
    freq_steps = jnp.arange(half_dim, dtype=F32)
    frequency = jnp.exp(freq_steps * (-2.0 * math.log(10000.0) / HEAD_SIZE))
    angles = position.astype(F32)[:, None] * frequency[None, :]
    return (jnp.cos(angles)[:, None, :], jnp.sin(angles)[:, None, :])


def rotate(values, cos_table, sin_table, direction):
    half_dim = values.shape[-1] // 2
    leading = values[..., :half_dim]
    trailing = values[..., half_dim:]
    return jnp.concatenate(
        [
            leading * cos_table - direction * trailing * sin_table,
            trailing * cos_table + direction * leading * sin_table,
        ],
        axis=-1,
    )


def capped_scores(rotated_query, k_rot):
    token_rows = rotated_query.shape[0]
    query_groups = rotated_query.reshape(
        token_rows, KEY_VALUE_HEADS, QUERY_HEADS // KEY_VALUE_HEADS, HEAD_SIZE
    )
    raw_scores = product("tkgd,skd->kgts", query_groups, k_rot) * HEAD_SIZE ** (-0.5)
    return SOFT_CAP * jnp.tanh(raw_scores / SOFT_CAP)


def attention_forward(rows, layout):
    token_rows = rows.shape[0]
    query_span_width = QUERY_HEADS * HEAD_SIZE
    key_value_width = KEY_VALUE_HEADS * HEAD_SIZE
    allowed, cos_table, sin_table = layout
    query_part = (
        rows[:, :query_span_width].astype(F32).reshape(token_rows, QUERY_HEADS, HEAD_SIZE)
    )
    key_slice = (
        rows[:, query_span_width : query_span_width + key_value_width]
        .astype(F32)
        .reshape(token_rows, KEY_VALUE_HEADS, HEAD_SIZE)
    )
    value_slice = rows[:, query_span_width + key_value_width :].reshape(
        token_rows, KEY_VALUE_HEADS, HEAD_SIZE
    )
    rotated_query = rotate(query_part, cos_table, sin_table, 1.0).astype(BF)
    k_rot = rotate(key_slice, cos_table, sin_table, 1.0).astype(BF)
    capped = capped_scores(rotated_query, k_rot)
    log_total = jnp.log(jnp.sum(jnp.where(allowed, jnp.exp(capped), 0.0), axis=-1))
    weights_f = jnp.where(allowed, jnp.exp(capped - log_total[..., None]), 0.0)
    mixing_rows = product("kgts,skd->tkgd", weights_f.astype(BF), value_slice)
    mixing_rows = mixing_rows.astype(BF).reshape(token_rows, query_span_width)
    return (mixing_rows, (rotated_query, k_rot, value_slice, log_total))


def attention_backward(mixing_gradient, mixing_rows, saved, layout):
    rotated_query, k_rot, value_slice, log_total = saved
    token_rows = mixing_gradient.shape[0]
    heads_per_group = QUERY_HEADS // KEY_VALUE_HEADS
    allowed, cos_table, sin_table = layout
    capped = capped_scores(rotated_query, k_rot)
    weights_f = jnp.where(allowed, jnp.exp(capped - log_total[..., None]), 0.0)
    gradient_by_group = mixing_gradient.reshape(
        token_rows, KEY_VALUE_HEADS, heads_per_group, HEAD_SIZE
    )
    output_by_group = mixing_rows.reshape(token_rows, KEY_VALUE_HEADS, heads_per_group, HEAD_SIZE)
    row_delta = product("tkgd,tkgd->kgt", gradient_by_group, output_by_group)
    value_gradient = product("maew,emaq->wmq", weights_f.astype(BF), gradient_by_group)
    weight_grad = product("tkgd,skd->kgts", gradient_by_group, value_slice)
    score_gradient = (
        weights_f
        * (weight_grad - row_delta[..., None])
        * (1.0 - (capped / SOFT_CAP) ** 2)
        * HEAD_SIZE ** (-0.5)
    )
    score_gradient = score_gradient.astype(BF)
    query_gradient = product("kgts,skd->tkgd", score_gradient, k_rot).reshape(
        token_rows, QUERY_HEADS, HEAD_SIZE
    )
    key_gradient = product(
        "maew,emaq->wmq",
        score_gradient,
        rotated_query.reshape(token_rows, KEY_VALUE_HEADS, heads_per_group, HEAD_SIZE),
    )
    query_gradient = rotate(query_gradient, cos_table, sin_table, -1.0)
    key_gradient = rotate(key_gradient, cos_table, sin_table, -1.0)
    return jnp.concatenate(
        [
            query_gradient.reshape(token_rows, QUERY_HEADS * HEAD_SIZE),
            key_gradient.reshape(token_rows, KEY_VALUE_HEADS * HEAD_SIZE),
            value_gradient.reshape(token_rows, KEY_VALUE_HEADS * HEAD_SIZE),
        ],
        axis=1,
    ).astype(BF)


def inverse_rms(values):
    return lax.rsqrt(jnp.mean(values * values, axis=1, keepdims=True) + EPSILON)


def norm_back(grad_rows, unit_rows, scale_rows, gain):
    scaled = grad_rows * gain
    return scale_rows * (scaled - unit_rows * jnp.mean(scaled * unit_rows, axis=1, keepdims=True))


def flip(index, mask):
    return index + mask - 2 * mask * ((index // mask) % 2)


def flip_all(index, masks):
    bit = 1
    while bit <= masks:
        if masks & bit:
            index = flip(index, bit)
        bit *= 2
    return index


def greet(me, bits, lanes=0):
    barrier = pltpu.get_barrier_semaphore()
    for bit in bits:
        pl.semaphore_signal(barrier, inc=1, device_id={"gy": flip(me, bit)}, device_id_type=MESH)
    for d in range(1, lanes):
        other = (lax.axis_index("gx") + d) % lanes
        pl.semaphore_signal(barrier, inc=1, device_id={"gx": other}, device_id_type=MESH)
    pl.semaphore_wait(barrier, len(bits) + max(lanes - 1, 0))


def bit_orders(size):
    bits = []
    bit = 2
    while bit < size:
        bits.append(bit)
        bit *= 2
    return (bits + [1], bits[::-1] + [1])


def lay_out(rows_ref, blocks_ref, strip):
    lanes, count, width = blocks_ref.shape

    @pl.loop(0, count // strip)
    def _(i):
        rows = pl.ds(i * strip, strip)
        for k in range(lanes):
            rows_ref[rows, k * width : (k + 1) * width] = blocks_ref[k, rows].astype(F32)


def cut_up(blocks_ref, rows_ref, strip):
    lanes, count, width = blocks_ref.shape

    @pl.loop(0, count // strip)
    def _(i):
        rows = pl.ds(i * strip, strip)
        for k in range(lanes):
            blocks_ref[k, rows] = rows_ref[rows, k * width : (k + 1) * width].astype(BF)


def swap_start(lanes, side_ref, there_ref, sems):
    me = lax.axis_index("gx")
    own, send_sem, recv_sem = sems
    made = [pltpu.make_async_copy(side_ref.at[me], there_ref.at[me], own)]
    for d in range(1, lanes):
        other = (me + d) % lanes
        made.append(
            pltpu.make_async_remote_copy(
                src_ref=side_ref.at[other],
                dst_ref=there_ref.at[me],
                send_sem=send_sem.at[d],
                recv_sem=recv_sem.at[d],
                device_id={"gx": other},
                device_id_type=MESH,
            )
        )
    for copy in made:
        copy.start()
    return made


def swap_sems(lanes):
    return [
        pltpu.SemaphoreType.DMA,
        pltpu.SemaphoreType.DMA((lanes,)),
        pltpu.SemaphoreType.DMA((lanes,)),
    ]


def greet_lanes(lanes):
    barrier = pltpu.get_barrier_semaphore()
    for d in range(1, lanes):
        other = (lax.axis_index("gx") + d) % lanes
        pl.semaphore_signal(barrier, inc=1, device_id={"gx": other}, device_id_type=MESH)
    pl.semaphore_wait(barrier, lanes - 1)


def gather_rows_kernel(lanes, native_ref, small_ref, rows_ref, wide_ref, *scratch):
    send_ref, there_ref, small_all, *sems = scratch
    big_sems, small_sems = sems[:3], sems[3:]
    fold, pair = send_ref.shape[1:]
    width = pair // 2
    strip = 16
    for j in range(lanes):
        for side in range(2):

            @pl.loop(0, fold // strip)
            def _(i):
                rows = pl.ds((2 * j + side) * fold + i * strip, strip)
                send_ref[j, pl.ds(i * strip, strip), side * width : (side + 1) * width] = (
                    native_ref[rows].astype(BF)
                )

    greet_lanes(lanes)
    copies = swap_start(lanes, send_ref, there_ref, big_sems)
    copies += hand_round(lanes, small_ref, small_all, small_sems)
    for copy in copies:
        copy.wait()
    for k in range(lanes):
        columns = slice(k * width, (k + 1) * width)
        wide_ref[:, columns] = small_all[k]
        for side in range(2):

            @pl.loop(0, fold // strip)
            def _(i):
                rows_ref[pl.ds(side * fold + i * strip, strip), columns] = there_ref[
                    k, pl.ds(i * strip, strip), side * width : (side + 1) * width
                ].astype(F32)


def scatter_rows_kernel(lanes, rows_ref, wide_ref, native_ref, small_ref, *scratch):
    send_ref, there_ref, small_send, small_all, *sems = scratch
    big_sems, small_sems = sems[:3], sems[3:]
    fold, pair = send_ref.shape[1:]
    width = pair // 2
    strip = 16
    for j in range(lanes):
        columns = slice(j * width, (j + 1) * width)
        small_send[j] = wide_ref[:, columns]
        for side in range(2):

            @pl.loop(0, fold // strip)
            def _(i):
                send_ref[j, pl.ds(i * strip, strip), side * width : (side + 1) * width] = rows_ref[
                    pl.ds(side * fold + i * strip, strip), columns
                ].astype(BF)

    greet_lanes(lanes)
    copies = swap_start(lanes, send_ref, there_ref, big_sems)
    copies += swap_start(lanes, small_send, small_all, small_sems)
    for copy in copies:
        copy.wait()
    total = small_all[0]
    for k in range(1, lanes):
        total = total + small_all[k]
    small_ref[...] = total
    for k in range(lanes):
        for side in range(2):

            @pl.loop(0, fold // strip)
            def _(i):
                rows = pl.ds((2 * k + side) * fold + i * strip, strip)
                native_ref[rows] = there_ref[
                    k, pl.ds(i * strip, strip), side * width : (side + 1) * width
                ].astype(F32)


def hand_round(lanes, own_ref, all_ref, sems):
    me = lax.axis_index("gx")
    own, send_sem, recv_sem = sems
    made = [pltpu.make_async_copy(own_ref, all_ref.at[me], own)]
    for d in range(1, lanes):
        made.append(
            pltpu.make_async_remote_copy(
                src_ref=own_ref,
                dst_ref=all_ref.at[me],
                send_sem=send_sem.at[d],
                recv_sem=recv_sem.at[d],
                device_id={"gx": (me + d) % lanes},
                device_id_type=MESH,
            )
        )
    for copy in made:
        copy.start()
    return made


def exchange(kernel, lanes, big, small, outs, extra, call):
    total, width = big.shape
    space = pl.BlockSpec(memory_space=pltpu.VMEM)
    count = total * width // (lanes * outs[2])
    block = (lanes, count // 2, 2 * outs[2])
    cut = (lanes, small.shape[0], outs[2])
    return pl.pallas_call(
        functools.partial(kernel, lanes),
        out_shape=[jax.ShapeDtypeStruct(v, F32) for v in outs[:2]],
        in_specs=[space] * 2,
        out_specs=[space] * 2,
        scratch_shapes=[pltpu.VMEM(block, BF), pltpu.VMEM(block, BF)]
        + [pltpu.VMEM(cut, F32)] * (1 + extra)
        + swap_sems(lanes)
        + swap_sems(lanes),
        compiler_params=pltpu.CompilerParams(
            collective_id=call, has_side_effects=True, vmem_limit_bytes=32 << 20
        ),
        cost_estimate=pl.CostEstimate(
            flops=0, bytes_accessed=total * width * 16, transcendentals=0
        ),
        name="exchange",
    )(big, small)


def to_whole_rows(values, small, lanes):
    total, width = values.shape
    outs = ((total // lanes, lanes * width), (small.shape[0], lanes * width), width)
    return exchange(gather_rows_kernel, lanes, values, small, outs, 0, 9)


def to_width_blocks(rows, small, lanes):
    count, whole = rows.shape
    width = whole // lanes
    outs = ((count * lanes, width), (small.shape[0], width), width)
    return exchange(scatter_rows_kernel, lanes, rows, small, outs, 1, 10)


def spread_kernel(size, lanes, *refs):
    if lanes:
        own_ref, rows_ref, all_ref, there_ref, local_sem, send_sem, recv_sem, *rest = refs
        side_ref, *sems = rest
    else:
        own_ref, all_ref, local_sem, send_sem, recv_sem = refs
    me = lax.axis_index("gy")
    orders = bit_orders(size)
    half = own_ref.shape[0] // 2
    greet(me, orders[0], lanes)
    keep = pltpu.make_async_copy(own_ref, all_ref.at[me], local_sem)
    keep.start()
    copies = {}
    arrival = {}

    def copy(h, bit, r):
        n = len(copies)
        rows = pl.ds(h * half, half)
        where = flip_all(me, r)
        source = own_ref.at[rows] if r == 0 else all_ref.at[where, rows]
        made = pltpu.make_async_remote_copy(
            src_ref=source,
            dst_ref=all_ref.at[where, rows],
            send_sem=send_sem.at[n],
            recv_sem=recv_sem.at[n],
            device_id={"gy": flip(me, bit)},
            device_id_type=MESH,
        )
        copies[h, bit, r] = made
        arrival[h, r ^ bit] = made
        made.start()

    for step in range(len(orders[0])):
        for h in range(2):
            copy(h, orders[h][step], 0)
    swapped = []
    if lanes:
        cut_up(side_ref, rows_ref, 16)
        swapped = swap_start(lanes, side_ref, there_ref, sems)
    landed = set()

    def land(h, r):
        if (h, r) not in landed:
            landed.add((h, r))
            arrival[h, r].wait_recv()

    held = [[0], [0]]
    for step in range(len(orders[0])):
        for h in range(2):
            bit = orders[h][step]
            for r in held[h]:
                if r:
                    land(h, r)
                    copy(h, bit, r)
        for h in range(2):
            held[h] = held[h] + [r ^ orders[h][step] for r in held[h]]
    for h in range(2):
        for r in range(1, size):
            land(h, r)
    for made in copies.values():
        made.wait_send()
    for copy in [keep] + swapped:
        copy.wait()


def spread(values, side=None):
    size = lax.axis_size("gy")
    values = values.astype(BF)
    rows, width = values.shape
    count = 2 * (size - 1)
    sides = [] if side is None else [side]
    lanes = 0 if side is None else lax.axis_size("gx")
    blocks = (lanes, rows, width // max(lanes, 1))
    space = pl.BlockSpec(memory_space=pltpu.VMEM)
    out = pl.pallas_call(
        functools.partial(spread_kernel, size, lanes),
        out_shape=[jax.ShapeDtypeStruct((size, rows, width), values.dtype)]
        + [jax.ShapeDtypeStruct(blocks, BF) for v in sides],
        in_specs=[space] * (1 + len(sides)),
        out_specs=[pl.BlockSpec(memory_space=pltpu.HBM)] * (1 + len(sides)),
        scratch_shapes=[
            pltpu.SemaphoreType.DMA,
            pltpu.SemaphoreType.DMA((count,)),
            pltpu.SemaphoreType.DMA((count,)),
        ]
        + ([pltpu.VMEM(blocks, BF)] + swap_sems(lanes) if lanes else []),
        compiler_params=pltpu.CompilerParams(
            collective_id=4 if lanes else 0, has_side_effects=True, vmem_limit_bytes=32 << 20
        ),
        cost_estimate=pl.CostEstimate(
            flops=0, bytes_accessed=size * rows * width * 16, transcendentals=0
        ),
        name="spread",
    )(values, *sides)
    whole = out[0].reshape(size * rows, width)
    return (whole, out[1]) if lanes else whole


def settle_kernel(size, lanes, fused, *refs):
    if fused:
        left_ref, right_ref, *refs = refs
        *refs, picked, product_ref = refs
        refs = [product_ref] + refs
    if lanes:
        parts_ref, side_ref, sum_ref, rows_ref, came, kept, send_sem, recv_sem, *rest = refs
        there_ref, *sems = rest
    else:
        parts_ref, sum_ref, came, kept, send_sem, recv_sem = refs
    me = lax.axis_index("gy")
    orders = tuple(order[::-1] for order in bit_orders(size)) * (PARTS // 2)
    half = sum_ref.shape[0] // PARTS
    strip = 16
    greet(me, orders[0], lanes)
    swapped = swap_start(lanes, side_ref, there_ref, sems) if lanes else []
    slot = {}
    for h in range(PARTS):
        held = list(range(size))
        for step, bit in enumerate(orders[h]):
            held = [r for r in held if not r & bit]
            for r in held:
                slot[h, step, r] = len(slot)
    copies = {}

    def multiply(group):
        count = left_ref.shape[1]
        for j, r in enumerate(group):
            where = flip_all(me, r)

            @pl.loop(0, count // strip)
            def _(i):
                picked[pl.ds(j * count + i * strip, strip)] = left_ref[
                    where, pl.ds(i * strip, strip)
                ]

        @pl.loop(0, right_ref.shape[0] // TILE)
        def _(i):
            columns = pl.ds(pl.multiple_of(i * TILE, TILE), TILE)
            block = lax.dot_general(
                picked[...],
                right_ref[columns],
                (((1,), (1,)), ((), ())),
                preferred_element_type=F32,
            ).astype(BF)
            for j, r in enumerate(group):
                parts_ref[flip_all(me, r), :, columns] = block[j * count : (j + 1) * count]

    def view(h, step, r):
        if step == 0:
            return parts_ref.at[flip_all(me, r), pl.ds(h * half, half)]
        return kept.at[h, r]

    def send(h, step):
        bit = orders[h][step]
        gone = set()
        for b in orders[h][:step]:
            gone.add(b)
        for r in range(size):
            if r & bit and not any(r & b for b in gone):
                n = slot[h, step, r ^ bit]
                made = pltpu.make_async_remote_copy(
                    src_ref=view(h, step, r),
                    dst_ref=came.at[n],
                    send_sem=send_sem.at[n],
                    recv_sem=recv_sem.at[n],
                    device_id={"gy": flip(me, bit)},
                    device_id_type=MESH,
                )
                copies[h, step, r ^ bit] = made
                made.start()

    def gather(h, step, r, last):
        n = slot[h, step, r]
        copies[h, step, r].wait_recv()

        @pl.loop(0, half // strip)
        def _(i):
            rows = pl.ds(i * strip, strip)
            total = view(h, step, r)[rows].astype(F32) + came[n, rows].astype(F32)
            if last:
                sum_ref[pl.ds(h * half + i * strip, strip)] = total
            else:
                kept[h, r, rows] = total.astype(BF)

    steps = len(orders[0])
    if fused:
        multiply([r for r in range(size) if r & 1])
    for h in range(PARTS):
        send(h, 0)
    if fused:
        multiply([r for r in range(size) if not r & 1])
    for step in range(steps):
        if lanes and step == steps - 1:
            for copy in swapped:
                copy.wait()
            lay_out(rows_ref, there_ref, strip)
        for h in range(PARTS):
            bits = orders[h][: step + 1]
            later = orders[h][step + 1] if step + 1 < steps else 0
            left = [r for r in range(size) if not any(r & b for b in bits)]
            for r in left:
                if r & later:
                    gather(h, step, r, False)
            if later:
                send(h, step + 1)
            for r in left:
                if not r & later:
                    gather(h, step, r, step == steps - 1)
    for made in copies.values():
        made.wait_send()


def settle(parts, side=None, right=None):
    size = lax.axis_size("gy")
    parts = parts.astype(BF)
    total, inner = parts.shape
    width = inner if right is None else right.shape[0]
    rows = total // size
    count = PARTS * (size - 1)
    sides = [] if side is None else [side]
    rights = [] if right is None else [right]
    lanes = 0 if side is None else side.shape[0]
    space = pl.BlockSpec(memory_space=pltpu.VMEM)
    scratch = [
        pltpu.VMEM((count, rows // PARTS, width), BF),
        pltpu.VMEM((PARTS, size, rows // PARTS, width), BF),
        pltpu.SemaphoreType.DMA((count,)),
        pltpu.SemaphoreType.DMA((count,)),
    ]
    if lanes:
        scratch += [pltpu.VMEM(side.shape, side.dtype)] + swap_sems(lanes)
    if rights:
        scratch += [pltpu.VMEM((total // 2, inner), BF), pltpu.VMEM((size, rows, width), BF)]
    out = pl.pallas_call(
        functools.partial(settle_kernel, size, lanes, bool(rights)),
        out_shape=[jax.ShapeDtypeStruct((rows, width), F32)] * (1 + len(sides)),
        in_specs=[space] * (1 + len(sides) + len(rights)),
        out_specs=[space] * (1 + len(sides)),
        scratch_shapes=scratch,
        compiler_params=pltpu.CompilerParams(
            collective_id=5 if lanes else 1, has_side_effects=True, vmem_limit_bytes=40 << 20
        ),
        cost_estimate=pl.CostEstimate(
            flops=0, bytes_accessed=total * width * 16, transcendentals=0
        ),
        name="settle",
    )(parts.reshape(size, rows, inner), *rights, *sides)
    return out if lanes else out[0]


def tally_kernel(size, own_ref, sum_ref, came, send_sem, recv_sem):
    me = lax.axis_index("gy")
    barrier = pltpu.get_barrier_semaphore()
    for d in range(1, size):
        pl.semaphore_signal(
            barrier, inc=1, device_id={"gy": (me + d) % size}, device_id_type=MESH
        )
    pl.semaphore_wait(barrier, size - 1)
    copies = []
    for d in range(1, size):
        made = pltpu.make_async_remote_copy(
            src_ref=own_ref,
            dst_ref=came.at[d],
            send_sem=send_sem.at[d],
            recv_sem=recv_sem.at[d],
            device_id={"gy": (me + d) % size},
            device_id_type=MESH,
        )
        made.start()
        copies.append(made)
    total = own_ref[...]
    for d in range(1, size):
        copies[d - 1].wait_recv()
        total = total + came[d]
    sum_ref[...] = total
    for made in copies:
        made.wait_send()


def tally(values, size):
    return pl.pallas_call(
        functools.partial(tally_kernel, size),
        out_shape=jax.ShapeDtypeStruct(values.shape, F32),
        in_specs=[pl.BlockSpec(memory_space=pltpu.VMEM)],
        out_specs=pl.BlockSpec(memory_space=pltpu.VMEM),
        scratch_shapes=[
            pltpu.VMEM((size,) + values.shape, F32),
            pltpu.SemaphoreType.DMA((size,)),
            pltpu.SemaphoreType.DMA((size,)),
        ],
        compiler_params=pltpu.CompilerParams(collective_id=2, has_side_effects=True),
        name="tally",
    )(values)


def make_shards(nx, ny):
    blocks = [((b // ny) * ny + b % ny, (b % nx) * ny + b // nx) for b in range(nx * ny)]

    def shards(
        inputs,
        segment_ids,
        qkv_weight,
        out_weight,
        gate_up_weight,
        down_weight,
        first_gain,
        second_gain,
        third_gain,
        fourth_gain,
        cotangent,
    ):
        width = inputs.shape[1]

        own = inputs.shape[0] // nx
        heads = qkv_weight.shape[1]
        both_w = lax.all_gather(
            jnp.concatenate([qkv_weight, out_weight.T], axis=1), "gx", axis=0, tiled=True
        )
        gains = jnp.stack([first_gain, second_gain, third_gain, fourth_gain])
        gains, both_w = lax.optimization_barrier((gains, both_w))
        x_rows, gains = to_whole_rows(inputs, gains, nx)
        gains = gains[:, None, :]
        gate_up_w = lax.all_gather(gate_up_weight, "gx", axis=0, tiled=True)
        down_w = lax.all_gather(down_weight.T, "gx", axis=0, tiled=True)
        qkv_w, out_w = both_w[:, :heads], both_w[:, heads:]

        segment_row = lax.ppermute(segment_ids[0], ("gx", "gy"), blocks)
        position, allowed = block_layout(segment_row)
        layout = (allowed,) + rope_tables(position)

        scale_one = inverse_rms(x_rows)
        unit_one = x_rows * scale_one
        normed_one = spread(unit_one * gains[0])
        rows = product("td,dc->tc", normed_one, qkv_w).astype(BF)
        rows = lax.all_to_all(rows, "gy", split_axis=0, concat_axis=1, tiled=True)
        mixing_rows, saved = attention_forward(rows, layout)
        mixed = lax.all_to_all(mixing_rows, "gy", split_axis=1, concat_axis=0, tiled=True)
        attn_branch = settle(product("tc,dc->td", mixed, out_w))
        scale_two = inverse_rms(attn_branch)
        unit_two = attn_branch * scale_two
        attn_term = unit_two * gains[1]
        middle = x_rows + attn_term
        scale_three = inverse_rms(middle)
        unit_three = middle * scale_three
        normed_two = spread(unit_three * gains[2])
        pre_gate = product("td,df->tf", normed_two, gate_up_w[:, 0, :])
        up_part = product("td,df->tf", normed_two, gate_up_w[:, 1, :])
        value, slope = gelu_parts(pre_gate)
        hidden = (value * up_part).astype(BF)
        ff_branch, cot_rows = settle(
            hidden, cotangent.astype(BF).reshape(nx, own, width), down_w
        )
        scale_four = inverse_rms(ff_branch)
        unit_four = ff_branch * scale_four
        ff_grad, delta = spread(
            norm_back(cot_rows, unit_four, scale_four, gains[3]),
            attn_term + unit_four * gains[3],
        )
        outputs = inputs + delta.reshape(inputs.shape).astype(F32)

        down_sum = product("td,tf->df", ff_grad, hidden).astype(BF)
        down_sum, ff_grad = lax.optimization_barrier((down_sum, ff_grad))
        down_done = lax.psum_scatter(down_sum, "gx", scatter_dimension=0, tiled=True)
        hidden_grad = product("td,df->tf", ff_grad, down_w)
        gate_grad = (hidden_grad * up_part * slope).astype(BF)
        up_grad = (hidden_grad * value).astype(BF)
        gate_up_sum = jnp.stack(
            [
                product("td,tf->df", normed_two, gate_grad).astype(BF),
                product("td,tf->df", normed_two, up_grad).astype(BF),
            ],
            axis=1,
        )
        gate_up_sum, gate_grad, up_grad = lax.optimization_barrier(
            (gate_up_sum, gate_grad, up_grad)
        )
        gate_up_done = lax.psum_scatter(gate_up_sum, "gx", scatter_dimension=0, tiled=True)
        normed_two_grad = settle(
            product("tf,df->td", gate_grad, gate_up_w[:, 0, :])
            + product("tf,df->td", up_grad, gate_up_w[:, 1, :])
        )
        middle_delta = norm_back(normed_two_grad, unit_three, scale_three, gains[2])
        middle_grad = cot_rows + middle_delta
        branch_grad = spread(norm_back(middle_grad, unit_two, scale_two, gains[1]))
        out_sum = product("td,tc->dc", branch_grad, mixed).astype(BF)
        mixing_gradient = product("td,dc->tc", branch_grad, out_w).astype(BF)
        mixing_gradient = lax.all_to_all(
            mixing_gradient, "gy", split_axis=0, concat_axis=1, tiled=True
        )
        qkv_grad_rows = attention_backward(mixing_gradient, mixing_rows, saved, layout)
        qkv_grad_rows, down_done = lax.optimization_barrier((qkv_grad_rows, down_done))
        qkv_grad_rows = lax.all_to_all(
            qkv_grad_rows, "gy", split_axis=1, concat_axis=0, tiled=True
        )
        normed_one_grad = settle(product("tc,dc->td", qkv_grad_rows, qkv_w))
        both_sum = jnp.concatenate(
            [product("td,tc->dc", normed_one, qkv_grad_rows).astype(BF), out_sum], axis=1
        )
        terms = jnp.stack(
            [
                jnp.sum(normed_one_grad * unit_one, axis=0),
                jnp.sum(middle_grad * unit_two, axis=0),
                jnp.sum(normed_two_grad * unit_three, axis=0),
                jnp.sum(cot_rows * unit_four, axis=0),
            ]
        )
        delta, terms = to_width_blocks(
            middle_delta + norm_back(normed_one_grad, unit_one, scale_one, gains[0]),
            tally(terms, ny),
            nx,
        )
        down_grad = down_done.astype(F32).T
        both_sum = with_layout_constraint(both_sum, Layout((0, 1)))
        gate_up_done, both_sum, delta, down_grad = lax.optimization_barrier(
            (gate_up_done, both_sum, delta, down_grad)
        )
        both_done = lax.psum_scatter(both_sum, "gx", scatter_dimension=0, tiled=True)
        gate_up_grad = gate_up_done.astype(F32)
        input_grad = cotangent + delta
        qkv_grad = both_done[:, :heads].astype(F32)
        out_grad = both_done[:, heads:].astype(F32).T
        return (outputs, input_grad, qkv_grad, out_grad, gate_up_grad, down_grad) + tuple(
            terms[i] for i in range(4)
        )

    return shards


def solution(mesh):
    placed = (
        P("gy", "gx"),
        P(("gx", "gy"), None),
        P("gx", "gy"),
        P("gy", "gx"),
        P("gx", None, "gy"),
        P("gy", "gx"),
        P("gx"),
        P("gx"),
        P("gx"),
        P("gx"),
        P("gy", "gx"),
    )
    return jax.shard_map(
        make_shards(mesh.shape["gx"], mesh.shape["gy"]),
        mesh=mesh,
        in_specs=placed,
        out_specs=(
            P("gy", "gx"),
            P("gy", "gx"),
            P("gx", "gy"),
            P("gy", "gx"),
            P("gx", None, "gy"),
            P("gy", "gx"),
            P("gx"),
            P("gx"),
            P("gx"),
            P("gx"),
        ),
        check_vma=False,
    )
```

```python
import functools
import math

import jax
import jax.numpy as jnp
from jax import lax
from jax.experimental import pallas as pl
from jax.experimental.layout import Layout, with_layout_constraint
from jax.experimental.pallas import tpu as pltpu
from jax.sharding import PartitionSpec as P

QUERY_HEADS = 8
KEY_VALUE_HEADS = 4
HEAD_SIZE = 256


EPSILON = 1e-06
SOFT_CAP = 50.0
GELU_COEF = 0.7978845608028654
CUBIC_COEF = 0.044715

BF = jnp.bfloat16
F32 = jnp.float32
MESH = pl.DeviceIdType.MESH
PARTS = 4
TILE = 256


def product(form, left, right):
    return jnp.einsum(form, left, right, preferred_element_type=F32)


def gelu_parts(pre_gate):
    inner_arg = GELU_COEF * (pre_gate + CUBIC_COEF * pre_gate * pre_gate * pre_gate)
    tanh_value = jnp.tanh(inner_arg)
    activated = 0.5 * pre_gate * (1.0 + tanh_value)
    derivative = 0.5 * (1.0 + tanh_value) + 0.5 * pre_gate * (
        1.0 - tanh_value * tanh_value
    ) * GELU_COEF * (1.0 + 3.0 * CUBIC_COEF * pre_gate * pre_gate)
    return (activated, derivative)


def block_layout(segment_row):
    length_total = segment_row.shape[0]
    places = jnp.arange(length_total, dtype=jnp.int32)
    same_doc = segment_row[:, None] == segment_row[None, :]
    starts = jnp.min(jnp.where(same_doc, places[None, :], length_total), axis=1)
    allowed = jnp.logical_and(same_doc, places[None, :] <= places[:, None])
    return (places - starts, allowed)


def rope_tables(position):
    half_dim = HEAD_SIZE // 2
    freq_steps = jnp.arange(half_dim, dtype=F32)
    frequency = jnp.exp(freq_steps * (-2.0 * math.log(10000.0) / HEAD_SIZE))
    angles = position.astype(F32)[:, None] * frequency[None, :]
    return (jnp.cos(angles)[:, None, :], jnp.sin(angles)[:, None, :])


def rotate(values, cos_table, sin_table, direction):
    half_dim = values.shape[-1] // 2
    leading = values[..., :half_dim]
    trailing = values[..., half_dim:]
    return jnp.concatenate(
        [
            leading * cos_table - direction * trailing * sin_table,
            trailing * cos_table + direction * leading * sin_table,
        ],
        axis=-1,
    )


def capped_scores(rotated_query, k_rot):
    token_rows = rotated_query.shape[0]
    query_groups = rotated_query.reshape(
        token_rows, KEY_VALUE_HEADS, QUERY_HEADS // KEY_VALUE_HEADS, HEAD_SIZE
    )
    raw_scores = product("tkgd,skd->kgts", query_groups, k_rot) * HEAD_SIZE ** (-0.5)
    return SOFT_CAP * jnp.tanh(raw_scores / SOFT_CAP)


def attention_forward(rows, layout):
    token_rows = rows.shape[0]
    query_span_width = QUERY_HEADS * HEAD_SIZE
    key_value_width = KEY_VALUE_HEADS * HEAD_SIZE
    allowed, cos_table, sin_table = layout
    query_part = (
        rows[:, :query_span_width].astype(F32).reshape(token_rows, QUERY_HEADS, HEAD_SIZE)
    )
    key_slice = (
        rows[:, query_span_width : query_span_width + key_value_width]
        .astype(F32)
        .reshape(token_rows, KEY_VALUE_HEADS, HEAD_SIZE)
    )
    value_slice = rows[:, query_span_width + key_value_width :].reshape(
        token_rows, KEY_VALUE_HEADS, HEAD_SIZE
    )
    rotated_query = rotate(query_part, cos_table, sin_table, 1.0).astype(BF)
    k_rot = rotate(key_slice, cos_table, sin_table, 1.0).astype(BF)
    capped = capped_scores(rotated_query, k_rot)
    log_total = jnp.log(jnp.sum(jnp.where(allowed, jnp.exp(capped), 0.0), axis=-1))
    weights_f = jnp.where(allowed, jnp.exp(capped - log_total[..., None]), 0.0)
    mixing_rows = product("kgts,skd->tkgd", weights_f.astype(BF), value_slice)
    mixing_rows = mixing_rows.astype(BF).reshape(token_rows, query_span_width)
    return (mixing_rows, (rotated_query, k_rot, value_slice, log_total))


def attention_backward(mixing_gradient, mixing_rows, saved, layout):
    rotated_query, k_rot, value_slice, log_total = saved
    token_rows = mixing_gradient.shape[0]
    heads_per_group = QUERY_HEADS // KEY_VALUE_HEADS
    allowed, cos_table, sin_table = layout
    capped = capped_scores(rotated_query, k_rot)
    weights_f = jnp.where(allowed, jnp.exp(capped - log_total[..., None]), 0.0)
    gradient_by_group = mixing_gradient.reshape(
        token_rows, KEY_VALUE_HEADS, heads_per_group, HEAD_SIZE
    )
    output_by_group = mixing_rows.reshape(token_rows, KEY_VALUE_HEADS, heads_per_group, HEAD_SIZE)
    row_delta = product("tkgd,tkgd->kgt", gradient_by_group, output_by_group)
    value_gradient = product("maew,emaq->wmq", weights_f.astype(BF), gradient_by_group)
    weight_grad = product("tkgd,skd->kgts", gradient_by_group, value_slice)
    score_gradient = (
        weights_f
        * (weight_grad - row_delta[..., None])
        * (1.0 - (capped / SOFT_CAP) ** 2)
        * HEAD_SIZE ** (-0.5)
    )
    score_gradient = score_gradient.astype(BF)
    query_gradient = product("kgts,skd->tkgd", score_gradient, k_rot).reshape(
        token_rows, QUERY_HEADS, HEAD_SIZE
    )
    key_gradient = product(
        "maew,emaq->wmq",
        score_gradient,
        rotated_query.reshape(token_rows, KEY_VALUE_HEADS, heads_per_group, HEAD_SIZE),
    )
    query_gradient = rotate(query_gradient, cos_table, sin_table, -1.0)
    key_gradient = rotate(key_gradient, cos_table, sin_table, -1.0)
    return jnp.concatenate(
        [
            query_gradient.reshape(token_rows, QUERY_HEADS * HEAD_SIZE),
            key_gradient.reshape(token_rows, KEY_VALUE_HEADS * HEAD_SIZE),
            value_gradient.reshape(token_rows, KEY_VALUE_HEADS * HEAD_SIZE),
        ],
        axis=1,
    ).astype(BF)


def inverse_rms(values):
    return lax.rsqrt(jnp.mean(values * values, axis=1, keepdims=True) + EPSILON)


def norm_back(grad_rows, unit_rows, scale_rows, gain):
    scaled = grad_rows * gain
    return scale_rows * (scaled - unit_rows * jnp.mean(scaled * unit_rows, axis=1, keepdims=True))


def flip(index, mask):
    return index + mask - 2 * mask * ((index // mask) % 2)


def flip_all(index, masks):
    bit = 1
    while bit <= masks:
        if masks & bit:
            index = flip(index, bit)
        bit *= 2
    return index


def greet(me, bits, lanes=0):
    barrier = pltpu.get_barrier_semaphore()
    for bit in bits:
        pl.semaphore_signal(barrier, inc=1, device_id={"gy": flip(me, bit)}, device_id_type=MESH)
    for d in range(1, lanes):
        other = (lax.axis_index("gx") + d) % lanes
        pl.semaphore_signal(barrier, inc=1, device_id={"gx": other}, device_id_type=MESH)
    pl.semaphore_wait(barrier, len(bits) + max(lanes - 1, 0))


def bit_orders(size):
    bits = []
    bit = 2
    while bit < size:
        bits.append(bit)
        bit *= 2
    return (bits + [1], bits[::-1] + [1])


def lay_out(rows_ref, blocks_ref, strip):
    lanes, count, width = blocks_ref.shape

    @pl.loop(0, count // strip)
    def _(i):
        rows = pl.ds(i * strip, strip)
        for k in range(lanes):
            rows_ref[rows, k * width : (k + 1) * width] = blocks_ref[k, rows].astype(F32)


def cut_up(blocks_ref, rows_ref, strip):
    lanes, count, width = blocks_ref.shape

    @pl.loop(0, count // strip)
    def _(i):
        rows = pl.ds(i * strip, strip)
        for k in range(lanes):
            blocks_ref[k, rows] = rows_ref[rows, k * width : (k + 1) * width].astype(BF)


def swap_start(lanes, side_ref, there_ref, sems):
    me = lax.axis_index("gx")
    own, send_sem, recv_sem = sems
    made = [pltpu.make_async_copy(side_ref.at[me], there_ref.at[me], own)]
    for d in range(1, lanes):
        other = (me + d) % lanes
        made.append(
            pltpu.make_async_remote_copy(
                src_ref=side_ref.at[other],
                dst_ref=there_ref.at[me],
                send_sem=send_sem.at[d],
                recv_sem=recv_sem.at[d],
                device_id={"gx": other},
                device_id_type=MESH,
            )
        )
    for copy in made:
        copy.start()
    return made


def swap_sems(lanes):
    return [
        pltpu.SemaphoreType.DMA,
        pltpu.SemaphoreType.DMA((lanes,)),
        pltpu.SemaphoreType.DMA((lanes,)),
    ]


def greet_lanes(lanes):
    barrier = pltpu.get_barrier_semaphore()
    for d in range(1, lanes):
        other = (lax.axis_index("gx") + d) % lanes
        pl.semaphore_signal(barrier, inc=1, device_id={"gx": other}, device_id_type=MESH)
    pl.semaphore_wait(barrier, lanes - 1)


def gather_rows_kernel(lanes, native_ref, small_ref, rows_ref, wide_ref, *scratch):
    send_ref, there_ref, small_all, *sems = scratch
    big_sems, small_sems = sems[:3], sems[3:]
    fold, pair = send_ref.shape[1:]
    width = pair // 2
    strip = 16
    for j in range(lanes):
        for side in range(2):

            @pl.loop(0, fold // strip)
            def _(i):
                rows = pl.ds((2 * j + side) * fold + i * strip, strip)
                send_ref[j, pl.ds(i * strip, strip), side * width : (side + 1) * width] = (
                    native_ref[rows].astype(BF)
                )

    greet_lanes(lanes)
    copies = swap_start(lanes, send_ref, there_ref, big_sems)
    copies += hand_round(lanes, small_ref, small_all, small_sems)
    for copy in copies:
        copy.wait()
    for k in range(lanes):
        columns = slice(k * width, (k + 1) * width)
        wide_ref[:, columns] = small_all[k]
        for side in range(2):

            @pl.loop(0, fold // strip)
            def _(i):
                rows_ref[pl.ds(side * fold + i * strip, strip), columns] = there_ref[
                    k, pl.ds(i * strip, strip), side * width : (side + 1) * width
                ].astype(F32)


def scatter_rows_kernel(lanes, rows_ref, wide_ref, native_ref, small_ref, *scratch):
    send_ref, there_ref, small_send, small_all, *sems = scratch
    big_sems, small_sems = sems[:3], sems[3:]
    fold, pair = send_ref.shape[1:]
    width = pair // 2
    strip = 16
    for j in range(lanes):
        columns = slice(j * width, (j + 1) * width)
        small_send[j] = wide_ref[:, columns]
        for side in range(2):

            @pl.loop(0, fold // strip)
            def _(i):
                send_ref[j, pl.ds(i * strip, strip), side * width : (side + 1) * width] = rows_ref[
                    pl.ds(side * fold + i * strip, strip), columns
                ].astype(BF)

    greet_lanes(lanes)
    copies = swap_start(lanes, send_ref, there_ref, big_sems)
    copies += swap_start(lanes, small_send, small_all, small_sems)
    for copy in copies:
        copy.wait()
    total = small_all[0]
    for k in range(1, lanes):
        total = total + small_all[k]
    small_ref[...] = total
    for k in range(lanes):
        for side in range(2):

            @pl.loop(0, fold // strip)
            def _(i):
                rows = pl.ds((2 * k + side) * fold + i * strip, strip)
                native_ref[rows] = there_ref[
                    k, pl.ds(i * strip, strip), side * width : (side + 1) * width
                ].astype(F32)


def hand_round(lanes, own_ref, all_ref, sems):
    me = lax.axis_index("gx")
    own, send_sem, recv_sem = sems
    made = [pltpu.make_async_copy(own_ref, all_ref.at[me], own)]
    for d in range(1, lanes):
        made.append(
            pltpu.make_async_remote_copy(
                src_ref=own_ref,
                dst_ref=all_ref.at[me],
                send_sem=send_sem.at[d],
                recv_sem=recv_sem.at[d],
                device_id={"gx": (me + d) % lanes},
                device_id_type=MESH,
            )
        )
    for copy in made:
        copy.start()
    return made


def exchange(kernel, lanes, big, small, outs, extra, call):
    total, width = big.shape
    space = pl.BlockSpec(memory_space=pltpu.VMEM)
    count = total * width // (lanes * outs[2])
    block = (lanes, count // 2, 2 * outs[2])
    cut = (lanes, small.shape[0], outs[2])
    return pl.pallas_call(
        functools.partial(kernel, lanes),
        out_shape=[jax.ShapeDtypeStruct(v, F32) for v in outs[:2]],
        in_specs=[space] * 2,
        out_specs=[space] * 2,
        scratch_shapes=[pltpu.VMEM(block, BF), pltpu.VMEM(block, BF)]
        + [pltpu.VMEM(cut, F32)] * (1 + extra)
        + swap_sems(lanes)
        + swap_sems(lanes),
        compiler_params=pltpu.CompilerParams(
            collective_id=call, has_side_effects=True, vmem_limit_bytes=32 << 20
        ),
        cost_estimate=pl.CostEstimate(
            flops=0, bytes_accessed=total * width * 16, transcendentals=0
        ),
        name="exchange",
    )(big, small)


def to_whole_rows(values, small, lanes):
    total, width = values.shape
    outs = ((total // lanes, lanes * width), (small.shape[0], lanes * width), width)
    return exchange(gather_rows_kernel, lanes, values, small, outs, 0, 9)


def to_width_blocks(rows, small, lanes):
    count, whole = rows.shape
    width = whole // lanes
    outs = ((count * lanes, width), (small.shape[0], width), width)
    return exchange(scatter_rows_kernel, lanes, rows, small, outs, 1, 10)


def spread_kernel(size, lanes, *refs):
    if lanes:
        own_ref, rows_ref, all_ref, there_ref, local_sem, send_sem, recv_sem, *rest = refs
        side_ref, *sems = rest
    else:
        own_ref, all_ref, local_sem, send_sem, recv_sem = refs
    me = lax.axis_index("gy")
    orders = bit_orders(size)
    half = own_ref.shape[0] // 2
    greet(me, orders[0], lanes)
    keep = pltpu.make_async_copy(own_ref, all_ref.at[me], local_sem)
    keep.start()
    copies = {}
    arrival = {}

    def copy(h, bit, r):
        n = len(copies)
        rows = pl.ds(h * half, half)
        where = flip_all(me, r)
        source = own_ref.at[rows] if r == 0 else all_ref.at[where, rows]
        made = pltpu.make_async_remote_copy(
            src_ref=source,
            dst_ref=all_ref.at[where, rows],
            send_sem=send_sem.at[n],
            recv_sem=recv_sem.at[n],
            device_id={"gy": flip(me, bit)},
            device_id_type=MESH,
        )
        copies[h, bit, r] = made
        arrival[h, r ^ bit] = made
        made.start()

    for step in range(len(orders[0])):
        for h in range(2):
            copy(h, orders[h][step], 0)
    swapped = []
    if lanes:
        cut_up(side_ref, rows_ref, 16)
        swapped = swap_start(lanes, side_ref, there_ref, sems)
    landed = set()

    def land(h, r):
        if (h, r) not in landed:
            landed.add((h, r))
            arrival[h, r].wait_recv()

    held = [[0], [0]]
    for step in range(len(orders[0])):
        for h in range(2):
            bit = orders[h][step]
            for r in held[h]:
                if r:
                    land(h, r)
                    copy(h, bit, r)
        for h in range(2):
            held[h] = held[h] + [r ^ orders[h][step] for r in held[h]]
    for h in range(2):
        for r in range(1, size):
            land(h, r)
    for made in copies.values():
        made.wait_send()
    for copy in [keep] + swapped:
        copy.wait()


def spread(values, side=None):
    size = lax.axis_size("gy")
    values = values.astype(BF)
    rows, width = values.shape
    count = 2 * (size - 1)
    sides = [] if side is None else [side]
    lanes = 0 if side is None else lax.axis_size("gx")
    blocks = (lanes, rows, width // max(lanes, 1))
    space = pl.BlockSpec(memory_space=pltpu.VMEM)
    out = pl.pallas_call(
        functools.partial(spread_kernel, size, lanes),
        out_shape=[jax.ShapeDtypeStruct((size, rows, width), values.dtype)]
        + [jax.ShapeDtypeStruct(blocks, BF) for v in sides],
        in_specs=[space] * (1 + len(sides)),
        out_specs=[pl.BlockSpec(memory_space=pltpu.HBM)] * (1 + len(sides)),
        scratch_shapes=[
            pltpu.SemaphoreType.DMA,
            pltpu.SemaphoreType.DMA((count,)),
            pltpu.SemaphoreType.DMA((count,)),
        ]
        + ([pltpu.VMEM(blocks, BF)] + swap_sems(lanes) if lanes else []),
        compiler_params=pltpu.CompilerParams(
            collective_id=4 if lanes else 0, has_side_effects=True, vmem_limit_bytes=32 << 20
        ),
        cost_estimate=pl.CostEstimate(
            flops=0, bytes_accessed=size * rows * width * 16, transcendentals=0
        ),
        name="spread",
    )(values, *sides)
    whole = out[0].reshape(size * rows, width)
    return (whole, out[1]) if lanes else whole


def settle_kernel(size, lanes, fused, *refs):
    if fused:
        left_ref, right_ref, *refs = refs
        *refs, picked, weights, product_ref, left_sem, right_sem = refs
        refs = [product_ref] + refs
    if lanes:
        parts_ref, side_ref, sum_ref, rows_ref, came, kept, send_sem, recv_sem, *rest = refs
        there_ref, *sems = rest
    else:
        parts_ref, sum_ref, came, kept, send_sem, recv_sem = refs
    me = lax.axis_index("gy")
    orders = tuple(order[::-1] for order in bit_orders(size)) * (PARTS // 2)
    half = sum_ref.shape[0] // PARTS
    strip = 16
    def left_copy(j):
        count = left_ref.shape[1]
        return pltpu.make_async_copy(
            left_ref.at[flip_all(me, turn[j])],
            picked.at[pl.ds(j * count, count)],
            left_sem.at[j],
        )

    def right_copy(i):
        rows = pl.ds(pl.multiple_of(i * TILE, TILE), TILE)
        return pltpu.make_async_copy(right_ref.at[rows], weights.at[rows], right_sem.at[i])

    def multiply(low, high):
        count = left_ref.shape[1]
        for j in range(low, high):
            left_copy(j).wait()

        @pl.loop(0, weights.shape[0] // TILE)
        def _(i):
            if low == 0:
                right_copy(i).wait()
            columns = pl.ds(pl.multiple_of(i * TILE, TILE), TILE)
            block = lax.dot_general(
                picked[low * count : high * count],
                weights[columns],
                (((1,), (1,)), ((), ())),
                preferred_element_type=F32,
            ).astype(BF)
            for j in range(low, high):
                parts_ref[flip_all(me, turn[j]), :, columns] = block[
                    (j - low) * count : (j - low + 1) * count
                ]

    turn = [r for r in range(size) if r & 1] + [r for r in range(size - 1, -1, -1) if not r & 1]
    if fused:
        for j in range(size // 2):
            left_copy(j).start()
        for i in range(weights.shape[0] // TILE):
            right_copy(i).start()
        for j in range(size // 2, size):
            left_copy(j).start()
    greet(me, orders[0], lanes)
    swapped = swap_start(lanes, side_ref, there_ref, sems) if lanes else []
    slot = {}
    for h in range(PARTS):
        held = list(range(size))
        for step, bit in enumerate(orders[h]):
            held = [r for r in held if not r & bit]
            for r in held:
                slot[h, step, r] = len(slot)
    copies = {}

    def view(h, step, r):
        if step == 0:
            return parts_ref.at[flip_all(me, r), pl.ds(h * half, half)]
        return kept.at[h, r]

    def send(h, step):
        bit = orders[h][step]
        gone = set()
        for b in orders[h][:step]:
            gone.add(b)
        for r in range(size):
            if r & bit and not any(r & b for b in gone):
                n = slot[h, step, r ^ bit]
                made = pltpu.make_async_remote_copy(
                    src_ref=view(h, step, r),
                    dst_ref=came.at[n],
                    send_sem=send_sem.at[n],
                    recv_sem=recv_sem.at[n],
                    device_id={"gy": flip(me, bit)},
                    device_id_type=MESH,
                )
                copies[h, step, r ^ bit] = made
                made.start()

    def gather(h, step, r, last):
        n = slot[h, step, r]
        copies[h, step, r].wait_recv()

        @pl.loop(0, half // strip)
        def _(i):
            rows = pl.ds(i * strip, strip)
            total = view(h, step, r)[rows].astype(F32) + came[n, rows].astype(F32)
            if last:
                sum_ref[pl.ds(h * half + i * strip, strip)] = total
            else:
                kept[h, r, rows] = total.astype(BF)

    steps = len(orders[0])
    if fused:
        multiply(0, size // 2)
    for h in range(PARTS):
        send(h, 0)
    if fused:
        multiply(size // 2, size - 1)
    for step in range(steps):
        if lanes and step == steps - 1:
            for copy in swapped:
                copy.wait()
            lay_out(rows_ref, there_ref, strip)
        for h in range(PARTS):
            bits = orders[h][: step + 1]
            later = orders[h][step + 1] if step + 1 < steps else 0
            left = [r for r in range(size) if not any(r & b for b in bits)]
            for r in left:
                if r & later:
                    gather(h, step, r, False)
            if later:
                send(h, step + 1)
            for r in left:
                if not r & later and not (fused and step == 0):
                    gather(h, step, r, step == steps - 1)
        if fused and step == 0:
            multiply(size - 1, size)
            for h in range(PARTS):
                for r in range(size):
                    if not r & orders[h][0] and not r & orders[h][1]:
                        gather(h, 0, r, False)
    for made in copies.values():
        made.wait_send()


def settle(parts, side=None, right=None):
    size = lax.axis_size("gy")
    parts = parts.astype(BF)
    total, inner = parts.shape
    width = inner if right is None else right.shape[0]
    rows = total // size
    count = PARTS * (size - 1)
    sides = [] if side is None else [side]
    rights = [] if right is None else [right]
    lanes = 0 if side is None else side.shape[0]
    space = pl.BlockSpec(memory_space=pltpu.VMEM)
    scratch = [
        pltpu.VMEM((count, rows // PARTS, width), BF),
        pltpu.VMEM((PARTS, size, rows // PARTS, width), BF),
        pltpu.SemaphoreType.DMA((count,)),
        pltpu.SemaphoreType.DMA((count,)),
    ]
    if lanes:
        scratch += [pltpu.VMEM(side.shape, side.dtype)] + swap_sems(lanes)
    if rights:
        scratch += [
            pltpu.VMEM((total, inner), BF),
            pltpu.VMEM((width, inner), BF),
            pltpu.VMEM((size, rows, width), BF),
            pltpu.SemaphoreType.DMA((size,)),
            pltpu.SemaphoreType.DMA((width // TILE,)),
        ]
    out = pl.pallas_call(
        functools.partial(settle_kernel, size, lanes, bool(rights)),
        out_shape=[jax.ShapeDtypeStruct((rows, width), F32)] * (1 + len(sides)),
        in_specs=[pl.BlockSpec(memory_space=pl.ANY)] * (2 * len(rights))
        + [space] * (1 - len(rights) + len(sides)),
        out_specs=[space] * (1 + len(sides)),
        scratch_shapes=scratch,
        compiler_params=pltpu.CompilerParams(
            collective_id=5 if lanes else 1, has_side_effects=True, vmem_limit_bytes=40 << 20
        ),
        cost_estimate=pl.CostEstimate(
            flops=0, bytes_accessed=total * width * 16, transcendentals=0
        ),
        name="settle",
    )
    operands = [parts.reshape(size, rows, inner)] + rights
    if rights:
        operands = [pltpu.with_memory_space_constraint(v, pltpu.HBM) for v in operands]
    out = out(*operands, *sides)
    return out if lanes else out[0]


def tally_kernel(size, own_ref, sum_ref, came, send_sem, recv_sem):
    me = lax.axis_index("gy")
    barrier = pltpu.get_barrier_semaphore()
    for d in range(1, size):
        pl.semaphore_signal(
            barrier, inc=1, device_id={"gy": (me + d) % size}, device_id_type=MESH
        )
    pl.semaphore_wait(barrier, size - 1)
    copies = []
    for d in range(1, size):
        made = pltpu.make_async_remote_copy(
            src_ref=own_ref,
            dst_ref=came.at[d],
            send_sem=send_sem.at[d],
            recv_sem=recv_sem.at[d],
            device_id={"gy": (me + d) % size},
            device_id_type=MESH,
        )
        made.start()
        copies.append(made)
    total = own_ref[...]
    for d in range(1, size):
        copies[d - 1].wait_recv()
        total = total + came[d]
    sum_ref[...] = total
    for made in copies:
        made.wait_send()


def tally(values, size):
    return pl.pallas_call(
        functools.partial(tally_kernel, size),
        out_shape=jax.ShapeDtypeStruct(values.shape, F32),
        in_specs=[pl.BlockSpec(memory_space=pltpu.VMEM)],
        out_specs=pl.BlockSpec(memory_space=pltpu.VMEM),
        scratch_shapes=[
            pltpu.VMEM((size,) + values.shape, F32),
            pltpu.SemaphoreType.DMA((size,)),
            pltpu.SemaphoreType.DMA((size,)),
        ],
        compiler_params=pltpu.CompilerParams(collective_id=2, has_side_effects=True),
        name="tally",
    )(values)


def make_shards(nx, ny):
    blocks = [((b // ny) * ny + b % ny, (b % nx) * ny + b // nx) for b in range(nx * ny)]

    def shards(
        inputs,
        segment_ids,
        qkv_weight,
        out_weight,
        gate_up_weight,
        down_weight,
        first_gain,
        second_gain,
        third_gain,
        fourth_gain,
        cotangent,
    ):
        width = inputs.shape[1]

        own = inputs.shape[0] // nx
        heads = qkv_weight.shape[1]
        both_w = lax.all_gather(
            jnp.concatenate([qkv_weight, out_weight.T], axis=1), "gx", axis=0, tiled=True
        )
        gains = jnp.stack([first_gain, second_gain, third_gain, fourth_gain])
        gains, both_w = lax.optimization_barrier((gains, both_w))
        x_rows, gains = to_whole_rows(inputs, gains, nx)
        gains = gains[:, None, :]
        gate_up_w = lax.all_gather(gate_up_weight, "gx", axis=0, tiled=True)
        down_w = lax.all_gather(down_weight.T, "gx", axis=0, tiled=True)
        qkv_w, out_w = both_w[:, :heads], both_w[:, heads:]

        segment_row = lax.ppermute(segment_ids[0], ("gx", "gy"), blocks)
        position, allowed = block_layout(segment_row)
        layout = (allowed,) + rope_tables(position)

        scale_one = inverse_rms(x_rows)
        unit_one = x_rows * scale_one
        normed_one = spread(unit_one * gains[0])
        rows = product("td,dc->tc", normed_one, qkv_w).astype(BF)
        rows = lax.all_to_all(rows, "gy", split_axis=0, concat_axis=1, tiled=True)
        mixing_rows, saved = attention_forward(rows, layout)
        mixed = lax.all_to_all(mixing_rows, "gy", split_axis=1, concat_axis=0, tiled=True)
        attn_branch = settle(product("tc,dc->td", mixed, out_w))
        scale_two = inverse_rms(attn_branch)
        unit_two = attn_branch * scale_two
        attn_term = unit_two * gains[1]
        middle = x_rows + attn_term
        scale_three = inverse_rms(middle)
        unit_three = middle * scale_three
        normed_two = spread(unit_three * gains[2])
        pre_gate = product("td,df->tf", normed_two, gate_up_w[:, 0, :])
        up_part = product("td,df->tf", normed_two, gate_up_w[:, 1, :])
        value, slope = gelu_parts(pre_gate)
        hidden = (value * up_part).astype(BF)
        ff_branch, cot_rows = settle(
            hidden, cotangent.astype(BF).reshape(nx, own, width), down_w
        )
        scale_four = inverse_rms(ff_branch)
        unit_four = ff_branch * scale_four
        ff_grad, delta = spread(
            norm_back(cot_rows, unit_four, scale_four, gains[3]),
            attn_term + unit_four * gains[3],
        )
        outputs = inputs + delta.reshape(inputs.shape).astype(F32)

        down_sum = product("td,tf->df", ff_grad, hidden).astype(BF)
        down_sum, ff_grad = lax.optimization_barrier((down_sum, ff_grad))
        down_done = lax.psum_scatter(down_sum, "gx", scatter_dimension=0, tiled=True)
        hidden_grad = product("td,df->tf", ff_grad, down_w)
        gate_grad = (hidden_grad * up_part * slope).astype(BF)
        up_grad = (hidden_grad * value).astype(BF)
        gate_up_sum = jnp.stack(
            [
                product("td,tf->df", normed_two, gate_grad).astype(BF),
                product("td,tf->df", normed_two, up_grad).astype(BF),
            ],
            axis=1,
        )
        gate_up_sum, gate_grad, up_grad = lax.optimization_barrier(
            (gate_up_sum, gate_grad, up_grad)
        )
        gate_up_done = lax.psum_scatter(gate_up_sum, "gx", scatter_dimension=0, tiled=True)
        normed_two_grad = settle(
            product("tf,df->td", gate_grad, gate_up_w[:, 0, :])
            + product("tf,df->td", up_grad, gate_up_w[:, 1, :])
        )
        middle_delta = norm_back(normed_two_grad, unit_three, scale_three, gains[2])
        middle_grad = cot_rows + middle_delta
        branch_grad = spread(norm_back(middle_grad, unit_two, scale_two, gains[1]))
        out_sum = product("td,tc->dc", branch_grad, mixed).astype(BF)
        mixing_gradient = product("td,dc->tc", branch_grad, out_w).astype(BF)
        mixing_gradient = lax.all_to_all(
            mixing_gradient, "gy", split_axis=0, concat_axis=1, tiled=True
        )
        qkv_grad_rows = attention_backward(mixing_gradient, mixing_rows, saved, layout)
        qkv_grad_rows, down_done = lax.optimization_barrier((qkv_grad_rows, down_done))
        qkv_grad_rows = lax.all_to_all(
            qkv_grad_rows, "gy", split_axis=1, concat_axis=0, tiled=True
        )
        normed_one_grad = settle(product("tc,dc->td", qkv_grad_rows, qkv_w))
        both_sum = jnp.concatenate(
            [product("td,tc->dc", normed_one, qkv_grad_rows).astype(BF), out_sum], axis=1
        )
        terms = jnp.stack(
            [
                jnp.sum(normed_one_grad * unit_one, axis=0),
                jnp.sum(middle_grad * unit_two, axis=0),
                jnp.sum(normed_two_grad * unit_three, axis=0),
                jnp.sum(cot_rows * unit_four, axis=0),
            ]
        )
        delta, terms = to_width_blocks(
            middle_delta + norm_back(normed_one_grad, unit_one, scale_one, gains[0]),
            tally(terms, ny),
            nx,
        )
        down_grad = down_done.astype(F32).T
        both_sum = with_layout_constraint(both_sum, Layout((0, 1)))
        gate_up_done, both_sum, delta, down_grad = lax.optimization_barrier(
            (gate_up_done, both_sum, delta, down_grad)
        )
        both_done = lax.psum_scatter(both_sum, "gx", scatter_dimension=0, tiled=True)
        gate_up_grad = gate_up_done.astype(F32)
        input_grad = cotangent + delta
        qkv_grad = both_done[:, :heads].astype(F32)
        out_grad = both_done[:, heads:].astype(F32).T
        return (outputs, input_grad, qkv_grad, out_grad, gate_up_grad, down_grad) + tuple(
            terms[i] for i in range(4)
        )

    return shards


def solution(mesh):
    placed = (
        P("gy", "gx"),
        P(("gx", "gy"), None),
        P("gx", "gy"),
        P("gy", "gx"),
        P("gx", None, "gy"),
        P("gy", "gx"),
        P("gx"),
        P("gx"),
        P("gx"),
        P("gx"),
        P("gy", "gx"),
    )
    return jax.shard_map(
        make_shards(mesh.shape["gx"], mesh.shape["gy"]),
        mesh=mesh,
        in_specs=placed,
        out_specs=(
            P("gy", "gx"),
            P("gy", "gx"),
            P("gx", "gy"),
            P("gy", "gx"),
            P("gx", None, "gy"),
            P("gy", "gx"),
            P("gx"),
            P("gx"),
            P("gx"),
            P("gx"),
        ),
        check_vma=False,
    )
```

```python
import functools
import math

import jax
import jax.numpy as jnp
from jax import lax
from jax.experimental import pallas as pl
from jax.experimental.layout import Layout, with_layout_constraint
from jax.experimental.pallas import tpu as pltpu
from jax.sharding import PartitionSpec as P

QUERY_HEADS = 8
KEY_VALUE_HEADS = 4
HEAD_SIZE = 256


EPSILON = 1e-06
SOFT_CAP = 50.0
GELU_COEF = 0.7978845608028654
CUBIC_COEF = 0.044715

BF = jnp.bfloat16
F32 = jnp.float32
MESH = pl.DeviceIdType.MESH
PARTS = 4
TILE = 768


def product(form, left, right):
    return jnp.einsum(form, left, right, preferred_element_type=F32)


def gelu_parts(pre_gate):
    inner_arg = GELU_COEF * (pre_gate + CUBIC_COEF * pre_gate * pre_gate * pre_gate)
    tanh_value = jnp.tanh(inner_arg)
    activated = 0.5 * pre_gate * (1.0 + tanh_value)
    derivative = 0.5 * (1.0 + tanh_value) + 0.5 * pre_gate * (
        1.0 - tanh_value * tanh_value
    ) * GELU_COEF * (1.0 + 3.0 * CUBIC_COEF * pre_gate * pre_gate)
    return (activated, derivative)


def block_layout(segment_row):
    length_total = segment_row.shape[0]
    places = jnp.arange(length_total, dtype=jnp.int32)
    same_doc = segment_row[:, None] == segment_row[None, :]
    starts = jnp.min(jnp.where(same_doc, places[None, :], length_total), axis=1)
    allowed = jnp.logical_and(same_doc, places[None, :] <= places[:, None])
    return (places - starts, allowed)


def rope_tables(position):
    half_dim = HEAD_SIZE // 2
    freq_steps = jnp.arange(half_dim, dtype=F32)
    frequency = jnp.exp(freq_steps * (-2.0 * math.log(10000.0) / HEAD_SIZE))
    angles = position.astype(F32)[:, None] * frequency[None, :]
    return (jnp.cos(angles)[:, None, :], jnp.sin(angles)[:, None, :])


def rotate(values, cos_table, sin_table, direction):
    half_dim = values.shape[-1] // 2
    leading = values[..., :half_dim]
    trailing = values[..., half_dim:]
    return jnp.concatenate(
        [
            leading * cos_table - direction * trailing * sin_table,
            trailing * cos_table + direction * leading * sin_table,
        ],
        axis=-1,
    )


def capped_scores(rotated_query, k_rot):
    token_rows = rotated_query.shape[0]
    query_groups = rotated_query.reshape(
        token_rows, KEY_VALUE_HEADS, QUERY_HEADS // KEY_VALUE_HEADS, HEAD_SIZE
    )
    raw_scores = product("tkgd,skd->kgts", query_groups, k_rot) * HEAD_SIZE ** (-0.5)
    return SOFT_CAP * jnp.tanh(raw_scores / SOFT_CAP)


def attention_forward(rows, layout):
    token_rows = rows.shape[0]
    query_span_width = QUERY_HEADS * HEAD_SIZE
    key_value_width = KEY_VALUE_HEADS * HEAD_SIZE
    allowed, cos_table, sin_table = layout
    query_part = (
        rows[:, :query_span_width].astype(F32).reshape(token_rows, QUERY_HEADS, HEAD_SIZE)
    )
    key_slice = (
        rows[:, query_span_width : query_span_width + key_value_width]
        .astype(F32)
        .reshape(token_rows, KEY_VALUE_HEADS, HEAD_SIZE)
    )
    value_slice = rows[:, query_span_width + key_value_width :].reshape(
        token_rows, KEY_VALUE_HEADS, HEAD_SIZE
    )
    rotated_query = rotate(query_part, cos_table, sin_table, 1.0).astype(BF)
    k_rot = rotate(key_slice, cos_table, sin_table, 1.0).astype(BF)
    capped = capped_scores(rotated_query, k_rot)
    log_total = jnp.log(jnp.sum(jnp.where(allowed, jnp.exp(capped), 0.0), axis=-1))
    weights_f = jnp.where(allowed, jnp.exp(capped - log_total[..., None]), 0.0)
    mixing_rows = product("kgts,skd->tkgd", weights_f.astype(BF), value_slice)
    mixing_rows = mixing_rows.astype(BF).reshape(token_rows, query_span_width)
    return (mixing_rows, (rotated_query, k_rot, value_slice, log_total))


def attention_backward(mixing_gradient, mixing_rows, saved, layout):
    rotated_query, k_rot, value_slice, log_total = saved
    token_rows = mixing_gradient.shape[0]
    heads_per_group = QUERY_HEADS // KEY_VALUE_HEADS
    allowed, cos_table, sin_table = layout
    capped = capped_scores(rotated_query, k_rot)
    weights_f = jnp.where(allowed, jnp.exp(capped - log_total[..., None]), 0.0)
    gradient_by_group = mixing_gradient.reshape(
        token_rows, KEY_VALUE_HEADS, heads_per_group, HEAD_SIZE
    )
    output_by_group = mixing_rows.reshape(token_rows, KEY_VALUE_HEADS, heads_per_group, HEAD_SIZE)
    row_delta = product("tkgd,tkgd->kgt", gradient_by_group, output_by_group)
    value_gradient = product("maew,emaq->wmq", weights_f.astype(BF), gradient_by_group)
    weight_grad = product("tkgd,skd->kgts", gradient_by_group, value_slice)
    score_gradient = (
        weights_f
        * (weight_grad - row_delta[..., None])
        * (1.0 - (capped / SOFT_CAP) ** 2)
        * HEAD_SIZE ** (-0.5)
    )
    score_gradient = score_gradient.astype(BF)
    query_gradient = product("kgts,skd->tkgd", score_gradient, k_rot).reshape(
        token_rows, QUERY_HEADS, HEAD_SIZE
    )
    key_gradient = product(
        "maew,emaq->wmq",
        score_gradient,
        rotated_query.reshape(token_rows, KEY_VALUE_HEADS, heads_per_group, HEAD_SIZE),
    )
    query_gradient = rotate(query_gradient, cos_table, sin_table, -1.0)
    key_gradient = rotate(key_gradient, cos_table, sin_table, -1.0)
    return jnp.concatenate(
        [
            query_gradient.reshape(token_rows, QUERY_HEADS * HEAD_SIZE),
            key_gradient.reshape(token_rows, KEY_VALUE_HEADS * HEAD_SIZE),
            value_gradient.reshape(token_rows, KEY_VALUE_HEADS * HEAD_SIZE),
        ],
        axis=1,
    ).astype(BF)


def inverse_rms(values):
    return lax.rsqrt(jnp.mean(values * values, axis=1, keepdims=True) + EPSILON)


def norm_back(grad_rows, unit_rows, scale_rows, gain):
    scaled = grad_rows * gain
    return scale_rows * (scaled - unit_rows * jnp.mean(scaled * unit_rows, axis=1, keepdims=True))


def flip(index, mask):
    return index + mask - 2 * mask * ((index // mask) % 2)


def flip_all(index, masks):
    bit = 1
    while bit <= masks:
        if masks & bit:
            index = flip(index, bit)
        bit *= 2
    return index


def greet(me, bits, lanes=0):
    barrier = pltpu.get_barrier_semaphore()
    for bit in bits:
        pl.semaphore_signal(barrier, inc=1, device_id={"gy": flip(me, bit)}, device_id_type=MESH)
    for d in range(1, lanes):
        other = (lax.axis_index("gx") + d) % lanes
        pl.semaphore_signal(barrier, inc=1, device_id={"gx": other}, device_id_type=MESH)
    pl.semaphore_wait(barrier, len(bits) + max(lanes - 1, 0))


def bit_orders(size):
    bits = []
    bit = 2
    while bit < size:
        bits.append(bit)
        bit *= 2
    return (bits + [1], bits[::-1] + [1])


def lay_out(rows_ref, blocks_ref, strip):
    lanes, count, width = blocks_ref.shape

    @pl.loop(0, count // strip)
    def _(i):
        rows = pl.ds(i * strip, strip)
        for k in range(lanes):
            rows_ref[rows, k * width : (k + 1) * width] = blocks_ref[k, rows].astype(F32)


def cut_up(blocks_ref, rows_ref, strip):
    lanes, count, width = blocks_ref.shape

    @pl.loop(0, count // strip)
    def _(i):
        rows = pl.ds(i * strip, strip)
        for k in range(lanes):
            blocks_ref[k, rows] = rows_ref[rows, k * width : (k + 1) * width].astype(BF)


def swap_start(lanes, side_ref, there_ref, sems):
    me = lax.axis_index("gx")
    own, send_sem, recv_sem = sems
    made = [pltpu.make_async_copy(side_ref.at[me], there_ref.at[me], own)]
    for d in range(1, lanes):
        other = (me + d) % lanes
        made.append(
            pltpu.make_async_remote_copy(
                src_ref=side_ref.at[other],
                dst_ref=there_ref.at[me],
                send_sem=send_sem.at[d],
                recv_sem=recv_sem.at[d],
                device_id={"gx": other},
                device_id_type=MESH,
            )
        )
    for copy in made:
        copy.start()
    return made


def swap_sems(lanes):
    return [
        pltpu.SemaphoreType.DMA,
        pltpu.SemaphoreType.DMA((lanes,)),
        pltpu.SemaphoreType.DMA((lanes,)),
    ]


def greet_lanes(lanes):
    barrier = pltpu.get_barrier_semaphore()
    for d in range(1, lanes):
        other = (lax.axis_index("gx") + d) % lanes
        pl.semaphore_signal(barrier, inc=1, device_id={"gx": other}, device_id_type=MESH)
    pl.semaphore_wait(barrier, lanes - 1)


def gather_rows_kernel(lanes, native_ref, small_ref, rows_ref, wide_ref, *scratch):
    send_ref, there_ref, small_all, *sems = scratch
    big_sems, small_sems = sems[:3], sems[3:]
    fold, pair = send_ref.shape[1:]
    width = pair // 2
    strip = 16
    for j in range(lanes):
        for side in range(2):

            @pl.loop(0, fold // strip)
            def _(i):
                rows = pl.ds((2 * j + side) * fold + i * strip, strip)
                send_ref[j, pl.ds(i * strip, strip), side * width : (side + 1) * width] = (
                    native_ref[rows].astype(BF)
                )

    greet_lanes(lanes)
    copies = swap_start(lanes, send_ref, there_ref, big_sems)
    copies += hand_round(lanes, small_ref, small_all, small_sems)
    for copy in copies:
        copy.wait()
    for k in range(lanes):
        columns = slice(k * width, (k + 1) * width)
        wide_ref[:, columns] = small_all[k]
        for side in range(2):

            @pl.loop(0, fold // strip)
            def _(i):
                rows_ref[pl.ds(side * fold + i * strip, strip), columns] = there_ref[
                    k, pl.ds(i * strip, strip), side * width : (side + 1) * width
                ].astype(F32)


def scatter_rows_kernel(lanes, rows_ref, wide_ref, native_ref, small_ref, *scratch):
    send_ref, there_ref, small_send, small_all, *sems = scratch
    big_sems, small_sems = sems[:3], sems[3:]
    fold, pair = send_ref.shape[1:]
    width = pair // 2
    strip = 16
    for j in range(lanes):
        columns = slice(j * width, (j + 1) * width)
        small_send[j] = wide_ref[:, columns]
        for side in range(2):

            @pl.loop(0, fold // strip)
            def _(i):
                send_ref[j, pl.ds(i * strip, strip), side * width : (side + 1) * width] = rows_ref[
                    pl.ds(side * fold + i * strip, strip), columns
                ].astype(BF)

    greet_lanes(lanes)
    copies = swap_start(lanes, send_ref, there_ref, big_sems)
    copies += swap_start(lanes, small_send, small_all, small_sems)
    for copy in copies:
        copy.wait()
    total = small_all[0]
    for k in range(1, lanes):
        total = total + small_all[k]
    small_ref[...] = total
    for k in range(lanes):
        for side in range(2):

            @pl.loop(0, fold // strip)
            def _(i):
                rows = pl.ds((2 * k + side) * fold + i * strip, strip)
                native_ref[rows] = there_ref[
                    k, pl.ds(i * strip, strip), side * width : (side + 1) * width
                ].astype(F32)


def hand_round(lanes, own_ref, all_ref, sems):
    me = lax.axis_index("gx")
    own, send_sem, recv_sem = sems
    made = [pltpu.make_async_copy(own_ref, all_ref.at[me], own)]
    for d in range(1, lanes):
        made.append(
            pltpu.make_async_remote_copy(
                src_ref=own_ref,
                dst_ref=all_ref.at[me],
                send_sem=send_sem.at[d],
                recv_sem=recv_sem.at[d],
                device_id={"gx": (me + d) % lanes},
                device_id_type=MESH,
            )
        )
    for copy in made:
        copy.start()
    return made


def exchange(kernel, lanes, big, small, outs, extra, call):
    total, width = big.shape
    space = pl.BlockSpec(memory_space=pltpu.VMEM)
    count = total * width // (lanes * outs[2])
    block = (lanes, count // 2, 2 * outs[2])
    cut = (lanes, small.shape[0], outs[2])
    return pl.pallas_call(
        functools.partial(kernel, lanes),
        out_shape=[jax.ShapeDtypeStruct(v, F32) for v in outs[:2]],
        in_specs=[space] * 2,
        out_specs=[space] * 2,
        scratch_shapes=[pltpu.VMEM(block, BF), pltpu.VMEM(block, BF)]
        + [pltpu.VMEM(cut, F32)] * (1 + extra)
        + swap_sems(lanes)
        + swap_sems(lanes),
        compiler_params=pltpu.CompilerParams(
            collective_id=call, has_side_effects=True, vmem_limit_bytes=32 << 20
        ),
        cost_estimate=pl.CostEstimate(
            flops=0, bytes_accessed=total * width * 16, transcendentals=0
        ),
        name="exchange",
    )(big, small)


def to_whole_rows(values, small, lanes):
    total, width = values.shape
    outs = ((total // lanes, lanes * width), (small.shape[0], lanes * width), width)
    return exchange(gather_rows_kernel, lanes, values, small, outs, 0, 9)


def to_width_blocks(rows, small, lanes):
    count, whole = rows.shape
    width = whole // lanes
    outs = ((count * lanes, width), (small.shape[0], width), width)
    return exchange(scatter_rows_kernel, lanes, rows, small, outs, 1, 10)


def spread_kernel(size, lanes, *refs):
    if lanes:
        own_ref, rows_ref, all_ref, there_ref, local_sem, send_sem, recv_sem, *rest = refs
        side_ref, *sems = rest
    else:
        own_ref, all_ref, local_sem, send_sem, recv_sem = refs
    me = lax.axis_index("gy")
    orders = bit_orders(size)
    half = own_ref.shape[0] // 2
    greet(me, orders[0], lanes)
    keep = pltpu.make_async_copy(own_ref, all_ref.at[me], local_sem)
    keep.start()
    copies = {}
    arrival = {}

    def copy(h, bit, r):
        n = len(copies)
        rows = pl.ds(h * half, half)
        where = flip_all(me, r)
        source = own_ref.at[rows] if r == 0 else all_ref.at[where, rows]
        made = pltpu.make_async_remote_copy(
            src_ref=source,
            dst_ref=all_ref.at[where, rows],
            send_sem=send_sem.at[n],
            recv_sem=recv_sem.at[n],
            device_id={"gy": flip(me, bit)},
            device_id_type=MESH,
        )
        copies[h, bit, r] = made
        arrival[h, r ^ bit] = made
        made.start()

    for step in range(len(orders[0])):
        for h in range(2):
            copy(h, orders[h][step], 0)
    swapped = []
    if lanes:
        cut_up(side_ref, rows_ref, 16)
        swapped = swap_start(lanes, side_ref, there_ref, sems)
    landed = set()

    def land(h, r):
        if (h, r) not in landed:
            landed.add((h, r))
            arrival[h, r].wait_recv()

    held = [[0], [0]]
    for step in range(len(orders[0])):
        for h in range(2):
            bit = orders[h][step]
            for r in held[h]:
                if r:
                    land(h, r)
                    copy(h, bit, r)
        for h in range(2):
            held[h] = held[h] + [r ^ orders[h][step] for r in held[h]]
    for h in range(2):
        for r in range(1, size):
            land(h, r)
    for made in copies.values():
        made.wait_send()
    for copy in [keep] + swapped:
        copy.wait()


def spread(values, side=None):
    size = lax.axis_size("gy")
    values = values.astype(BF)
    rows, width = values.shape
    count = 2 * (size - 1)
    sides = [] if side is None else [side]
    lanes = 0 if side is None else lax.axis_size("gx")
    blocks = (lanes, rows, width // max(lanes, 1))
    space = pl.BlockSpec(memory_space=pltpu.VMEM)
    out = pl.pallas_call(
        functools.partial(spread_kernel, size, lanes),
        out_shape=[jax.ShapeDtypeStruct((size, rows, width), values.dtype)]
        + [jax.ShapeDtypeStruct(blocks, BF) for v in sides],
        in_specs=[space] * (1 + len(sides)),
        out_specs=[pl.BlockSpec(memory_space=pltpu.HBM)] * (1 + len(sides)),
        scratch_shapes=[
            pltpu.SemaphoreType.DMA,
            pltpu.SemaphoreType.DMA((count,)),
            pltpu.SemaphoreType.DMA((count,)),
        ]
        + ([pltpu.VMEM(blocks, BF)] + swap_sems(lanes) if lanes else []),
        compiler_params=pltpu.CompilerParams(
            collective_id=4 if lanes else 0, has_side_effects=True, vmem_limit_bytes=32 << 20
        ),
        cost_estimate=pl.CostEstimate(
            flops=0, bytes_accessed=size * rows * width * 16, transcendentals=0
        ),
        name="spread",
    )(values, *sides)
    whole = out[0].reshape(size * rows, width)
    return (whole, out[1]) if lanes else whole


def settle_kernel(size, lanes, fused, *refs):
    if fused:
        left_ref, right_ref, *refs = refs
        *refs, picked, weights, product_ref, left_sem, right_sem = refs
        refs = [product_ref] + refs
    if lanes:
        parts_ref, side_ref, sum_ref, rows_ref, came, kept, send_sem, recv_sem, *rest = refs
        there_ref, *sems = rest
    else:
        parts_ref, sum_ref, came, kept, send_sem, recv_sem = refs
    me = lax.axis_index("gy")
    orders = tuple(order[::-1] for order in bit_orders(size)) * (PARTS // 2)
    half = sum_ref.shape[0] // PARTS
    strip = 16
    def left_copy(j):
        count = left_ref.shape[1]
        return pltpu.make_async_copy(
            left_ref.at[flip_all(me, turn[j])],
            picked.at[pl.ds(j * count, count)],
            left_sem.at[j],
        )

    def right_copy(i):
        rows = pl.ds(pl.multiple_of(i * TILE, TILE), TILE)
        return pltpu.make_async_copy(right_ref.at[rows], weights.at[rows], right_sem.at[i])

    def multiply(low, high):
        count = left_ref.shape[1]
        for j in range(low, high):
            left_copy(j).wait()

        @pl.loop(0, weights.shape[0] // TILE)
        def _(i):
            if low == 0:
                right_copy(i).wait()
            columns = pl.ds(pl.multiple_of(i * TILE, TILE), TILE)
            block = lax.dot_general(
                picked[low * count : high * count],
                weights[columns],
                (((1,), (1,)), ((), ())),
                preferred_element_type=F32,
            ).astype(BF)
            for j in range(low, high):
                parts_ref[flip_all(me, turn[j]), :, columns] = block[
                    (j - low) * count : (j - low + 1) * count
                ]

    turn = [r for r in range(size) if r & 1] + [r for r in range(size - 1, -1, -1) if not r & 1]
    if fused:
        for j in range(size // 2):
            left_copy(j).start()
        for i in range(weights.shape[0] // TILE):
            right_copy(i).start()
        for j in range(size // 2, size):
            left_copy(j).start()
    greet(me, orders[0], lanes)
    swapped = swap_start(lanes, side_ref, there_ref, sems) if lanes else []
    slot = {}
    for h in range(PARTS):
        held = list(range(size))
        for step, bit in enumerate(orders[h]):
            held = [r for r in held if not r & bit]
            for r in held:
                slot[h, step, r] = len(slot)
    copies = {}

    def view(h, step, r):
        if step == 0:
            return parts_ref.at[flip_all(me, r), pl.ds(h * half, half)]
        return kept.at[h, r]

    def send(h, step):
        bit = orders[h][step]
        gone = set()
        for b in orders[h][:step]:
            gone.add(b)
        for r in range(size):
            if r & bit and not any(r & b for b in gone):
                n = slot[h, step, r ^ bit]
                made = pltpu.make_async_remote_copy(
                    src_ref=view(h, step, r),
                    dst_ref=came.at[n],
                    send_sem=send_sem.at[n],
                    recv_sem=recv_sem.at[n],
                    device_id={"gy": flip(me, bit)},
                    device_id_type=MESH,
                )
                copies[h, step, r ^ bit] = made
                made.start()

    def gather(h, step, r, last):
        n = slot[h, step, r]
        copies[h, step, r].wait_recv()

        @pl.loop(0, half // strip)
        def _(i):
            rows = pl.ds(i * strip, strip)
            total = view(h, step, r)[rows].astype(F32) + came[n, rows].astype(F32)
            if last:
                sum_ref[pl.ds(h * half + i * strip, strip)] = total
            else:
                kept[h, r, rows] = total.astype(BF)

    steps = len(orders[0])
    if fused:
        multiply(0, size // 2)
    for h in range(PARTS):
        send(h, 0)
    if fused:
        multiply(size // 2, size - 1)
    for step in range(steps):
        if lanes and step == steps - 1:
            for copy in swapped:
                copy.wait()
            lay_out(rows_ref, there_ref, strip)
        for h in range(PARTS):
            bits = orders[h][: step + 1]
            later = orders[h][step + 1] if step + 1 < steps else 0
            left = [r for r in range(size) if not any(r & b for b in bits)]
            for r in left:
                if r & later:
                    gather(h, step, r, False)
            if later:
                send(h, step + 1)
            for r in left:
                if not r & later and not (fused and step == 0):
                    gather(h, step, r, step == steps - 1)
        if fused and step == 0:
            multiply(size - 1, size)
            for h in range(PARTS):
                for r in range(size):
                    if not r & orders[h][0] and not r & orders[h][1]:
                        gather(h, 0, r, False)
    for made in copies.values():
        made.wait_send()


def settle(parts, side=None, right=None):
    size = lax.axis_size("gy")
    parts = parts.astype(BF)
    total, inner = parts.shape
    width = inner if right is None else right.shape[0]
    rows = total // size
    count = PARTS * (size - 1)
    sides = [] if side is None else [side]
    rights = [] if right is None else [right]
    lanes = 0 if side is None else side.shape[0]
    space = pl.BlockSpec(memory_space=pltpu.VMEM)
    scratch = [
        pltpu.VMEM((count, rows // PARTS, width), BF),
        pltpu.VMEM((PARTS, size, rows // PARTS, width), BF),
        pltpu.SemaphoreType.DMA((count,)),
        pltpu.SemaphoreType.DMA((count,)),
    ]
    if lanes:
        scratch += [pltpu.VMEM(side.shape, side.dtype)] + swap_sems(lanes)
    if rights:
        scratch += [
            pltpu.VMEM((total, inner), BF),
            pltpu.VMEM((width, inner), BF),
            pltpu.VMEM((size, rows, width), BF),
            pltpu.SemaphoreType.DMA((size,)),
            pltpu.SemaphoreType.DMA((width // TILE,)),
        ]
    out = pl.pallas_call(
        functools.partial(settle_kernel, size, lanes, bool(rights)),
        out_shape=[jax.ShapeDtypeStruct((rows, width), F32)] * (1 + len(sides)),
        in_specs=[pl.BlockSpec(memory_space=pl.ANY)] * (2 * len(rights))
        + [space] * (1 - len(rights) + len(sides)),
        out_specs=[space] * (1 + len(sides)),
        scratch_shapes=scratch,
        compiler_params=pltpu.CompilerParams(
            collective_id=5 if lanes else 1, has_side_effects=True, vmem_limit_bytes=40 << 20
        ),
        cost_estimate=pl.CostEstimate(
            flops=0, bytes_accessed=total * width * 16, transcendentals=0
        ),
        name="settle",
    )
    operands = [parts.reshape(size, rows, inner)] + rights
    if rights:
        operands = [pltpu.with_memory_space_constraint(v, pltpu.HBM) for v in operands]
    out = out(*operands, *sides)
    return out if lanes else out[0]


def tally_kernel(size, own_ref, sum_ref, came, send_sem, recv_sem):
    me = lax.axis_index("gy")
    barrier = pltpu.get_barrier_semaphore()
    for d in range(1, size):
        pl.semaphore_signal(
            barrier, inc=1, device_id={"gy": (me + d) % size}, device_id_type=MESH
        )
    pl.semaphore_wait(barrier, size - 1)
    copies = []
    for d in range(1, size):
        made = pltpu.make_async_remote_copy(
            src_ref=own_ref,
            dst_ref=came.at[d],
            send_sem=send_sem.at[d],
            recv_sem=recv_sem.at[d],
            device_id={"gy": (me + d) % size},
            device_id_type=MESH,
        )
        made.start()
        copies.append(made)
    total = own_ref[...]
    for d in range(1, size):
        copies[d - 1].wait_recv()
        total = total + came[d]
    sum_ref[...] = total
    for made in copies:
        made.wait_send()


def tally(values, size):
    return pl.pallas_call(
        functools.partial(tally_kernel, size),
        out_shape=jax.ShapeDtypeStruct(values.shape, F32),
        in_specs=[pl.BlockSpec(memory_space=pltpu.VMEM)],
        out_specs=pl.BlockSpec(memory_space=pltpu.VMEM),
        scratch_shapes=[
            pltpu.VMEM((size,) + values.shape, F32),
            pltpu.SemaphoreType.DMA((size,)),
            pltpu.SemaphoreType.DMA((size,)),
        ],
        compiler_params=pltpu.CompilerParams(collective_id=2, has_side_effects=True),
        name="tally",
    )(values)


def make_shards(nx, ny):
    blocks = [((b // ny) * ny + b % ny, (b % nx) * ny + b // nx) for b in range(nx * ny)]

    def shards(
        inputs,
        segment_ids,
        qkv_weight,
        out_weight,
        gate_up_weight,
        down_weight,
        first_gain,
        second_gain,
        third_gain,
        fourth_gain,
        cotangent,
    ):
        width = inputs.shape[1]

        own = inputs.shape[0] // nx
        heads = qkv_weight.shape[1]
        qkv_w = lax.all_gather(qkv_weight, "gx", axis=0, tiled=True)
        gains = jnp.stack([first_gain, second_gain, third_gain, fourth_gain])
        gains, qkv_w = lax.optimization_barrier((gains, qkv_w))
        x_rows, gains = to_whole_rows(inputs, gains, nx)
        gains = gains[:, None, :]
        hid = gate_up_weight.shape[2]
        wide_w = lax.all_gather(
            jnp.concatenate([gate_up_weight.reshape(width, 2 * hid), out_weight.T], axis=1),
            "gx",
            axis=0,
            tiled=True,
        )
        gate_w, up_w, out_w = wide_w[:, :hid], wide_w[:, hid : 2 * hid], wide_w[:, 2 * hid :]
        down_w = lax.all_gather(down_weight.T, "gx", axis=0, tiled=True)

        segment_row = lax.ppermute(segment_ids[0], ("gx", "gy"), blocks)
        position, allowed = block_layout(segment_row)
        layout = (allowed,) + rope_tables(position)

        scale_one = inverse_rms(x_rows)
        unit_one = x_rows * scale_one
        normed_one = spread(unit_one * gains[0])
        rows = product("td,dc->tc", normed_one, qkv_w).astype(BF)
        rows = lax.all_to_all(rows, "gy", split_axis=0, concat_axis=1, tiled=True)
        mixing_rows, saved = attention_forward(rows, layout)
        mixed = lax.all_to_all(mixing_rows, "gy", split_axis=1, concat_axis=0, tiled=True)
        attn_branch = settle(product("tc,dc->td", mixed, out_w))
        scale_two = inverse_rms(attn_branch)
        unit_two = attn_branch * scale_two
        attn_term = unit_two * gains[1]
        middle = x_rows + attn_term
        scale_three = inverse_rms(middle)
        unit_three = middle * scale_three
        normed_two = spread(unit_three * gains[2])
        pre_gate = product("td,df->tf", normed_two, gate_w)
        up_part = product("td,df->tf", normed_two, up_w)
        value, slope = gelu_parts(pre_gate)
        hidden = (value * up_part).astype(BF)
        ff_branch, cot_rows = settle(
            hidden, cotangent.astype(BF).reshape(nx, own, width), down_w
        )
        scale_four = inverse_rms(ff_branch)
        unit_four = ff_branch * scale_four
        ff_grad, delta = spread(
            norm_back(cot_rows, unit_four, scale_four, gains[3]),
            attn_term + unit_four * gains[3],
        )
        outputs = inputs + delta.reshape(inputs.shape).astype(F32)

        down_sum = product("td,tf->df", ff_grad, hidden).astype(BF)
        down_sum, ff_grad = lax.optimization_barrier((down_sum, ff_grad))
        down_done = lax.psum_scatter(down_sum, "gx", scatter_dimension=0, tiled=True)
        hidden_grad = product("td,df->tf", ff_grad, down_w)
        gate_grad = (hidden_grad * up_part * slope).astype(BF)
        up_grad = (hidden_grad * value).astype(BF)
        gate_up_sum = jnp.stack(
            [
                product("td,tf->df", normed_two, gate_grad).astype(BF),
                product("td,tf->df", normed_two, up_grad).astype(BF),
            ],
            axis=1,
        )
        gate_up_sum, gate_grad, up_grad = lax.optimization_barrier(
            (gate_up_sum, gate_grad, up_grad)
        )
        gate_up_done = lax.psum_scatter(gate_up_sum, "gx", scatter_dimension=0, tiled=True)
        normed_two_grad = settle(
            product("tf,df->td", gate_grad, gate_w)
            + product("tf,df->td", up_grad, up_w)
        )
        middle_delta = norm_back(normed_two_grad, unit_three, scale_three, gains[2])
        middle_grad = cot_rows + middle_delta
        branch_grad = spread(norm_back(middle_grad, unit_two, scale_two, gains[1]))
        out_sum = product("td,tc->dc", branch_grad, mixed).astype(BF)
        mixing_gradient = product("td,dc->tc", branch_grad, out_w).astype(BF)
        mixing_gradient = lax.all_to_all(
            mixing_gradient, "gy", split_axis=0, concat_axis=1, tiled=True
        )
        qkv_grad_rows = attention_backward(mixing_gradient, mixing_rows, saved, layout)
        qkv_grad_rows, down_done = lax.optimization_barrier((qkv_grad_rows, down_done))
        qkv_grad_rows = lax.all_to_all(
            qkv_grad_rows, "gy", split_axis=1, concat_axis=0, tiled=True
        )
        normed_one_grad = settle(product("tc,dc->td", qkv_grad_rows, qkv_w))
        both_sum = jnp.concatenate(
            [product("td,tc->dc", normed_one, qkv_grad_rows).astype(BF), out_sum], axis=1
        )
        terms = jnp.stack(
            [
                jnp.sum(normed_one_grad * unit_one, axis=0),
                jnp.sum(middle_grad * unit_two, axis=0),
                jnp.sum(normed_two_grad * unit_three, axis=0),
                jnp.sum(cot_rows * unit_four, axis=0),
            ]
        )
        delta, terms = to_width_blocks(
            middle_delta + norm_back(normed_one_grad, unit_one, scale_one, gains[0]),
            tally(terms, ny),
            nx,
        )
        down_grad = down_done.astype(F32).T
        both_sum = with_layout_constraint(both_sum, Layout((0, 1)))
        gate_up_done, both_sum, delta, down_grad = lax.optimization_barrier(
            (gate_up_done, both_sum, delta, down_grad)
        )
        both_done = lax.psum_scatter(both_sum, "gx", scatter_dimension=0, tiled=True)
        gate_up_grad = gate_up_done.astype(F32)
        input_grad = cotangent + delta
        qkv_grad = both_done[:, :heads].astype(F32)
        out_grad = both_done[:, heads:].astype(F32).T
        return (outputs, input_grad, qkv_grad, out_grad, gate_up_grad, down_grad) + tuple(
            terms[i] for i in range(4)
        )

    return shards


def solution(mesh):
    placed = (
        P("gy", "gx"),
        P(("gx", "gy"), None),
        P("gx", "gy"),
        P("gy", "gx"),
        P("gx", None, "gy"),
        P("gy", "gx"),
        P("gx"),
        P("gx"),
        P("gx"),
        P("gx"),
        P("gy", "gx"),
    )
    return jax.shard_map(
        make_shards(mesh.shape["gx"], mesh.shape["gy"]),
        mesh=mesh,
        in_specs=placed,
        out_specs=(
            P("gy", "gx"),
            P("gy", "gx"),
            P("gx", "gy"),
            P("gy", "gx"),
            P("gx", None, "gy"),
            P("gy", "gx"),
            P("gx"),
            P("gx"),
            P("gx"),
            P("gx"),
        ),
        check_vma=False,
    )
```

```python
import functools
import math

import jax
import jax.numpy as jnp
from jax import lax
from jax.experimental import pallas as pl
from jax.experimental.layout import Layout, with_layout_constraint
from jax.experimental.pallas import tpu as pltpu
from jax.sharding import PartitionSpec as P

QUERY_HEADS = 8
KEY_VALUE_HEADS = 4
HEAD_SIZE = 256


EPSILON = 1e-06
SOFT_CAP = 50.0
GELU_COEF = 0.7978845608028654
CUBIC_COEF = 0.044715

BF = jnp.bfloat16
F32 = jnp.float32
MESH = pl.DeviceIdType.MESH
PARTS = 4
TILE = 768


def product(form, left, right):
    return jnp.einsum(form, left, right, preferred_element_type=F32)


def gelu_parts(pre_gate):
    inner_arg = GELU_COEF * (pre_gate + CUBIC_COEF * pre_gate * pre_gate * pre_gate)
    tanh_value = jnp.tanh(inner_arg)
    activated = 0.5 * pre_gate * (1.0 + tanh_value)
    derivative = 0.5 * (1.0 + tanh_value) + 0.5 * pre_gate * (
        1.0 - tanh_value * tanh_value
    ) * GELU_COEF * (1.0 + 3.0 * CUBIC_COEF * pre_gate * pre_gate)
    return (activated, derivative)


def block_layout(segment_row):
    length_total = segment_row.shape[0]
    places = jnp.arange(length_total, dtype=jnp.int32)
    same_doc = segment_row[:, None] == segment_row[None, :]
    starts = jnp.min(jnp.where(same_doc, places[None, :], length_total), axis=1)
    allowed = jnp.logical_and(same_doc, places[None, :] <= places[:, None])
    return (places - starts, allowed)


def rope_tables(position):
    half_dim = HEAD_SIZE // 2
    freq_steps = jnp.arange(half_dim, dtype=F32)
    frequency = jnp.exp(freq_steps * (-2.0 * math.log(10000.0) / HEAD_SIZE))
    angles = position.astype(F32)[:, None] * frequency[None, :]
    return (jnp.cos(angles)[:, None, :], jnp.sin(angles)[:, None, :])


def rotate(values, cos_table, sin_table, direction):
    half_dim = values.shape[-1] // 2
    leading = values[..., :half_dim]
    trailing = values[..., half_dim:]
    return jnp.concatenate(
        [
            leading * cos_table - direction * trailing * sin_table,
            trailing * cos_table + direction * leading * sin_table,
        ],
        axis=-1,
    )


def capped_scores(rotated_query, k_rot):
    token_rows = rotated_query.shape[0]
    query_groups = rotated_query.reshape(
        token_rows, KEY_VALUE_HEADS, QUERY_HEADS // KEY_VALUE_HEADS, HEAD_SIZE
    )
    raw_scores = product("tkgd,skd->kgts", query_groups, k_rot) * HEAD_SIZE ** (-0.5)
    return SOFT_CAP * jnp.tanh(raw_scores / SOFT_CAP)


def attention_forward(rows, layout):
    token_rows = rows.shape[0]
    query_span_width = QUERY_HEADS * HEAD_SIZE
    key_value_width = KEY_VALUE_HEADS * HEAD_SIZE
    allowed, cos_table, sin_table = layout
    query_part = (
        rows[:, :query_span_width].astype(F32).reshape(token_rows, QUERY_HEADS, HEAD_SIZE)
    )
    key_slice = (
        rows[:, query_span_width : query_span_width + key_value_width]
        .astype(F32)
        .reshape(token_rows, KEY_VALUE_HEADS, HEAD_SIZE)
    )
    value_slice = rows[:, query_span_width + key_value_width :].reshape(
        token_rows, KEY_VALUE_HEADS, HEAD_SIZE
    )
    rotated_query = rotate(query_part, cos_table, sin_table, 1.0).astype(BF)
    k_rot = rotate(key_slice, cos_table, sin_table, 1.0).astype(BF)
    capped = capped_scores(rotated_query, k_rot)
    log_total = jnp.log(jnp.sum(jnp.where(allowed, jnp.exp(capped), 0.0), axis=-1))
    weights_f = jnp.where(allowed, jnp.exp(capped - log_total[..., None]), 0.0)
    mixing_rows = product("kgts,skd->tkgd", weights_f.astype(BF), value_slice)
    mixing_rows = mixing_rows.astype(BF).reshape(token_rows, query_span_width)
    return (mixing_rows, (rotated_query, k_rot, value_slice, log_total))


def attention_backward(mixing_gradient, mixing_rows, saved, layout):
    rotated_query, k_rot, value_slice, log_total = saved
    token_rows = mixing_gradient.shape[0]
    heads_per_group = QUERY_HEADS // KEY_VALUE_HEADS
    allowed, cos_table, sin_table = layout
    capped = capped_scores(rotated_query, k_rot)
    weights_f = jnp.where(allowed, jnp.exp(capped - log_total[..., None]), 0.0)
    gradient_by_group = mixing_gradient.reshape(
        token_rows, KEY_VALUE_HEADS, heads_per_group, HEAD_SIZE
    )
    output_by_group = mixing_rows.reshape(token_rows, KEY_VALUE_HEADS, heads_per_group, HEAD_SIZE)
    row_delta = product("tkgd,tkgd->kgt", gradient_by_group, output_by_group)
    value_gradient = product("maew,emaq->wmq", weights_f.astype(BF), gradient_by_group)
    weight_grad = product("tkgd,skd->kgts", gradient_by_group, value_slice)
    score_gradient = (
        weights_f
        * (weight_grad - row_delta[..., None])
        * (1.0 - (capped / SOFT_CAP) ** 2)
        * HEAD_SIZE ** (-0.5)
    )
    score_gradient = score_gradient.astype(BF)
    query_gradient = product("kgts,skd->tkgd", score_gradient, k_rot).reshape(
        token_rows, QUERY_HEADS, HEAD_SIZE
    )
    key_gradient = product(
        "maew,emaq->wmq",
        score_gradient,
        rotated_query.reshape(token_rows, KEY_VALUE_HEADS, heads_per_group, HEAD_SIZE),
    )
    query_gradient = rotate(query_gradient, cos_table, sin_table, -1.0)
    key_gradient = rotate(key_gradient, cos_table, sin_table, -1.0)
    return jnp.concatenate(
        [
            query_gradient.reshape(token_rows, QUERY_HEADS * HEAD_SIZE),
            key_gradient.reshape(token_rows, KEY_VALUE_HEADS * HEAD_SIZE),
            value_gradient.reshape(token_rows, KEY_VALUE_HEADS * HEAD_SIZE),
        ],
        axis=1,
    ).astype(BF)


def inverse_rms(values):
    return lax.rsqrt(jnp.mean(values * values, axis=1, keepdims=True) + EPSILON)


def norm_back(grad_rows, unit_rows, scale_rows, gain):
    scaled = grad_rows * gain
    return scale_rows * (scaled - unit_rows * jnp.mean(scaled * unit_rows, axis=1, keepdims=True))


def flip(index, mask):
    return index + mask - 2 * mask * ((index // mask) % 2)


def flip_all(index, masks):
    bit = 1
    while bit <= masks:
        if masks & bit:
            index = flip(index, bit)
        bit *= 2
    return index


def greet(me, bits, lanes=0):
    barrier = pltpu.get_barrier_semaphore()
    for bit in bits:
        pl.semaphore_signal(barrier, inc=1, device_id={"gy": flip(me, bit)}, device_id_type=MESH)
    for d in range(1, lanes):
        other = (lax.axis_index("gx") + d) % lanes
        pl.semaphore_signal(barrier, inc=1, device_id={"gx": other}, device_id_type=MESH)
    pl.semaphore_wait(barrier, len(bits) + max(lanes - 1, 0))


def bit_orders(size):
    bits = []
    bit = 2
    while bit < size:
        bits.append(bit)
        bit *= 2
    return (bits + [1], bits[::-1] + [1])


def lay_out(rows_ref, blocks_ref, strip):
    lanes, count, width = blocks_ref.shape

    @pl.loop(0, count // strip)
    def _(i):
        rows = pl.ds(i * strip, strip)
        for k in range(lanes):
            rows_ref[rows, k * width : (k + 1) * width] = blocks_ref[k, rows].astype(F32)


def cut_up(blocks_ref, rows_ref, strip):
    lanes, count, width = blocks_ref.shape

    @pl.loop(0, count // strip)
    def _(i):
        rows = pl.ds(i * strip, strip)
        for k in range(lanes):
            blocks_ref[k, rows] = rows_ref[rows, k * width : (k + 1) * width].astype(BF)


def swap_start(lanes, side_ref, there_ref, sems):
    me = lax.axis_index("gx")
    own, send_sem, recv_sem = sems
    made = [pltpu.make_async_copy(side_ref.at[me], there_ref.at[me], own)]
    for d in range(1, lanes):
        other = (me + d) % lanes
        made.append(
            pltpu.make_async_remote_copy(
                src_ref=side_ref.at[other],
                dst_ref=there_ref.at[me],
                send_sem=send_sem.at[d],
                recv_sem=recv_sem.at[d],
                device_id={"gx": other},
                device_id_type=MESH,
            )
        )
    for copy in made:
        copy.start()
    return made


def swap_sems(lanes):
    return [
        pltpu.SemaphoreType.DMA,
        pltpu.SemaphoreType.DMA((lanes,)),
        pltpu.SemaphoreType.DMA((lanes,)),
    ]


def greet_lanes(lanes):
    barrier = pltpu.get_barrier_semaphore()
    for d in range(1, lanes):
        other = (lax.axis_index("gx") + d) % lanes
        pl.semaphore_signal(barrier, inc=1, device_id={"gx": other}, device_id_type=MESH)
    pl.semaphore_wait(barrier, lanes - 1)


def gather_rows_kernel(lanes, native_ref, small_ref, rows_ref, wide_ref, *scratch):
    send_ref, there_ref, small_all, *sems = scratch
    big_sems, small_sems = sems[:3], sems[3:]
    fold, pair = send_ref.shape[1:]
    width = pair // 2
    strip = 16
    for j in range(lanes):
        for side in range(2):

            @pl.loop(0, fold // strip)
            def _(i):
                rows = pl.ds((2 * j + side) * fold + i * strip, strip)
                send_ref[j, pl.ds(i * strip, strip), side * width : (side + 1) * width] = (
                    native_ref[rows].astype(BF)
                )

    greet_lanes(lanes)
    copies = swap_start(lanes, send_ref, there_ref, big_sems)
    copies += hand_round(lanes, small_ref, small_all, small_sems)
    for copy in copies:
        copy.wait()
    for k in range(lanes):
        columns = slice(k * width, (k + 1) * width)
        wide_ref[:, columns] = small_all[k]
        for side in range(2):

            @pl.loop(0, fold // strip)
            def _(i):
                rows_ref[pl.ds(side * fold + i * strip, strip), columns] = there_ref[
                    k, pl.ds(i * strip, strip), side * width : (side + 1) * width
                ].astype(F32)


def scatter_rows_kernel(lanes, rows_ref, wide_ref, native_ref, small_ref, *scratch):
    send_ref, there_ref, small_send, small_all, *sems = scratch
    big_sems, small_sems = sems[:3], sems[3:]
    fold, pair = send_ref.shape[1:]
    width = pair // 2
    strip = 16
    for j in range(lanes):
        columns = slice(j * width, (j + 1) * width)
        small_send[j] = wide_ref[:, columns]
        for side in range(2):

            @pl.loop(0, fold // strip)
            def _(i):
                send_ref[j, pl.ds(i * strip, strip), side * width : (side + 1) * width] = rows_ref[
                    pl.ds(side * fold + i * strip, strip), columns
                ].astype(BF)

    greet_lanes(lanes)
    copies = swap_start(lanes, send_ref, there_ref, big_sems)
    copies += swap_start(lanes, small_send, small_all, small_sems)
    for copy in copies:
        copy.wait()
    total = small_all[0]
    for k in range(1, lanes):
        total = total + small_all[k]
    small_ref[...] = total
    for k in range(lanes):
        for side in range(2):

            @pl.loop(0, fold // strip)
            def _(i):
                rows = pl.ds((2 * k + side) * fold + i * strip, strip)
                native_ref[rows] = there_ref[
                    k, pl.ds(i * strip, strip), side * width : (side + 1) * width
                ].astype(F32)


def hand_round(lanes, own_ref, all_ref, sems):
    me = lax.axis_index("gx")
    own, send_sem, recv_sem = sems
    made = [pltpu.make_async_copy(own_ref, all_ref.at[me], own)]
    for d in range(1, lanes):
        made.append(
            pltpu.make_async_remote_copy(
                src_ref=own_ref,
                dst_ref=all_ref.at[me],
                send_sem=send_sem.at[d],
                recv_sem=recv_sem.at[d],
                device_id={"gx": (me + d) % lanes},
                device_id_type=MESH,
            )
        )
    for copy in made:
        copy.start()
    return made


def exchange(kernel, lanes, big, small, outs, extra, call):
    total, width = big.shape
    space = pl.BlockSpec(memory_space=pltpu.VMEM)
    count = total * width // (lanes * outs[2])
    block = (lanes, count // 2, 2 * outs[2])
    cut = (lanes, small.shape[0], outs[2])
    return pl.pallas_call(
        functools.partial(kernel, lanes),
        out_shape=[jax.ShapeDtypeStruct(v, F32) for v in outs[:2]],
        in_specs=[space] * 2,
        out_specs=[space] * 2,
        scratch_shapes=[pltpu.VMEM(block, BF), pltpu.VMEM(block, BF)]
        + [pltpu.VMEM(cut, F32)] * (1 + extra)
        + swap_sems(lanes)
        + swap_sems(lanes),
        compiler_params=pltpu.CompilerParams(
            collective_id=call, has_side_effects=True, vmem_limit_bytes=32 << 20
        ),
        cost_estimate=pl.CostEstimate(
            flops=0, bytes_accessed=total * width * 16, transcendentals=0
        ),
        name="exchange",
    )(big, small)


def to_whole_rows(values, small, lanes):
    total, width = values.shape
    outs = ((total // lanes, lanes * width), (small.shape[0], lanes * width), width)
    return exchange(gather_rows_kernel, lanes, values, small, outs, 0, 9)


def to_width_blocks(rows, small, lanes):
    count, whole = rows.shape
    width = whole // lanes
    outs = ((count * lanes, width), (small.shape[0], width), width)
    return exchange(scatter_rows_kernel, lanes, rows, small, outs, 1, 10)


def spread_kernel(size, lanes, *refs):
    if lanes:
        own_ref, rows_ref, all_ref, there_ref, local_sem, send_sem, recv_sem, *rest = refs
        side_ref, *sems = rest
    else:
        own_ref, all_ref, local_sem, send_sem, recv_sem = refs
    me = lax.axis_index("gy")
    orders = bit_orders(size) * (PARTS // 2)
    half = own_ref.shape[0] // PARTS
    greet(me, orders[0], lanes)
    keep = pltpu.make_async_copy(own_ref, all_ref.at[me], local_sem)
    keep.start()
    copies = {}
    arrival = {}

    def copy(h, bit, r):
        n = len(copies)
        rows = pl.ds(h * half, half)
        where = flip_all(me, r)
        source = own_ref.at[rows] if r == 0 else all_ref.at[where, rows]
        made = pltpu.make_async_remote_copy(
            src_ref=source,
            dst_ref=all_ref.at[where, rows],
            send_sem=send_sem.at[n],
            recv_sem=recv_sem.at[n],
            device_id={"gy": flip(me, bit)},
            device_id_type=MESH,
        )
        copies[h, bit, r] = made
        arrival[h, r ^ bit] = made
        made.start()

    for step in range(len(orders[0])):
        for h in range(PARTS):
            copy(h, orders[h][step], 0)
    swapped = []
    if lanes:
        cut_up(side_ref, rows_ref, 16)
        swapped = swap_start(lanes, side_ref, there_ref, sems)
    landed = set()

    def land(h, r):
        if (h, r) not in landed:
            landed.add((h, r))
            arrival[h, r].wait_recv()

    held = [[0] for h in range(PARTS)]
    for step in range(len(orders[0])):
        for h in range(PARTS):
            bit = orders[h][step]
            for r in held[h]:
                if r:
                    land(h, r)
                    copy(h, bit, r)
        for h in range(PARTS):
            held[h] = held[h] + [r ^ orders[h][step] for r in held[h]]
    for h in range(PARTS):
        for r in range(1, size):
            land(h, r)
    for made in copies.values():
        made.wait_send()
    for copy in [keep] + swapped:
        copy.wait()


def spread(values, side=None):
    size = lax.axis_size("gy")
    values = values.astype(BF)
    rows, width = values.shape
    count = PARTS * (size - 1)
    sides = [] if side is None else [side]
    lanes = 0 if side is None else lax.axis_size("gx")
    blocks = (lanes, rows, width // max(lanes, 1))
    space = pl.BlockSpec(memory_space=pltpu.VMEM)
    out = pl.pallas_call(
        functools.partial(spread_kernel, size, lanes),
        out_shape=[jax.ShapeDtypeStruct((size, rows, width), values.dtype)]
        + [jax.ShapeDtypeStruct(blocks, BF) for v in sides],
        in_specs=[space] * (1 + len(sides)),
        out_specs=[pl.BlockSpec(memory_space=pltpu.HBM)] * (1 + len(sides)),
        scratch_shapes=[
            pltpu.SemaphoreType.DMA,
            pltpu.SemaphoreType.DMA((count,)),
            pltpu.SemaphoreType.DMA((count,)),
        ]
        + ([pltpu.VMEM(blocks, BF)] + swap_sems(lanes) if lanes else []),
        compiler_params=pltpu.CompilerParams(
            collective_id=4 if lanes else 0, has_side_effects=True, vmem_limit_bytes=32 << 20
        ),
        cost_estimate=pl.CostEstimate(
            flops=0, bytes_accessed=size * rows * width * 16, transcendentals=0
        ),
        name="spread",
    )(values, *sides)
    whole = out[0].reshape(size * rows, width)
    return (whole, out[1]) if lanes else whole


def settle_kernel(size, lanes, fused, *refs):
    if fused:
        left_ref, right_ref, *refs = refs
        *refs, picked, weights, product_ref, left_sem, right_sem = refs
        refs = [product_ref] + refs
    if lanes:
        parts_ref, side_ref, sum_ref, rows_ref, came, kept, send_sem, recv_sem, *rest = refs
        there_ref, *sems = rest
    else:
        parts_ref, sum_ref, came, kept, send_sem, recv_sem = refs
    me = lax.axis_index("gy")
    orders = tuple(order[::-1] for order in bit_orders(size)) * (PARTS // 2)
    half = sum_ref.shape[0] // PARTS
    strip = 16
    def left_copy(j):
        count = left_ref.shape[1]
        return pltpu.make_async_copy(
            left_ref.at[flip_all(me, turn[j])],
            picked.at[pl.ds(j * count, count)],
            left_sem.at[j],
        )

    def right_copy(i):
        rows = pl.ds(pl.multiple_of(i * TILE, TILE), TILE)
        return pltpu.make_async_copy(right_ref.at[rows], weights.at[rows], right_sem.at[i])

    def multiply(low, high):
        count = left_ref.shape[1]
        for j in range(low, high):
            left_copy(j).wait()

        @pl.loop(0, weights.shape[0] // TILE)
        def _(i):
            if low == 0:
                right_copy(i).wait()
            columns = pl.ds(pl.multiple_of(i * TILE, TILE), TILE)
            block = lax.dot_general(
                picked[low * count : high * count],
                weights[columns],
                (((1,), (1,)), ((), ())),
                preferred_element_type=F32,
            ).astype(BF)
            for j in range(low, high):
                parts_ref[flip_all(me, turn[j]), :, columns] = block[
                    (j - low) * count : (j - low + 1) * count
                ]

    turn = [r for r in range(size) if r & 1] + [r for r in range(size - 1, -1, -1) if not r & 1]
    if fused:
        for j in range(size // 2):
            left_copy(j).start()
        for i in range(weights.shape[0] // TILE):
            right_copy(i).start()
        for j in range(size // 2, size):
            left_copy(j).start()
    greet(me, orders[0], lanes)
    swapped = swap_start(lanes, side_ref, there_ref, sems) if lanes else []
    slot = {}
    for h in range(PARTS):
        held = list(range(size))
        for step, bit in enumerate(orders[h]):
            held = [r for r in held if not r & bit]
            for r in held:
                slot[h, step, r] = len(slot)
    copies = {}

    def view(h, step, r):
        if step == 0:
            return parts_ref.at[flip_all(me, r), pl.ds(h * half, half)]
        return kept.at[h, r]

    def send(h, step):
        bit = orders[h][step]
        gone = set()
        for b in orders[h][:step]:
            gone.add(b)
        for r in range(size):
            if r & bit and not any(r & b for b in gone):
                n = slot[h, step, r ^ bit]
                made = pltpu.make_async_remote_copy(
                    src_ref=view(h, step, r),
                    dst_ref=came.at[n],
                    send_sem=send_sem.at[n],
                    recv_sem=recv_sem.at[n],
                    device_id={"gy": flip(me, bit)},
                    device_id_type=MESH,
                )
                copies[h, step, r ^ bit] = made
                made.start()

    def gather(h, step, r, last):
        n = slot[h, step, r]
        copies[h, step, r].wait_recv()

        @pl.loop(0, half // strip)
        def _(i):
            rows = pl.ds(i * strip, strip)
            total = view(h, step, r)[rows].astype(F32) + came[n, rows].astype(F32)
            if last:
                sum_ref[pl.ds(h * half + i * strip, strip)] = total
            else:
                kept[h, r, rows] = total.astype(BF)

    steps = len(orders[0])
    if fused:
        multiply(0, size // 2)
    for h in range(PARTS):
        send(h, 0)
    if fused:
        multiply(size // 2, size - 1)
    for step in range(steps):
        if lanes and step == steps - 1:
            for copy in swapped:
                copy.wait()
            lay_out(rows_ref, there_ref, strip)
        for h in range(PARTS):
            bits = orders[h][: step + 1]
            later = orders[h][step + 1] if step + 1 < steps else 0
            left = [r for r in range(size) if not any(r & b for b in bits)]
            for r in left:
                if r & later:
                    gather(h, step, r, False)
            if later:
                send(h, step + 1)
            for r in left:
                if not r & later and not (fused and step == 0):
                    gather(h, step, r, step == steps - 1)
        if fused and step == 0:
            multiply(size - 1, size)
            for h in range(PARTS):
                for r in range(size):
                    if not r & orders[h][0] and not r & orders[h][1]:
                        gather(h, 0, r, False)
    for made in copies.values():
        made.wait_send()


def settle(parts, side=None, right=None):
    size = lax.axis_size("gy")
    parts = parts.astype(BF)
    total, inner = parts.shape
    width = inner if right is None else right.shape[0]
    rows = total // size
    count = PARTS * (size - 1)
    sides = [] if side is None else [side]
    rights = [] if right is None else [right]
    lanes = 0 if side is None else side.shape[0]
    space = pl.BlockSpec(memory_space=pltpu.VMEM)
    scratch = [
        pltpu.VMEM((count, rows // PARTS, width), BF),
        pltpu.VMEM((PARTS, size, rows // PARTS, width), BF),
        pltpu.SemaphoreType.DMA((count,)),
        pltpu.SemaphoreType.DMA((count,)),
    ]
    if lanes:
        scratch += [pltpu.VMEM(side.shape, side.dtype)] + swap_sems(lanes)
    if rights:
        scratch += [
            pltpu.VMEM((total, inner), BF),
            pltpu.VMEM((width, inner), BF),
            pltpu.VMEM((size, rows, width), BF),
            pltpu.SemaphoreType.DMA((size,)),
            pltpu.SemaphoreType.DMA((width // TILE,)),
        ]
    out = pl.pallas_call(
        functools.partial(settle_kernel, size, lanes, bool(rights)),
        out_shape=[jax.ShapeDtypeStruct((rows, width), F32)] * (1 + len(sides)),
        in_specs=[pl.BlockSpec(memory_space=pl.ANY)] * (2 * len(rights))
        + [space] * (1 - len(rights) + len(sides)),
        out_specs=[space] * (1 + len(sides)),
        scratch_shapes=scratch,
        compiler_params=pltpu.CompilerParams(
            collective_id=5 if lanes else 1, has_side_effects=True, vmem_limit_bytes=40 << 20
        ),
        cost_estimate=pl.CostEstimate(
            flops=0, bytes_accessed=total * width * 16, transcendentals=0
        ),
        name="settle",
    )
    operands = [parts.reshape(size, rows, inner)] + rights
    if rights:
        operands = [pltpu.with_memory_space_constraint(v, pltpu.HBM) for v in operands]
    out = out(*operands, *sides)
    return out if lanes else out[0]


def tally_kernel(size, own_ref, sum_ref, came, send_sem, recv_sem):
    me = lax.axis_index("gy")
    barrier = pltpu.get_barrier_semaphore()
    for d in range(1, size):
        pl.semaphore_signal(
            barrier, inc=1, device_id={"gy": (me + d) % size}, device_id_type=MESH
        )
    pl.semaphore_wait(barrier, size - 1)
    copies = []
    for d in range(1, size):
        made = pltpu.make_async_remote_copy(
            src_ref=own_ref,
            dst_ref=came.at[d],
            send_sem=send_sem.at[d],
            recv_sem=recv_sem.at[d],
            device_id={"gy": (me + d) % size},
            device_id_type=MESH,
        )
        made.start()
        copies.append(made)
    total = own_ref[...]
    for d in range(1, size):
        copies[d - 1].wait_recv()
        total = total + came[d]
    sum_ref[...] = total
    for made in copies:
        made.wait_send()


def tally(values, size):
    return pl.pallas_call(
        functools.partial(tally_kernel, size),
        out_shape=jax.ShapeDtypeStruct(values.shape, F32),
        in_specs=[pl.BlockSpec(memory_space=pltpu.VMEM)],
        out_specs=pl.BlockSpec(memory_space=pltpu.VMEM),
        scratch_shapes=[
            pltpu.VMEM((size,) + values.shape, F32),
            pltpu.SemaphoreType.DMA((size,)),
            pltpu.SemaphoreType.DMA((size,)),
        ],
        compiler_params=pltpu.CompilerParams(collective_id=2, has_side_effects=True),
        name="tally",
    )(values)


def make_shards(nx, ny):
    blocks = [((b // ny) * ny + b % ny, (b % nx) * ny + b // nx) for b in range(nx * ny)]

    def shards(
        inputs,
        segment_ids,
        qkv_weight,
        out_weight,
        gate_up_weight,
        down_weight,
        first_gain,
        second_gain,
        third_gain,
        fourth_gain,
        cotangent,
    ):
        width = inputs.shape[1]

        own = inputs.shape[0] // nx
        heads = qkv_weight.shape[1]
        qkv_w = lax.all_gather(qkv_weight, "gx", axis=0, tiled=True)
        gains = jnp.stack([first_gain, second_gain, third_gain, fourth_gain])
        gains, qkv_w = lax.optimization_barrier((gains, qkv_w))
        x_rows, gains = to_whole_rows(inputs, gains, nx)
        gains = gains[:, None, :]
        hid = gate_up_weight.shape[2]
        wide_w = lax.all_gather(
            jnp.concatenate([gate_up_weight.reshape(width, 2 * hid), out_weight.T], axis=1),
            "gx",
            axis=0,
            tiled=True,
        )
        gate_w, up_w, out_w = wide_w[:, :hid], wide_w[:, hid : 2 * hid], wide_w[:, 2 * hid :]
        down_w = lax.all_gather(down_weight.T, "gx", axis=0, tiled=True)

        segment_row = lax.ppermute(segment_ids[0], ("gx", "gy"), blocks)
        position, allowed = block_layout(segment_row)
        layout = (allowed,) + rope_tables(position)

        scale_one = inverse_rms(x_rows)
        unit_one = x_rows * scale_one
        normed_one = spread(unit_one * gains[0])
        rows = product("td,dc->tc", normed_one, qkv_w).astype(BF)
        rows = lax.all_to_all(rows, "gy", split_axis=0, concat_axis=1, tiled=True)
        mixing_rows, saved = attention_forward(rows, layout)
        mixed = lax.all_to_all(mixing_rows, "gy", split_axis=1, concat_axis=0, tiled=True)
        attn_branch = settle(product("tc,dc->td", mixed, out_w))
        scale_two = inverse_rms(attn_branch)
        unit_two = attn_branch * scale_two
        attn_term = unit_two * gains[1]
        middle = x_rows + attn_term
        scale_three = inverse_rms(middle)
        unit_three = middle * scale_three
        normed_two = spread(unit_three * gains[2])
        pre_gate = product("td,df->tf", normed_two, gate_w)
        up_part = product("td,df->tf", normed_two, up_w)
        value, slope = gelu_parts(pre_gate)
        hidden = (value * up_part).astype(BF)
        ff_branch, cot_rows = settle(
            hidden, cotangent.astype(BF).reshape(nx, own, width), down_w
        )
        scale_four = inverse_rms(ff_branch)
        unit_four = ff_branch * scale_four
        ff_grad, delta = spread(
            norm_back(cot_rows, unit_four, scale_four, gains[3]),
            attn_term + unit_four * gains[3],
        )
        outputs = inputs + delta.reshape(inputs.shape).astype(F32)

        down_sum = product("td,tf->df", ff_grad, hidden).astype(BF)
        down_sum, ff_grad = lax.optimization_barrier((down_sum, ff_grad))
        down_done = lax.psum_scatter(down_sum, "gx", scatter_dimension=0, tiled=True)
        hidden_grad = product("td,df->tf", ff_grad, down_w)
        gate_grad = (hidden_grad * up_part * slope).astype(BF)
        up_grad = (hidden_grad * value).astype(BF)
        gate_up_sum = jnp.stack(
            [
                product("td,tf->df", normed_two, gate_grad).astype(BF),
                product("td,tf->df", normed_two, up_grad).astype(BF),
            ],
            axis=1,
        )
        gate_up_sum, gate_grad, up_grad = lax.optimization_barrier(
            (gate_up_sum, gate_grad, up_grad)
        )
        gate_up_done = lax.psum_scatter(gate_up_sum, "gx", scatter_dimension=0, tiled=True)
        normed_two_grad = settle(
            product("tf,df->td", gate_grad, gate_w)
            + product("tf,df->td", up_grad, up_w)
        )
        middle_delta = norm_back(normed_two_grad, unit_three, scale_three, gains[2])
        middle_grad = cot_rows + middle_delta
        branch_grad = spread(norm_back(middle_grad, unit_two, scale_two, gains[1]))
        out_sum = product("td,tc->dc", branch_grad, mixed).astype(BF)
        mixing_gradient = product("td,dc->tc", branch_grad, out_w).astype(BF)
        mixing_gradient = lax.all_to_all(
            mixing_gradient, "gy", split_axis=0, concat_axis=1, tiled=True
        )
        qkv_grad_rows = attention_backward(mixing_gradient, mixing_rows, saved, layout)
        qkv_grad_rows, down_done = lax.optimization_barrier((qkv_grad_rows, down_done))
        qkv_grad_rows = lax.all_to_all(
            qkv_grad_rows, "gy", split_axis=1, concat_axis=0, tiled=True
        )
        normed_one_grad = settle(product("tc,dc->td", qkv_grad_rows, qkv_w))
        both_sum = jnp.concatenate(
            [product("td,tc->dc", normed_one, qkv_grad_rows).astype(BF), out_sum], axis=1
        )
        terms = jnp.stack(
            [
                jnp.sum(normed_one_grad * unit_one, axis=0),
                jnp.sum(middle_grad * unit_two, axis=0),
                jnp.sum(normed_two_grad * unit_three, axis=0),
                jnp.sum(cot_rows * unit_four, axis=0),
            ]
        )
        delta, terms = to_width_blocks(
            middle_delta + norm_back(normed_one_grad, unit_one, scale_one, gains[0]),
            tally(terms, ny),
            nx,
        )
        down_grad = down_done.astype(F32).T
        both_sum = with_layout_constraint(both_sum, Layout((0, 1)))
        gate_up_done, both_sum, delta, down_grad = lax.optimization_barrier(
            (gate_up_done, both_sum, delta, down_grad)
        )
        both_done = lax.psum_scatter(both_sum, "gx", scatter_dimension=0, tiled=True)
        gate_up_grad = gate_up_done.astype(F32)
        input_grad = cotangent + delta
        qkv_grad = both_done[:, :heads].astype(F32)
        out_grad = both_done[:, heads:].astype(F32).T
        return (outputs, input_grad, qkv_grad, out_grad, gate_up_grad, down_grad) + tuple(
            terms[i] for i in range(4)
        )

    return shards


def solution(mesh):
    placed = (
        P("gy", "gx"),
        P(("gx", "gy"), None),
        P("gx", "gy"),
        P("gy", "gx"),
        P("gx", None, "gy"),
        P("gy", "gx"),
        P("gx"),
        P("gx"),
        P("gx"),
        P("gx"),
        P("gy", "gx"),
    )
    return jax.shard_map(
        make_shards(mesh.shape["gx"], mesh.shape["gy"]),
        mesh=mesh,
        in_specs=placed,
        out_specs=(
            P("gy", "gx"),
            P("gy", "gx"),
            P("gx", "gy"),
            P("gy", "gx"),
            P("gx", None, "gy"),
            P("gy", "gx"),
            P("gx"),
            P("gx"),
            P("gx"),
            P("gx"),
        ),
        check_vma=False,
    )
```

```python
import functools
import math

import jax
import jax.numpy as jnp
from jax import lax
from jax.experimental import pallas as pl
from jax.experimental.layout import Layout, with_layout_constraint
from jax.experimental.pallas import tpu as pltpu
from jax.sharding import PartitionSpec as P

QUERY_HEADS = 8
KEY_VALUE_HEADS = 4
HEAD_SIZE = 256


EPSILON = 1e-06
SOFT_CAP = 50.0
GELU_COEF = 0.7978845608028654
CUBIC_COEF = 0.044715

BF = jnp.bfloat16
F32 = jnp.float32
MESH = pl.DeviceIdType.MESH
PARTS = 4
TILE = 768


def product(form, left, right):
    return jnp.einsum(form, left, right, preferred_element_type=F32)


def gelu_parts(pre_gate):
    inner_arg = GELU_COEF * (pre_gate + CUBIC_COEF * pre_gate * pre_gate * pre_gate)
    tanh_value = jnp.tanh(inner_arg)
    activated = 0.5 * pre_gate * (1.0 + tanh_value)
    derivative = 0.5 * (1.0 + tanh_value) + 0.5 * pre_gate * (
        1.0 - tanh_value * tanh_value
    ) * GELU_COEF * (1.0 + 3.0 * CUBIC_COEF * pre_gate * pre_gate)
    return (activated, derivative)


def block_layout(segment_row):
    length_total = segment_row.shape[0]
    places = jnp.arange(length_total, dtype=jnp.int32)
    same_doc = segment_row[:, None] == segment_row[None, :]
    starts = jnp.min(jnp.where(same_doc, places[None, :], length_total), axis=1)
    allowed = jnp.logical_and(same_doc, places[None, :] <= places[:, None])
    return (places - starts, allowed)


def rope_tables(position):
    half_dim = HEAD_SIZE // 2
    freq_steps = jnp.arange(half_dim, dtype=F32)
    frequency = jnp.exp(freq_steps * (-2.0 * math.log(10000.0) / HEAD_SIZE))
    angles = position.astype(F32)[:, None] * frequency[None, :]
    return (jnp.cos(angles)[:, None, :], jnp.sin(angles)[:, None, :])


def rotate(values, cos_table, sin_table, direction):
    half_dim = values.shape[-1] // 2
    leading = values[..., :half_dim]
    trailing = values[..., half_dim:]
    return jnp.concatenate(
        [
            leading * cos_table - direction * trailing * sin_table,
            trailing * cos_table + direction * leading * sin_table,
        ],
        axis=-1,
    )


def capped_scores(rotated_query, k_rot):
    token_rows = rotated_query.shape[0]
    query_groups = rotated_query.reshape(
        token_rows, KEY_VALUE_HEADS, QUERY_HEADS // KEY_VALUE_HEADS, HEAD_SIZE
    )
    raw_scores = product("tkgd,skd->kgts", query_groups, k_rot) * HEAD_SIZE ** (-0.5)
    return SOFT_CAP * jnp.tanh(raw_scores / SOFT_CAP)


def attention_forward(rows, layout):
    token_rows = rows.shape[0]
    query_span_width = QUERY_HEADS * HEAD_SIZE
    key_value_width = KEY_VALUE_HEADS * HEAD_SIZE
    allowed, cos_table, sin_table = layout
    query_part = (
        rows[:, :query_span_width].astype(F32).reshape(token_rows, QUERY_HEADS, HEAD_SIZE)
    )
    key_slice = (
        rows[:, query_span_width : query_span_width + key_value_width]
        .astype(F32)
        .reshape(token_rows, KEY_VALUE_HEADS, HEAD_SIZE)
    )
    value_slice = rows[:, query_span_width + key_value_width :].reshape(
        token_rows, KEY_VALUE_HEADS, HEAD_SIZE
    )
    rotated_query = rotate(query_part, cos_table, sin_table, 1.0).astype(BF)
    k_rot = rotate(key_slice, cos_table, sin_table, 1.0).astype(BF)
    capped = capped_scores(rotated_query, k_rot)
    log_total = jnp.log(jnp.sum(jnp.where(allowed, jnp.exp(capped), 0.0), axis=-1))
    weights_f = jnp.where(allowed, jnp.exp(capped - log_total[..., None]), 0.0)
    mixing_rows = product("kgts,skd->tkgd", weights_f.astype(BF), value_slice)
    mixing_rows = mixing_rows.astype(BF).reshape(token_rows, query_span_width)
    return (mixing_rows, (rotated_query, k_rot, value_slice, log_total))


def attention_backward(mixing_gradient, mixing_rows, saved, layout):
    rotated_query, k_rot, value_slice, log_total = saved
    token_rows = mixing_gradient.shape[0]
    heads_per_group = QUERY_HEADS // KEY_VALUE_HEADS
    allowed, cos_table, sin_table = layout
    capped = capped_scores(rotated_query, k_rot)
    weights_f = jnp.where(allowed, jnp.exp(capped - log_total[..., None]), 0.0)
    gradient_by_group = mixing_gradient.reshape(
        token_rows, KEY_VALUE_HEADS, heads_per_group, HEAD_SIZE
    )
    output_by_group = mixing_rows.reshape(token_rows, KEY_VALUE_HEADS, heads_per_group, HEAD_SIZE)
    row_delta = product("tkgd,tkgd->kgt", gradient_by_group, output_by_group)
    value_gradient = product("maew,emaq->wmq", weights_f.astype(BF), gradient_by_group)
    weight_grad = product("tkgd,skd->kgts", gradient_by_group, value_slice)
    score_gradient = (
        weights_f
        * (weight_grad - row_delta[..., None])
        * (1.0 - (capped / SOFT_CAP) ** 2)
        * HEAD_SIZE ** (-0.5)
    )
    score_gradient = score_gradient.astype(BF)
    query_gradient = product("kgts,skd->tkgd", score_gradient, k_rot).reshape(
        token_rows, QUERY_HEADS, HEAD_SIZE
    )
    key_gradient = product(
        "maew,emaq->wmq",
        score_gradient,
        rotated_query.reshape(token_rows, KEY_VALUE_HEADS, heads_per_group, HEAD_SIZE),
    )
    query_gradient = rotate(query_gradient, cos_table, sin_table, -1.0)
    key_gradient = rotate(key_gradient, cos_table, sin_table, -1.0)
    return jnp.concatenate(
        [
            query_gradient.reshape(token_rows, QUERY_HEADS * HEAD_SIZE),
            key_gradient.reshape(token_rows, KEY_VALUE_HEADS * HEAD_SIZE),
            value_gradient.reshape(token_rows, KEY_VALUE_HEADS * HEAD_SIZE),
        ],
        axis=1,
    ).astype(BF)


def inverse_rms(values):
    return lax.rsqrt(jnp.mean(values * values, axis=1, keepdims=True) + EPSILON)


def norm_back(grad_rows, unit_rows, scale_rows, gain):
    scaled = grad_rows * gain
    return scale_rows * (scaled - unit_rows * jnp.mean(scaled * unit_rows, axis=1, keepdims=True))


def flip(index, mask):
    return index + mask - 2 * mask * ((index // mask) % 2)


def flip_all(index, masks):
    bit = 1
    while bit <= masks:
        if masks & bit:
            index = flip(index, bit)
        bit *= 2
    return index


def greet(me, bits, lanes=0):
    barrier = pltpu.get_barrier_semaphore()
    for bit in bits:
        pl.semaphore_signal(barrier, inc=1, device_id={"gy": flip(me, bit)}, device_id_type=MESH)
    for d in range(1, lanes):
        other = (lax.axis_index("gx") + d) % lanes
        pl.semaphore_signal(barrier, inc=1, device_id={"gx": other}, device_id_type=MESH)
    pl.semaphore_wait(barrier, len(bits) + max(lanes - 1, 0))


def bit_orders(size):
    bits = []
    bit = 2
    while bit < size:
        bits.append(bit)
        bit *= 2
    return (bits + [1], bits[::-1] + [1])


def lay_out(rows_ref, blocks_ref, strip):
    lanes, count, width = blocks_ref.shape

    @pl.loop(0, count // strip)
    def _(i):
        rows = pl.ds(i * strip, strip)
        for k in range(lanes):
            rows_ref[rows, k * width : (k + 1) * width] = blocks_ref[k, rows].astype(F32)


def cut_up(blocks_ref, rows_ref, strip):
    lanes, count, width = blocks_ref.shape

    @pl.loop(0, count // strip)
    def _(i):
        rows = pl.ds(i * strip, strip)
        for k in range(lanes):
            blocks_ref[k, rows] = rows_ref[rows, k * width : (k + 1) * width].astype(BF)


def swap_start(lanes, side_ref, there_ref, sems):
    me = lax.axis_index("gx")
    own, send_sem, recv_sem = sems
    made = [pltpu.make_async_copy(side_ref.at[me], there_ref.at[me], own)]
    for d in range(1, lanes):
        other = (me + d) % lanes
        made.append(
            pltpu.make_async_remote_copy(
                src_ref=side_ref.at[other],
                dst_ref=there_ref.at[me],
                send_sem=send_sem.at[d],
                recv_sem=recv_sem.at[d],
                device_id={"gx": other},
                device_id_type=MESH,
            )
        )
    for copy in made:
        copy.start()
    return made


def swap_sems(lanes):
    return [
        pltpu.SemaphoreType.DMA,
        pltpu.SemaphoreType.DMA((lanes,)),
        pltpu.SemaphoreType.DMA((lanes,)),
    ]


def greet_lanes(lanes):
    barrier = pltpu.get_barrier_semaphore()
    for d in range(1, lanes):
        other = (lax.axis_index("gx") + d) % lanes
        pl.semaphore_signal(barrier, inc=1, device_id={"gx": other}, device_id_type=MESH)
    pl.semaphore_wait(barrier, lanes - 1)


def gather_rows_kernel(lanes, native_ref, small_ref, rows_ref, wide_ref, *scratch):
    send_ref, there_ref, small_all, *sems = scratch
    big_sems, small_sems = sems[:3], sems[3:]
    fold, pair = send_ref.shape[1:]
    width = pair // 2
    strip = 16
    for j in range(lanes):
        for side in range(2):

            @pl.loop(0, fold // strip)
            def _(i):
                rows = pl.ds((2 * j + side) * fold + i * strip, strip)
                send_ref[j, pl.ds(i * strip, strip), side * width : (side + 1) * width] = (
                    native_ref[rows].astype(BF)
                )

    greet_lanes(lanes)
    copies = swap_start(lanes, send_ref, there_ref, big_sems)
    copies += hand_round(lanes, small_ref, small_all, small_sems)
    for copy in copies:
        copy.wait()
    for k in range(lanes):
        columns = slice(k * width, (k + 1) * width)
        wide_ref[:, columns] = small_all[k]
        for side in range(2):

            @pl.loop(0, fold // strip)
            def _(i):
                rows_ref[pl.ds(side * fold + i * strip, strip), columns] = there_ref[
                    k, pl.ds(i * strip, strip), side * width : (side + 1) * width
                ].astype(F32)


def scatter_rows_kernel(lanes, rows_ref, wide_ref, native_ref, small_ref, *scratch):
    send_ref, there_ref, small_send, small_all, *sems = scratch
    big_sems, small_sems = sems[:3], sems[3:]
    fold, pair = send_ref.shape[1:]
    width = pair // 2
    strip = 16
    for j in range(lanes):
        columns = slice(j * width, (j + 1) * width)
        small_send[j] = wide_ref[:, columns]
        for side in range(2):

            @pl.loop(0, fold // strip)
            def _(i):
                send_ref[j, pl.ds(i * strip, strip), side * width : (side + 1) * width] = rows_ref[
                    pl.ds(side * fold + i * strip, strip), columns
                ].astype(BF)

    greet_lanes(lanes)
    copies = swap_start(lanes, send_ref, there_ref, big_sems)
    copies += swap_start(lanes, small_send, small_all, small_sems)
    for copy in copies:
        copy.wait()
    total = small_all[0]
    for k in range(1, lanes):
        total = total + small_all[k]
    small_ref[...] = total
    for k in range(lanes):
        for side in range(2):

            @pl.loop(0, fold // strip)
            def _(i):
                rows = pl.ds((2 * k + side) * fold + i * strip, strip)
                native_ref[rows] = there_ref[
                    k, pl.ds(i * strip, strip), side * width : (side + 1) * width
                ].astype(F32)


def hand_round(lanes, own_ref, all_ref, sems):
    me = lax.axis_index("gx")
    own, send_sem, recv_sem = sems
    made = [pltpu.make_async_copy(own_ref, all_ref.at[me], own)]
    for d in range(1, lanes):
        made.append(
            pltpu.make_async_remote_copy(
                src_ref=own_ref,
                dst_ref=all_ref.at[me],
                send_sem=send_sem.at[d],
                recv_sem=recv_sem.at[d],
                device_id={"gx": (me + d) % lanes},
                device_id_type=MESH,
            )
        )
    for copy in made:
        copy.start()
    return made


def exchange(kernel, lanes, big, small, outs, extra, call):
    total, width = big.shape
    space = pl.BlockSpec(memory_space=pltpu.VMEM)
    count = total * width // (lanes * outs[2])
    block = (lanes, count // 2, 2 * outs[2])
    cut = (lanes, small.shape[0], outs[2])
    return pl.pallas_call(
        functools.partial(kernel, lanes),
        out_shape=[jax.ShapeDtypeStruct(v, F32) for v in outs[:2]],
        in_specs=[space] * 2,
        out_specs=[space] * 2,
        scratch_shapes=[pltpu.VMEM(block, BF), pltpu.VMEM(block, BF)]
        + [pltpu.VMEM(cut, F32)] * (1 + extra)
        + swap_sems(lanes)
        + swap_sems(lanes),
        compiler_params=pltpu.CompilerParams(
            collective_id=call, has_side_effects=True, vmem_limit_bytes=32 << 20
        ),
        cost_estimate=pl.CostEstimate(
            flops=0, bytes_accessed=total * width * 16, transcendentals=0
        ),
        name="exchange",
    )(big, small)


def to_whole_rows(values, small, lanes):
    total, width = values.shape
    outs = ((total // lanes, lanes * width), (small.shape[0], lanes * width), width)
    return exchange(gather_rows_kernel, lanes, values, small, outs, 0, 9)


def to_width_blocks(rows, small, lanes):
    count, whole = rows.shape
    width = whole // lanes
    outs = ((count * lanes, width), (small.shape[0], width), width)
    return exchange(scatter_rows_kernel, lanes, rows, small, outs, 1, 10)


def spread_kernel(size, lanes, *refs):
    if lanes:
        own_ref, rows_ref, all_ref, there_ref, local_sem, send_sem, recv_sem, *rest = refs
        side_ref, *sems = rest
    else:
        own_ref, all_ref, local_sem, send_sem, recv_sem = refs
    me = lax.axis_index("gy")
    orders = bit_orders(size)
    half = own_ref.shape[0] // 2
    greet(me, orders[0], lanes)
    keep = pltpu.make_async_copy(own_ref, all_ref.at[me], local_sem)
    keep.start()
    copies = {}
    arrival = {}

    def copy(h, bit, r):
        n = len(copies)
        rows = pl.ds(h * half, half)
        where = flip_all(me, r)
        source = own_ref.at[rows] if r == 0 else all_ref.at[where, rows]
        made = pltpu.make_async_remote_copy(
            src_ref=source,
            dst_ref=all_ref.at[where, rows],
            send_sem=send_sem.at[n],
            recv_sem=recv_sem.at[n],
            device_id={"gy": flip(me, bit)},
            device_id_type=MESH,
        )
        copies[h, bit, r] = made
        arrival[h, r ^ bit] = made
        made.start()

    for step in range(len(orders[0])):
        for h in range(2):
            copy(h, orders[h][step], 0)
    swapped = []
    if lanes:
        cut_up(side_ref, rows_ref, 16)
        swapped = swap_start(lanes, side_ref, there_ref, sems)
    landed = set()

    def land(h, r):
        if (h, r) not in landed:
            landed.add((h, r))
            arrival[h, r].wait_recv()

    held = [[0], [0]]
    for step in range(len(orders[0])):
        for h in range(2):
            bit = orders[h][step]
            for r in held[h]:
                if r:
                    land(h, r)
                    copy(h, bit, r)
        for h in range(2):
            held[h] = held[h] + [r ^ orders[h][step] for r in held[h]]
    for h in range(2):
        for r in range(1, size):
            land(h, r)
    for made in copies.values():
        made.wait_send()
    for copy in [keep] + swapped:
        copy.wait()


def spread(values, side=None):
    size = lax.axis_size("gy")
    values = values.astype(BF)
    rows, width = values.shape
    count = 2 * (size - 1)
    sides = [] if side is None else [side]
    lanes = 0 if side is None else lax.axis_size("gx")
    blocks = (lanes, rows, width // max(lanes, 1))
    space = pl.BlockSpec(memory_space=pltpu.VMEM)
    out = pl.pallas_call(
        functools.partial(spread_kernel, size, lanes),
        out_shape=[jax.ShapeDtypeStruct((size, rows, width), values.dtype)]
        + [jax.ShapeDtypeStruct(blocks, BF) for v in sides],
        in_specs=[space] * (1 + len(sides)),
        out_specs=[pl.BlockSpec(memory_space=pltpu.HBM)] * (1 + len(sides)),
        scratch_shapes=[
            pltpu.SemaphoreType.DMA,
            pltpu.SemaphoreType.DMA((count,)),
            pltpu.SemaphoreType.DMA((count,)),
        ]
        + ([pltpu.VMEM(blocks, BF)] + swap_sems(lanes) if lanes else []),
        compiler_params=pltpu.CompilerParams(
            collective_id=4 if lanes else 0, has_side_effects=True, vmem_limit_bytes=60 << 20 if lanes else 32 << 20
        ),
        cost_estimate=pl.CostEstimate(
            flops=0, bytes_accessed=size * rows * width * 16, transcendentals=0
        ),
        name="spread",
    )(values, *sides)
    whole = out[0].reshape(size * rows, width)
    return (whole, out[1]) if lanes else whole


def settle_kernel(size, lanes, fused, *refs):
    if fused:
        left_ref, right_ref, *refs = refs
        *refs, picked, weights, product_ref, left_sem, right_sem = refs
        refs = [product_ref] + refs
    if lanes:
        parts_ref, side_ref, sum_ref, rows_ref, came, kept, send_sem, recv_sem, *rest = refs
        there_ref, *sems = rest
    else:
        parts_ref, sum_ref, came, kept, send_sem, recv_sem = refs
    me = lax.axis_index("gy")
    orders = tuple(order[::-1] for order in bit_orders(size)) * (PARTS // 2)
    half = sum_ref.shape[0] // PARTS
    strip = 16
    def left_copy(j):
        count = left_ref.shape[1]
        return pltpu.make_async_copy(
            left_ref.at[flip_all(me, turn[j])],
            picked.at[pl.ds(j * count, count)],
            left_sem.at[j],
        )

    def right_copy(i):
        rows = pl.ds(pl.multiple_of(i * TILE, TILE), TILE)
        return pltpu.make_async_copy(right_ref.at[rows], weights.at[rows], right_sem.at[i])

    def multiply(low, high):
        count = left_ref.shape[1]
        for j in range(low, high):
            left_copy(j).wait()

        @pl.loop(0, weights.shape[0] // TILE)
        def _(i):
            if low == 0:
                right_copy(i).wait()
            columns = pl.ds(pl.multiple_of(i * TILE, TILE), TILE)
            block = lax.dot_general(
                picked[low * count : high * count],
                weights[columns],
                (((1,), (1,)), ((), ())),
                preferred_element_type=F32,
            ).astype(BF)
            for j in range(low, high):
                parts_ref[flip_all(me, turn[j]), :, columns] = block[
                    (j - low) * count : (j - low + 1) * count
                ]

    turn = [r for r in range(size) if r & 1] + [r for r in range(size - 1, -1, -1) if not r & 1]
    if fused:
        for j in range(size // 2):
            left_copy(j).start()
        for i in range(weights.shape[0] // TILE):
            right_copy(i).start()
        for j in range(size // 2, size):
            left_copy(j).start()
    greet(me, orders[0], lanes)
    swapped = swap_start(lanes, side_ref, there_ref, sems) if lanes else []
    slot = {}
    for h in range(PARTS):
        held = list(range(size))
        for step, bit in enumerate(orders[h]):
            held = [r for r in held if not r & bit]
            for r in held:
                slot[h, step, r] = len(slot)
    copies = {}

    def view(h, step, r):
        if step == 0:
            return parts_ref.at[flip_all(me, r), pl.ds(h * half, half)]
        return kept.at[h, r]

    def send(h, step):
        bit = orders[h][step]
        gone = set()
        for b in orders[h][:step]:
            gone.add(b)
        for r in range(size):
            if r & bit and not any(r & b for b in gone):
                n = slot[h, step, r ^ bit]
                made = pltpu.make_async_remote_copy(
                    src_ref=view(h, step, r),
                    dst_ref=came.at[n],
                    send_sem=send_sem.at[n],
                    recv_sem=recv_sem.at[n],
                    device_id={"gy": flip(me, bit)},
                    device_id_type=MESH,
                )
                copies[h, step, r ^ bit] = made
                made.start()

    def gather(h, step, r, last):
        n = slot[h, step, r]
        copies[h, step, r].wait_recv()

        @pl.loop(0, half // strip)
        def _(i):
            rows = pl.ds(i * strip, strip)
            total = view(h, step, r)[rows].astype(F32) + came[n, rows].astype(F32)
            if last:
                sum_ref[pl.ds(h * half + i * strip, strip)] = total
            else:
                kept[h, r, rows] = total.astype(BF)

    steps = len(orders[0])
    if fused:
        multiply(0, size // 2)
    for h in range(PARTS):
        send(h, 0)
    if fused:
        multiply(size // 2, size - 1)
    for step in range(steps):
        if lanes and step == steps - 1:
            for copy in swapped:
                copy.wait()
            lay_out(rows_ref, there_ref, strip)
        for h in range(PARTS):
            bits = orders[h][: step + 1]
            later = orders[h][step + 1] if step + 1 < steps else 0
            left = [r for r in range(size) if not any(r & b for b in bits)]
            for r in left:
                if r & later:
                    gather(h, step, r, False)
            if later:
                send(h, step + 1)
            for r in left:
                if not r & later and not (fused and step == 0):
                    gather(h, step, r, step == steps - 1)
        if fused and step == 0:
            multiply(size - 1, size)
            for h in range(PARTS):
                for r in range(size):
                    if not r & orders[h][0] and not r & orders[h][1]:
                        gather(h, 0, r, False)
    for made in copies.values():
        made.wait_send()


def settle(parts, side=None, right=None):
    size = lax.axis_size("gy")
    parts = parts.astype(BF)
    total, inner = parts.shape
    width = inner if right is None else right.shape[0]
    rows = total // size
    count = PARTS * (size - 1)
    sides = [] if side is None else [side]
    rights = [] if right is None else [right]
    lanes = 0 if side is None else side.shape[0]
    space = pl.BlockSpec(memory_space=pltpu.VMEM)
    scratch = [
        pltpu.VMEM((count, rows // PARTS, width), BF),
        pltpu.VMEM((PARTS, size, rows // PARTS, width), BF),
        pltpu.SemaphoreType.DMA((count,)),
        pltpu.SemaphoreType.DMA((count,)),
    ]
    if lanes:
        scratch += [pltpu.VMEM(side.shape, side.dtype)] + swap_sems(lanes)
    if rights:
        scratch += [
            pltpu.VMEM((total, inner), BF),
            pltpu.VMEM((width, inner), BF),
            pltpu.VMEM((size, rows, width), BF),
            pltpu.SemaphoreType.DMA((size,)),
            pltpu.SemaphoreType.DMA((width // TILE,)),
        ]
    out = pl.pallas_call(
        functools.partial(settle_kernel, size, lanes, bool(rights)),
        out_shape=[jax.ShapeDtypeStruct((rows, width), F32)] * (1 + len(sides)),
        in_specs=[pl.BlockSpec(memory_space=pl.ANY)] * (2 * len(rights))
        + [space] * (1 - len(rights) + len(sides)),
        out_specs=[space] * (1 + len(sides)),
        scratch_shapes=scratch,
        compiler_params=pltpu.CompilerParams(
            collective_id=5 if lanes else 1, has_side_effects=True, vmem_limit_bytes=40 << 20
        ),
        cost_estimate=pl.CostEstimate(
            flops=0, bytes_accessed=total * width * 16, transcendentals=0
        ),
        name="settle",
    )
    operands = [parts.reshape(size, rows, inner)] + rights
    if rights:
        operands = [pltpu.with_memory_space_constraint(v, pltpu.HBM) for v in operands]
    out = out(*operands, *sides)
    return out if lanes else out[0]


def tally_kernel(size, own_ref, sum_ref, came, send_sem, recv_sem):
    me = lax.axis_index("gy")
    barrier = pltpu.get_barrier_semaphore()
    for d in range(1, size):
        pl.semaphore_signal(
            barrier, inc=1, device_id={"gy": (me + d) % size}, device_id_type=MESH
        )
    pl.semaphore_wait(barrier, size - 1)
    copies = []
    for d in range(1, size):
        made = pltpu.make_async_remote_copy(
            src_ref=own_ref,
            dst_ref=came.at[d],
            send_sem=send_sem.at[d],
            recv_sem=recv_sem.at[d],
            device_id={"gy": (me + d) % size},
            device_id_type=MESH,
        )
        made.start()
        copies.append(made)
    total = own_ref[...]
    for d in range(1, size):
        copies[d - 1].wait_recv()
        total = total + came[d]
    sum_ref[...] = total
    for made in copies:
        made.wait_send()


def tally(values, size):
    return pl.pallas_call(
        functools.partial(tally_kernel, size),
        out_shape=jax.ShapeDtypeStruct(values.shape, F32),
        in_specs=[pl.BlockSpec(memory_space=pltpu.VMEM)],
        out_specs=pl.BlockSpec(memory_space=pltpu.VMEM),
        scratch_shapes=[
            pltpu.VMEM((size,) + values.shape, F32),
            pltpu.SemaphoreType.DMA((size,)),
            pltpu.SemaphoreType.DMA((size,)),
        ],
        compiler_params=pltpu.CompilerParams(collective_id=2, has_side_effects=True),
        name="tally",
    )(values)


def make_shards(nx, ny):
    blocks = [((b // ny) * ny + b % ny, (b % nx) * ny + b // nx) for b in range(nx * ny)]

    def shards(
        inputs,
        segment_ids,
        qkv_weight,
        out_weight,
        gate_up_weight,
        down_weight,
        first_gain,
        second_gain,
        third_gain,
        fourth_gain,
        cotangent,
    ):
        width = inputs.shape[1]

        own = inputs.shape[0] // nx
        heads = qkv_weight.shape[1]
        qkv_w = lax.all_gather(qkv_weight, "gx", axis=0, tiled=True)
        gains = jnp.stack([first_gain, second_gain, third_gain, fourth_gain])
        gains, qkv_w = lax.optimization_barrier((gains, qkv_w))
        x_rows, gains = to_whole_rows(inputs, gains, nx)
        gains = gains[:, None, :]
        hid = gate_up_weight.shape[2]
        wide_w = lax.all_gather(
            jnp.concatenate([gate_up_weight.reshape(width, 2 * hid), out_weight.T], axis=1),
            "gx",
            axis=0,
            tiled=True,
        )
        gate_w, up_w, out_w = wide_w[:, :hid], wide_w[:, hid : 2 * hid], wide_w[:, 2 * hid :]
        down_w = lax.all_gather(down_weight.T, "gx", axis=0, tiled=True)

        segment_row = lax.ppermute(segment_ids[0], ("gx", "gy"), blocks)
        position, allowed = block_layout(segment_row)
        layout = (allowed,) + rope_tables(position)

        scale_one = inverse_rms(x_rows)
        unit_one = x_rows * scale_one
        normed_one = spread(unit_one * gains[0])
        rows = product("td,dc->tc", normed_one, qkv_w).astype(BF)
        rows = lax.all_to_all(rows, "gy", split_axis=0, concat_axis=1, tiled=True)
        mixing_rows, saved = attention_forward(rows, layout)
        mixed = lax.all_to_all(mixing_rows, "gy", split_axis=1, concat_axis=0, tiled=True)
        attn_branch = settle(product("tc,dc->td", mixed, out_w))
        scale_two = inverse_rms(attn_branch)
        unit_two = attn_branch * scale_two
        attn_term = unit_two * gains[1]
        middle = x_rows + attn_term
        scale_three = inverse_rms(middle)
        unit_three = middle * scale_three
        normed_two = spread(unit_three * gains[2])
        pre_gate = product("td,df->tf", normed_two, gate_w)
        up_part = product("td,df->tf", normed_two, up_w)
        value, slope = gelu_parts(pre_gate)
        hidden = (value * up_part).astype(BF)
        ff_branch, cot_rows = settle(
            hidden, cotangent.astype(BF).reshape(nx, own, width), down_w
        )
        scale_four = inverse_rms(ff_branch)
        unit_four = ff_branch * scale_four
        ff_grad, delta = spread(
            norm_back(cot_rows, unit_four, scale_four, gains[3]),
            attn_term + unit_four * gains[3],
        )
        outputs = inputs + delta.reshape(inputs.shape).astype(F32)

        down_sum = product("td,tf->df", ff_grad, hidden).astype(BF)
        down_sum, ff_grad = lax.optimization_barrier((down_sum, ff_grad))
        down_done = lax.psum_scatter(down_sum, "gx", scatter_dimension=0, tiled=True)
        hidden_grad = product("td,df->tf", ff_grad, down_w)
        gate_grad = (hidden_grad * up_part * slope).astype(BF)
        up_grad = (hidden_grad * value).astype(BF)
        gate_up_sum = jnp.stack(
            [
                product("td,tf->df", normed_two, gate_grad).astype(BF),
                product("td,tf->df", normed_two, up_grad).astype(BF),
            ],
            axis=1,
        )
        gate_up_sum, gate_grad, up_grad = lax.optimization_barrier(
            (gate_up_sum, gate_grad, up_grad)
        )
        gate_up_done = lax.psum_scatter(gate_up_sum, "gx", scatter_dimension=0, tiled=True)
        normed_two_grad = settle(
            product("tf,df->td", gate_grad, gate_w)
            + product("tf,df->td", up_grad, up_w)
        )
        middle_delta = norm_back(normed_two_grad, unit_three, scale_three, gains[2])
        middle_grad = cot_rows + middle_delta
        branch_grad = spread(norm_back(middle_grad, unit_two, scale_two, gains[1]))
        out_sum = product("td,tc->dc", branch_grad, mixed).astype(BF)
        mixing_gradient = product("td,dc->tc", branch_grad, out_w).astype(BF)
        mixing_gradient = lax.all_to_all(
            mixing_gradient, "gy", split_axis=0, concat_axis=1, tiled=True
        )
        qkv_grad_rows = attention_backward(mixing_gradient, mixing_rows, saved, layout)
        qkv_grad_rows, down_done = lax.optimization_barrier((qkv_grad_rows, down_done))
        qkv_grad_rows = lax.all_to_all(
            qkv_grad_rows, "gy", split_axis=1, concat_axis=0, tiled=True
        )
        normed_one_grad = settle(product("tc,dc->td", qkv_grad_rows, qkv_w))
        both_sum = jnp.concatenate(
            [product("td,tc->dc", normed_one, qkv_grad_rows).astype(BF), out_sum], axis=1
        )
        terms = jnp.stack(
            [
                jnp.sum(normed_one_grad * unit_one, axis=0),
                jnp.sum(middle_grad * unit_two, axis=0),
                jnp.sum(normed_two_grad * unit_three, axis=0),
                jnp.sum(cot_rows * unit_four, axis=0),
            ]
        )
        delta, terms = to_width_blocks(
            middle_delta + norm_back(normed_one_grad, unit_one, scale_one, gains[0]),
            tally(terms, ny),
            nx,
        )
        down_grad = down_done.astype(F32).T
        both_sum = with_layout_constraint(both_sum, Layout((0, 1)))
        gate_up_done, both_sum, delta, down_grad = lax.optimization_barrier(
            (gate_up_done, both_sum, delta, down_grad)
        )
        both_done = lax.psum_scatter(both_sum, "gx", scatter_dimension=0, tiled=True)
        gate_up_grad = gate_up_done.astype(F32)
        input_grad = cotangent + delta
        qkv_grad = both_done[:, :heads].astype(F32)
        out_grad = both_done[:, heads:].astype(F32).T
        return (outputs, input_grad, qkv_grad, out_grad, gate_up_grad, down_grad) + tuple(
            terms[i] for i in range(4)
        )

    return shards


def solution(mesh):
    placed = (
        P("gy", "gx"),
        P(("gx", "gy"), None),
        P("gx", "gy"),
        P("gy", "gx"),
        P("gx", None, "gy"),
        P("gy", "gx"),
        P("gx"),
        P("gx"),
        P("gx"),
        P("gx"),
        P("gy", "gx"),
    )
    return jax.shard_map(
        make_shards(mesh.shape["gx"], mesh.shape["gy"]),
        mesh=mesh,
        in_specs=placed,
        out_specs=(
            P("gy", "gx"),
            P("gy", "gx"),
            P("gx", "gy"),
            P("gy", "gx"),
            P("gx", None, "gy"),
            P("gy", "gx"),
            P("gx"),
            P("gx"),
            P("gx"),
            P("gx"),
        ),
        check_vma=False,
    )
```
